128 devices in a mesh: seq: 32 (over x, y, core), head: 4 (over z).
Axes of the slice: x: 4, y: 4, z: 4, core: 2. Of those that a mesh axis runs over, the one named last changes fastest.
Arguments:
- queries: bfloat16 [4096, 8192], P('seq', 'head'), may hold values from -2.5 to 2.5
- keys: bfloat16 [4096, 8192], P('seq', 'head'), may hold values from -2.5 to 2.5
- values: bfloat16 [4096, 4096], P('seq', 'head'), may hold values from -2.5 to 2.5
- out_grad: bfloat16 [4096, 4096], P('seq', 'head'), may hold values from -2.5 to 2.5
- log_gate: float32 [64, 4096], P('head', 'seq'), may hold values from -1 to 0
- level_weight: float32 [6, 64, 4096], P(None, 'head', 'seq'), may hold values from 0.25 to 2
- doc_start: int32 [4096], P('seq'), may hold values 0 or 1
Outputs:
- grad_queries: bfloat16 [4096, 8192], P('seq', 'head')
- grad_keys: bfloat16 [4096, 8192], P('seq', 'head')
- grad_values: bfloat16 [4096, 4096], P('seq', 'head')
- grad_level_weight: float32 [6, 64, 4096], P(None, 'head', 'seq')
- grad_log_gate: float32 [64, 4096], P('head', 'seq')
The draws below stay inside these ranges and needn't reach their ends.
All inputs are finite; a program needn't handle non-finite values. No bound on the sum of `doc_start` on one device may be relied on, other than what follows from the above.
Results may differ from the reference program's by a relative error of at most 0.0027.
Values sent between devices are 32-bit elements; how exact they have to be, the bound alone decides.
A program may use at most 128 MiB of HBM per device.

```python
import math
import jax
import jax.numpy as jnp
from jax import lax

HEAD_COUNT = 64
DK = 128
DV = 64
NL = 6
SPAN = 64
TOK_DEV = 128
TOKEN_COUNT = 4096
SPANS = 64


def draw_log_gate(key, part):
    every_key = jax.random.split(key, 7)
    slow_share = 0.5
    sluggish_head = jax.random.uniform(every_key[0], (HEAD_COUNT, 1)) < slow_share
    fast_rate = jnp.exp(jax.random.uniform(every_key[1], (HEAD_COUNT, 1), minval=jnp.log(0.02), maxval=jnp.log(0.05)))
    slow_rate = jnp.exp(jax.random.uniform(every_key[2], (HEAD_COUNT, 1), minval=jnp.log(0.1), maxval=jnp.log(0.56))) / TOKEN_COUNT
    block_count = TOKEN_COUNT // TOK_DEV
    block_factor = jnp.exp(jax.random.uniform(every_key[3], (HEAD_COUNT, block_count), minval=jnp.log(0.5), maxval=jnp.log(2.0)))
    block_factor = jnp.repeat(block_factor, TOK_DEV, axis=1)
    rough = jax.random.uniform(every_key[4], (HEAD_COUNT, TOKEN_COUNT), minval=0.5, maxval=2.0)
    decay_speed = jnp.where(sluggish_head, slow_rate, fast_rate * block_factor) * rough
    spike_position = jax.random.randint(every_key[5], (3,), 0, TOKEN_COUNT)
    spike_struck = jnp.any(jnp.arange(TOKEN_COUNT)[None, :] == spike_position[:, None], axis=0)
    spike_length = jnp.log(1.0 - jax.random.uniform(every_key[6], (HEAD_COUNT, 1), minval=0.2, maxval=0.4))
    spike_event = jnp.where(sluggish_head & spike_struck[None, :], spike_length, 0.0)
    return (spike_event - decay_speed).astype(jnp.float32)


def place_ends(values, rng, smallest, top_value):
    spot = [jax.random.randint(jax.random.fold_in(rng, axis), (), 0, length) for axis, length in enumerate(values.shape)]
    longest = values.shape.index(max(values.shape))
    neighbour = spot[:longest] + [(spot[longest] + 1) % values.shape[longest]] + spot[longest + 1:]
    return values.at[tuple(spot)].set(smallest).at[tuple(neighbour)].set(top_value)


def block_scale(key, dims, cuts, smallest, largest):
    loudness, own = 1.0, jax.random.fold_in(key, 6)
    for dim, shards_of in cuts:
        draws = jnp.exp(jax.random.uniform(jax.random.fold_in(own, dim), (shards_of,), jnp.float32, smallest / len(cuts), largest / len(cuts)))
        loudness = loudness * jnp.repeat(draws, dims[dim] // shards_of).reshape([-1 if axis == dim else 1 for axis in range(len(dims))])
    return loudness


def scatter_about(rng, extent, deviation, reach, shards=(), dtype=jnp.bfloat16):
    result = jax.random.normal(rng, extent, jnp.float32) * deviation
    if len(shards) > 0:
        result = block_scale(rng, extent, shards, -0.22, 0.18) * result
    return jnp.clip(result, min=-reach, max=reach).astype(dtype)


def setup_inputs(seed: int = 0) -> dict:
    key_of = jax.random.split(jax.random.key(seed), 8)
    return {
        "queries": scatter_about(key_of[0], (TOKEN_COUNT, HEAD_COUNT * DK), 0.16, 2.5, ((0, 32), (1, 4))),
        "keys": scatter_about(key_of[1], (TOKEN_COUNT, HEAD_COUNT * DK), 0.16, 2.5, ((0, 32), (1, 4))),
        "values": scatter_about(key_of[2], (TOKEN_COUNT, HEAD_COUNT * DV), 0.16, 2.5, ((0, 32), (1, 4))),
        "out_grad": scatter_about(key_of[3], (TOKEN_COUNT, HEAD_COUNT * DV), 0.16, 2.5, ((0, 32), (1, 4))),
        "log_gate": draw_log_gate(jax.random.fold_in(key_of[7], 71), 0),
        "level_weight": jnp.clip(jnp.exp(math.log(2.0) - 2.0794415 * jax.random.uniform(key_of[5], (NL, HEAD_COUNT, TOKEN_COUNT), jnp.float32) ** block_scale(key_of[5], (NL, HEAD_COUNT, TOKEN_COUNT), ((1, 4), (2, 32)), -0.2, 0.2)), 0.25, 2.0),
        "doc_start": place_ends((jax.random.randint(key_of[6], (TOKEN_COUNT,), 0, TOK_DEV * 8) < 1).astype(jnp.int32), jax.random.fold_in(key_of[6], 1), 0, 1),
    }


exact_mode = lax.Precision.HIGHEST

def group_sums(span_log, span_dead, width):
    groups = span_log.shape[0] // width
    logs = span_log.reshape(groups, width)
    deads = span_dead.reshape(groups, width)
    return (jnp.cumsum(logs, axis=1), jnp.cumsum(deads, axis=1), logs, deads)

def fenwick_pull(states, span_log, span_dead):
    total = states.shape[1]
    rows = states.shape[2]
    cols = states.shape[3]
    pieces = [jnp.zeros((total, rows, cols), jnp.float32)]
    for level in range(1, NL - 1):
        width = 2 ** (level - 1)
        groups = total // (2 * width)
        cum_log, cum_dead, logs, deads = group_sums(span_log, span_dead, 2 * width)
        source = states[level].reshape(groups, 2 * width, rows, cols)[:, :width]
        reach_log = cum_log[:, width - 1:2 * width - 1]
        reach_dead = cum_dead[:, width - 1:2 * width - 1]
        same = reach_dead[:, :, None] == cum_dead[:, None, :width]
        gap = reach_log[:, :, None] - cum_log[:, None, :width]
        weight = jnp.where(same, jnp.exp(jnp.where(same, gap, 0.0)), 0.0)
        pulled = jnp.einsum('gis,gsde->gide', weight, source, precision=exact_mode)
        pieces.append(jnp.concatenate([jnp.zeros_like(pulled), pulled], axis=1).reshape(total, rows, cols))
    width = 2 ** (NL - 2)
    groups = total // width
    cum_log, cum_dead, logs, deads = group_sums(span_log, span_dead, width)
    source = states[NL - 1].reshape(groups, width, rows, cols)
    end_same = cum_dead[:, -1:] == cum_dead
    end_weight = jnp.where(end_same, jnp.exp(jnp.where(end_same, cum_log[:, -1:] - cum_log, 0.0)), 0.0)
    block_total = jnp.einsum('gs,gsde->gde', end_weight, source, precision=exact_mode)
    block_decay = jnp.exp(cum_log[:, -1]) * (cum_dead[:, -1] == 0).astype(jnp.float32)

    def carry_step(carry, inputs):
        decay_now, total_now = inputs
        return (decay_now * carry + total_now, carry)
    _, entering = lax.scan(carry_step, jnp.zeros((rows, cols), jnp.float32), (block_decay, block_total))
    lead = jnp.exp(cum_log - logs) * (cum_dead - deads == 0).astype(jnp.float32)
    pieces.append((lead[:, :, None, None] * entering[:, None]).reshape(total, rows, cols))
    return jnp.stack(pieces)

def head_pass(query_h, key_h, value_h, grad_h, gate_h, weight_h, start_all):
    positions = jnp.arange(SPAN)
    causal = positions[:, None] >= positions[None, :]
    cum_gate = jnp.cumsum(gate_h, axis=1)
    cum_reset = jnp.cumsum(start_all, axis=1)
    valid = causal[None] & (cum_reset[:, :, None] == cum_reset[:, None, :])
    gap = cum_gate[:, :, None] - cum_gate[:, None, :]
    decay_in = jnp.where(valid, jnp.exp(jnp.where(valid, gap, 0.0)), 0.0)
    from_start = jnp.exp(cum_gate) * (cum_reset == 0).astype(jnp.float32)
    to_end = jnp.exp(cum_gate[:, -1:] - cum_gate) * (cum_reset == cum_reset[:, -1:]).astype(jnp.float32)
    span_log = cum_gate[:, -1]
    span_dead = (cum_reset[:, -1] > 0).astype(jnp.int32)
    query_f = query_h.astype(jnp.float32)
    key_f = key_h.astype(jnp.float32)
    value_f = value_h.astype(jnp.float32)
    grad_f = grad_h.astype(jnp.float32)
    scores = jnp.einsum('ctd,csd->cts', query_f, key_f, precision=exact_mode)
    grad_dot = jnp.einsum('cte,cse->cts', grad_f, value_f, precision=exact_mode)
    weighted = decay_in * weight_h[0][:, :, None]
    prob_mix = (weighted * scores).astype(jnp.bfloat16)
    grad_mix = (weighted * grad_dot).astype(jnp.bfloat16)
    intra = lax.optimization_barrier(jnp.sum(decay_in * scores * grad_dot, axis=2))
    end_col = to_end[:, :, None]
    span_state = jnp.einsum('csd,cse->cde', key_f * end_col, value_f, precision=exact_mode)
    forward = fenwick_pull(jnp.broadcast_to(span_state[None], (NL,) + span_state.shape), span_log, span_dead)
    query_state = jnp.einsum('ctd,lcde->lcte', query_f, forward, precision=exact_mode)
    lam_start = weight_h * from_start[None]
    out_in = jnp.einsum('lcte,lct->cte', query_state, lam_start, precision=exact_mode)
    level_in = jnp.einsum('lcte,cte->lct', query_state, grad_f, precision=exact_mode) * from_start[None]
    grad_weighted = lam_start[:, :, :, None] * grad_f[None]
    query_in = jnp.einsum('lcte,lcde->ctd', grad_weighted, forward, precision=exact_mode)
    out_loc = jnp.einsum('cts,cse->cte', prob_mix.astype(jnp.float32), value_f, precision=exact_mode)
    query_loc = jnp.einsum('cts,csd->ctd', grad_mix.astype(jnp.float32), key_f, precision=exact_mode)
    outputs = out_loc + out_in
    grad_query = (query_loc + query_in).astype(jnp.bfloat16)
    level_zero = (jnp.arange(NL) == 0).astype(jnp.float32)
    grad_level = level_in + level_zero[:, None, None] * intra[None]
    lam_query = lam_start[:, :, :, None] * query_f[None]
    back_local = jnp.einsum('lctd,cte->lcde', lam_query, grad_f, precision=exact_mode)
    backward = fenwick_pull(back_local[:, ::-1], span_log[::-1], span_dead[::-1])[:, ::-1]
    back_sum = lax.optimization_barrier(jnp.sum(backward, axis=0))
    key_in = jnp.einsum('cse,cde->csd', value_f * end_col, back_sum, precision=exact_mode)
    value_in = jnp.einsum('csd,cde->cse', key_f * end_col, back_sum, precision=exact_mode)
    key_loc = jnp.einsum('cts,ctd->csd', grad_mix.astype(jnp.float32), query_f, precision=exact_mode)
    value_loc = jnp.einsum('cts,cte->cse', prob_mix.astype(jnp.float32), grad_f, precision=exact_mode)
    value_grad = value_loc + value_in
    drift = lax.optimization_barrier(jnp.sum(grad_f * outputs, axis=2)) - lax.optimization_barrier(jnp.sum(value_f * value_grad, axis=2))
    return (grad_query, (key_loc + key_in).astype(jnp.bfloat16), value_grad.astype(jnp.bfloat16), grad_level, drift)

def reference(queries, keys, values, out_grad, log_gate, level_weight, doc_start):
    query_all = queries.reshape(SPANS, SPAN, HEAD_COUNT, DK).transpose(2, 0, 1, 3)
    key_all = keys.reshape(SPANS, SPAN, HEAD_COUNT, DK).transpose(2, 0, 1, 3)
    value_all = values.reshape(SPANS, SPAN, HEAD_COUNT, DV).transpose(2, 0, 1, 3)
    grad_all = out_grad.reshape(SPANS, SPAN, HEAD_COUNT, DV).transpose(2, 0, 1, 3)
    gate_all = log_gate.reshape(HEAD_COUNT, SPANS, SPAN)
    start_all = doc_start.reshape(SPANS, SPAN)
    weight_all = level_weight.reshape(NL, HEAD_COUNT, SPANS, SPAN).transpose(1, 0, 2, 3)

    def one_head(inputs):
        query_h, key_h, value_h, grad_h, gate_h, weight_h = inputs
        return head_pass(query_h, key_h, value_h, grad_h, gate_h, weight_h, start_all)
    results = lax.map(one_head, (query_all, key_all, value_all, grad_all, gate_all, weight_all))
    grad_query, grad_key, grad_value, grad_level, drift = results
    grad_queries = grad_query.transpose(1, 2, 0, 3).reshape(TOKEN_COUNT, HEAD_COUNT * DK)
    grad_keys = grad_key.transpose(1, 2, 0, 3).reshape(TOKEN_COUNT, HEAD_COUNT * DK)
    grad_values = grad_value.transpose(1, 2, 0, 3).reshape(TOKEN_COUNT, HEAD_COUNT * DV)
    grad_level_weight = grad_level.transpose(1, 0, 2, 3).reshape(NL, HEAD_COUNT, TOKEN_COUNT)
    drift_term = drift.reshape(HEAD_COUNT, TOKEN_COUNT)
    tail = lax.cumsum(drift_term, axis=1, reverse=True)
    squares = jnp.sum(tail * tail)
    factor = jnp.minimum(1.0, lax.rsqrt(squares / (HEAD_COUNT * TOKEN_COUNT) + 1e-06))
    return (grad_queries, grad_keys, grad_values, grad_level_weight, tail * factor)
```

```python
import functools

import jax
import jax.numpy as jnp
from jax import lax
from jax.experimental import pallas as pl
from jax.experimental.pallas import tpu as pltpu
from jax.sharding import Mesh
from jax.sharding import PartitionSpec as P

SEQ = ("seq_0", "seq_1", "seq_2")
MESH = pl.DeviceIdType.MESH
F32 = jnp.float32
BF16 = jnp.bfloat16
NEG = -1e30

NN = (((1,), (0,)), ((), ()))
NT = (((1,), (1,)), ((), ()))
TN = (((0,), (0,)), ((), ()))


def dot(a, b, dims):
    return lax.dot_general(a, b, dims, preferred_element_type=F32)


def split(a):
    hi = a.astype(BF16)
    return hi, (a - hi.astype(F32)).astype(BF16)


def prefix(a, lane):
    shift = 1
    while shift < a.shape[1]:
        a = a + jnp.where(lane >= shift, pltpu.roll(a, shift, 1), 0.0)
        shift *= 2
    return a


def suffix(a, lane):
    size = a.shape[1]
    shift = 1
    while shift < size:
        a = a + jnp.where(lane < size - shift, pltpu.roll(a, size - shift, 1), 0.0)
        shift *= 2
    return a


def kernel(
    q_in, k_in, v_in, g_in, lg_in, lw_in, ds_in,
    gq_out, gk_out, gv_out, glw_out, glg_out,
    sq, sk, sv, sg, ss, rq, rk, rv, rg, rs,
    qb, kb, vb, gb, vt, gt,
    gates, doc, cum, fs, de, wts, cm, bias, pt, rt,
    gq, gk, gv, gvt, glw, drift, small,
    ys, yr, zs, zr, xs, xr, ein, xin,
    bq, bk, bv, bs,
    a_buf, b_buf,
    in_send, in_recv, y1_send, y1_recv, y2_send, y2_recv, x_send, x_recv,
    out_send, out_recv, last_send, last_recv, a_send, a_recv, b_send, b_recv,
):
    x, y, c, z = (lax.axis_index(n) for n in ("seq_0", "seq_1", "seq_2", "head"))
    other = 1 - c
    chip = x * 4 + y
    group = z * 2 + c

    def remote(src, dst, send, recv, **to):
        return pltpu.make_async_remote_copy(
            src_ref=src, dst_ref=dst, send_sem=send, recv_sem=recv,
            device_id=to, device_id_type=MESH,
        )

    barrier = pltpu.get_barrier_semaphore()
    for step in range(1, 16):
        peer = (chip + step) % 16
        pl.semaphore_signal(
            barrier, inc=1, device_id={"seq_0": peer // 4, "seq_1": peer % 4}, device_id_type=MESH
        )
    for step in range(1, 8):
        peer = (group + step) % 8
        pl.semaphore_signal(
            barrier, inc=1, device_id={"head": peer // 2, "seq_2": peer % 2}, device_id_type=MESH
        )

    q_cols = pl.ds(pl.multiple_of(other * 1024, 1024), 1024)
    v_cols = pl.ds(pl.multiple_of(other * 512, 512), 512)
    own_q = pl.ds(pl.multiple_of(c * 1024, 1024), 1024)
    own_v = pl.ds(pl.multiple_of(c * 512, 512), 512)
    own_rows = pl.ds(pl.multiple_of(c * 128, 128), 128)
    other_rows = pl.ds(pl.multiple_of(other * 128, 128), 128)
    own_heads = pl.ds(pl.multiple_of(c * 8, 8), 8)
    other_heads = pl.ds(pl.multiple_of(other * 8, 8), 8)
    ds_row = jnp.broadcast_to(ds_in[...].astype(F32), (8, 128))
    ss[0:8, :] = lg_in[other_heads, :]
    for level in range(6):
        ss[8 + 8 * level : 16 + 8 * level, :] = lw_in[level, other_heads, :]
    ss[56:64, :] = ds_row
    sk[...] = k_in[:, q_cols].astype(F32)
    sv[...] = v_in[:, v_cols].astype(F32)
    sg[...] = g_in[:, v_cols].astype(F32)
    sq[...] = q_in[:, q_cols].astype(F32)

    pl.semaphore_wait(barrier, 22)
    swaps = [
        remote(src, dst, in_send.at[n], in_recv.at[n], seq_2=other)
        for n, (src, dst) in enumerate(((ss, rs), (sk, rk), (sv, rv), (sg, rg), (sq, rq)))
    ]
    for swap in swaps:
        swap.start()

    kb[own_rows, :] = k_in[:, own_q]
    vb[own_rows, :] = v_in[:, own_v]
    gb[own_rows, :] = g_in[:, own_v]
    qb[own_rows, :] = q_in[:, own_q]
    gates[:, own_rows] = lg_in[own_heads, :]
    for level in range(6):
        wts[level, :, own_rows] = lw_in[level, own_heads, :]
    doc[:, own_rows] = ds_row
    ein[...] = jnp.zeros_like(ein)
    xin[...] = jnp.zeros_like(xin)
    pt[128:256, 0:128] = jnp.zeros((128, 128), BF16)
    rt[128:256, 0:128] = jnp.zeros((128, 128), BF16)

    zero_slab = jnp.zeros((128, 128), F32)
    for level, absent in ((0, y % 2 == 0), (1, y < 2), (2, x == 0)):

        @pl.when(absent)
        def _():
            for pair in range(4):
                zr[pair, level] = zero_slab

    swaps[0].wait_recv()
    gates[:, other_rows] = rs[0:8, :]
    for level in range(6):
        wts[level, :, other_rows] = rs[8 + 8 * level : 16 + 8 * level, :]
    doc[:, other_rows] = rs[56:64, :]
    lane = lax.broadcasted_iota(jnp.int32, (8, 256), 1)
    cum_now = prefix(gates[...], lane)
    reset = prefix(doc[...], lane)
    total = cum_now[:, 255:256]
    reset_total = reset[:, 255:256]
    cum[...] = cum_now
    fs[...] = jnp.where(reset == 0.0, jnp.exp(cum_now), 0.0)
    de[...] = jnp.where(reset == reset_total, jnp.exp(total - cum_now), 0.0)
    decay = jnp.broadcast_to(jnp.where(reset_total == 0.0, jnp.exp(total), 0.0), (8, 128))
    small[...] = decay
    columns = jnp.transpose(
        jnp.concatenate([cum_now, reset, jnp.zeros((112, 256), F32)], axis=0)
    )
    for head in range(8):
        cm[head] = jnp.broadcast_to(columns[:, head : head + 1], (256, 128))
    reset_col = jnp.broadcast_to(columns[:, 8:9], (256, 128))
    for half in range(2):
        reset_row = jnp.broadcast_to(reset[0:1, 128 * half : 128 * half + 128], (256, 128))
        s_pos = lax.broadcasted_iota(jnp.int32, (256, 128), 0)
        t_pos = lax.broadcasted_iota(jnp.int32, (256, 128), 1) + 128 * half
        bias[:, 128 * half : 128 * half + 128] = jnp.where(
            (t_pos >= s_pos) & (reset_col == reset_row), 0.0, NEG
        )

    swaps[1].wait_recv()
    kb[other_rows, :] = rk[...].astype(BF16)
    swaps[2].wait_recv()
    vb[other_rows, :] = rv[...].astype(BF16)
    swaps[3].wait_recv()
    gb[other_rows, :] = rg[...].astype(BF16)
    swaps[4].wait_recv()
    qb[other_rows, :] = rq[...].astype(BF16)

    def head_cols(pair, i):
        return pl.ds(pl.multiple_of(pair * 256 + i * 128, 128), 128)

    def pair_cols(pair):
        return pl.ds(pl.multiple_of(pair * 128, 128), 128)

    def sent(kind, at_y):
        return (True, x > 0, at_y % 2 == 1, at_y >= 2)[kind]

    def y1_copy(pair, kind, at_y):
        rows = 136 if kind == 0 else 128
        return remote(
            ys.at[pair, kind, pl.ds(0, rows)], yr.at[at_y, kind, pl.ds(0, rows)],
            y1_send.at[pair, kind], y1_recv.at[at_y, kind], seq_1=pair,
        )

    def states(pair):
        vt[pair] = jnp.transpose(vb[:, pair_cols(pair)].astype(F32))
        gt[pair] = jnp.transpose(gb[:, pair_cols(pair)].astype(F32))
        for i in range(2):
            head = pl.ds(pair * 2 + i, 1)
            rows = pl.ds(64 * i, 64)
            gate = fs[head, :]
            value_hi, value_lo = split(vt[pair, rows] * de[head, :])
            parts = [split(gt[pair, rows] * (gate * wts[level, head, :])) for level in (5, 3, 4)]
            state = dot(
                jnp.concatenate([value_hi, value_lo], axis=0), kb[:, head_cols(pair, i)], NN
            )
            back = dot(
                jnp.concatenate([p[0] for p in parts] + [p[1] for p in parts], axis=0),
                qb[:, head_cols(pair, i)], NN,
            )
            slabs = [state[0:64] + state[64:128]] + [
                back[64 * n : 64 * n + 64] + back[192 + 64 * n : 256 + 64 * n] for n in range(3)
            ]
            row = small[head, :]

            @pl.when(pair == y)
            def _():
                for kind in range(4):
                    yr[y, kind, rows] = slabs[kind]
                yr[y, 0, 128 + i : 129 + i] = row

            @pl.when(pair != y)
            def _():
                for kind in range(4):
                    ys[pair, kind, rows] = slabs[kind]
                ys[pair, 0, 128 + i : 129 + i] = row

        for kind in range(4):

            @pl.when((pair != y) & sent(kind, y))
            def _():
                y1_copy(pair, kind, y).start()

    def intra(pair):
        for i in range(2):
            number = pair * 2 + i
            head = pl.ds(number, 1)
            rows = pl.ds(64 * i, 64)
            query = qb[:, head_cols(pair, i)]
            key = kb[:, head_cols(pair, i)]
            grad = gb[:, pair_cols(pair)]
            value = vb[:, pair_cols(pair)]
            mine = lax.broadcasted_iota(jnp.int32, (64, 128), 1) // 64 == i
            weight = [wts[level, head, :] for level in range(3)]
            span = lax.broadcasted_iota(jnp.int32, (1, 256), 1) // 64
            cum_row = cum[head, :]
            level_rows = [jnp.zeros((1, 256), F32) for level in range(3)]
            drift_row = jnp.zeros((1, 256), F32)
            for b in range(4):
                low = 0 if b < 2 else 128
                blk = slice(64 * b, 64 * b + 64)
                score = dot(key[blk], query[low:256], NT)
                pair_dot = dot(
                    jnp.where(mine, value[blk], jnp.zeros((64, 128), BF16)), grad[low:256], NT
                )
                col = cm[number, blk, :]
                if low == 0:
                    col = jnp.concatenate([col, col], axis=1)
                decayed = jnp.exp((cum_row[:, low:256] - col) + bias[blk, low:256])
                at = span[:, low:256]
                near = (at == b).astype(jnp.int32), ((at ^ 1) == b).astype(jnp.int32)
                mix = jnp.where(
                    near[0] == 1, weight[0][:, low:256],
                    jnp.where(near[1] == 1, weight[1][:, low:256], weight[2][:, low:256]),
                )
                scored = decayed * score
                joint = jnp.sum(scored * pair_dot, axis=0, keepdims=True)
                prob = (scored * mix).astype(BF16)
                pt[blk, low:256] = prob
                rt[blk, low:256] = (decayed * mix * pair_dot).astype(BF16)
                drifted = jnp.sum(prob.astype(F32) * pair_dot, axis=0, keepdims=True)
                if low:
                    pad = jnp.zeros((1, 128), F32)
                    joint = jnp.concatenate([pad, joint], axis=1)
                    drifted = jnp.concatenate([pad, drifted], axis=1)
                drift_row = drift_row + drifted
                level_rows[0] = level_rows[0] + jnp.where(span == b, joint, 0.0)
                level_rows[1] = level_rows[1] + jnp.where((span ^ 1) == b, joint, 0.0)
                level_rows[2] = level_rows[2] + jnp.where(
                    (span != b) & ((span ^ 1) != b), joint, 0.0
                )
            for level in range(3):
                glw[level, head, :] = level_rows[level]
            drift[head, :] = drift_row
            gvt[pair, rows] = dot(gt[pair, rows].astype(BF16), pt[...], NT)
            gk[:, head_cols(pair, i)] = dot(rt[...], query, NN)
            gq[:, head_cols(pair, i)] = dot(rt[...], key, TN)

    def y2_copy(to_y, kind, src):
        return remote(
            src, zr.at[y, kind], y2_send.at[to_y, kind], y2_recv.at[y, kind], seq_1=to_y
        )

    def y2_source(to_y, kind):
        if kind == 0:
            return yr.at[to_y - 1, 0, pl.ds(0, 128)]
        return zs.at[to_y, kind]

    def hand_back(to_y, kind):
        def go():
            @pl.when(to_y != y)
            def _():
                y2_copy(to_y, kind, y2_source(to_y, kind)).start()

            @pl.when(to_y == y)
            def _():
                zr[y, kind] = y2_source(to_y, kind)[...]

        if kind == 2:
            pl.when(x > 0)(go)
        else:
            go()

    def y1_wait(kind):
        for at_y in range(4):
            here = sent(kind, at_y)
            if here is False:
                continue

            @pl.when((y != at_y) & here)
            def _():
                y1_copy(y, kind, at_y).wait_recv()

    def x_copy(to_x, kind):
        return remote(xs.at[kind], xr.at[x], x_send.at[to_x], x_recv.at[x], seq_0=to_x)

    def combine_first():
        y1_wait(0)
        y1_wait(1)
        for i in range(2):
            rows = slice(64 * i, 64 * i + 64)
            dec = [yr[n, 0, 128 + i : 129 + i] for n in range(4)]
            both = dec[1] * yr[0, 0, rows] + yr[1, 0, rows]
            zs[2, 1, rows] = both
            after = dec[2] * both
            zs[3, 1, rows] = after
            xs[0, rows] = dec[3] * (after + yr[2, 0, rows]) + yr[3, 0, rows]
            all_decay = dec[0] * dec[1] * (dec[2] * dec[3])
            xs[0, 128 + i : 129 + i] = all_decay
            xs[1, 128 + i : 129 + i] = all_decay

            @pl.when(x > 0)
            def _():
                back = yr[2, 1, rows] + dec[2] * yr[3, 1, rows]
                back = yr[1, 1, rows] + dec[1] * back
                xs[1, rows] = yr[0, 1, rows] + dec[0] * back

        for to_x in range(4):

            @pl.when(to_x > x)
            def _():
                x_copy(to_x, 0).start()

            @pl.when(to_x < x)
            def _():
                x_copy(to_x, 1).start()

        hand_back(1, 0)
        hand_back(3, 0)
        hand_back(2, 1)
        hand_back(3, 1)

    def combine_second():
        y1_wait(2)
        y1_wait(3)

        def take(at_x, acc):
            remote(
                xs.at[0], xr.at[at_x], x_send.at[at_x], x_recv.at[at_x], seq_0=at_x
            ).wait_recv()
            for i in range(2):
                rows = slice(64 * i, 64 * i + 64)
                acc[rows] = xr[at_x, 128 + i : 129 + i] * acc[rows] + xr[at_x, rows]

        for at_x in range(4):
            pl.when(at_x < x)(functools.partial(take, at_x, ein))
        for at_x in range(3, -1, -1):
            pl.when(at_x > x)(functools.partial(take, at_x, xin))
        for i in range(2):
            rows = slice(64 * i, 64 * i + 64)
            dec = [yr[n, 0, 128 + i : 129 + i] for n in range(4)]
            into = ein[rows]
            for at_y in range(4):
                zs[at_y, 2, rows] = into
                into = dec[at_y] * into
            late = xin[rows]
            zs[3, 3, rows] = late
            late = dec[3] * late
            zs[2, 3, rows] = late + yr[3, 2, rows]
            late = dec[2] * late + (yr[2, 3, rows] + dec[2] * yr[3, 3, rows])
            zs[1, 3, rows] = late
            zs[0, 3, rows] = dec[1] * late + yr[1, 2, rows]
        for at_y in range(4):
            hand_back(at_y, 2)
            hand_back(at_y, 3)

    def back_copy(pair, kind):
        if kind == 2:
            cols, src, dst = pair_cols(pair), gv, bv
        else:
            cols = pl.ds(pl.multiple_of(pair * 256, 256), 256)
            src, dst = ((gq, bq), (gk, bk))[kind]
        return remote(
            src.at[other_rows, cols], dst.at[:, cols],
            out_send.at[pair, kind], out_recv.at[pair, kind], seq_2=other,
        )

    def cross(pair):
        for kind in range(4):
            here = (y % 2 == 1, y >= 2, x > 0, True)[kind]

            @pl.when((pair != y) & here)
            def _():
                remote(
                    zs.at[0, kind], zr.at[pair, kind], y2_send.at[0, kind],
                    y2_recv.at[pair, kind], seq_1=pair,
                ).wait_recv()

        for i in range(2):
            number = pair * 2 + i
            head = pl.ds(number, 1)
            rows = pl.ds(64 * i, 64)
            query = qb[:, head_cols(pair, i)]
            key = kb[:, head_cols(pair, i)]
            grad = gt[pair, rows]
            value = vt[pair, rows]
            gate = fs[head, :]
            end = de[head, :]
            weight = [wts[level, head, :] for level in (3, 4, 5)]
            enter = jnp.concatenate([zr[pair, n, rows] for n in range(3)], axis=0)
            enter_hi, enter_lo = split(enter)
            mixed = dot(jnp.concatenate([enter_hi, enter_lo], axis=0), query, NT)
            drift_row = drift[head, :]
            for n in range(3):
                state_row = mixed[64 * n : 64 * n + 64] + mixed[192 + 64 * n : 256 + 64 * n]
                level_row = gate * jnp.sum(state_row * grad, axis=0, keepdims=True)
                glw[3 + n, head, :] = level_row
                drift_row = drift_row + weight[n] * level_row
            weighted_hi, weighted_lo = split(
                jnp.concatenate([grad * (gate * weight[n]) for n in range(3)], axis=0)
            )
            gq[:, head_cols(pair, i)] = gq[:, head_cols(pair, i)] + dot(
                jnp.concatenate([weighted_hi, weighted_lo, weighted_hi], axis=0),
                jnp.concatenate([enter_hi, enter_hi, enter_lo], axis=0), TN,
            )
            leave_hi, leave_lo = split(zr[pair, 3, rows])
            left = dot(jnp.concatenate([leave_hi, leave_lo], axis=0), key, NT)
            value_grad = gvt[pair, rows] + end * (left[0:64] + left[64:128])
            gvt[pair, rows] = value_grad
            drift[head, :] = drift_row - jnp.sum(value * value_grad, axis=0, keepdims=True)
            ended_hi, ended_lo = split(value * end)
            gk[:, head_cols(pair, i)] = gk[:, head_cols(pair, i)] + dot(
                jnp.concatenate([ended_hi, ended_lo, ended_hi], axis=0),
                jnp.concatenate([leave_hi, leave_hi, leave_lo], axis=0), TN,
            )
        gv[:, pair_cols(pair)] = jnp.transpose(gvt[pair])
        for kind in range(3):
            back_copy(pair, kind).start()
        wide = pl.ds(pl.multiple_of(pair * 256, 256), 256)
        out_wide = pl.ds(pl.multiple_of(c * 1024 + pair * 256, 256), 256)
        out_narrow = pl.ds(pl.multiple_of(c * 512 + pair * 128, 128), 128)
        gq_out[:, out_wide] = gq[own_rows, wide].astype(BF16)
        gk_out[:, out_wide] = gk[own_rows, wide].astype(BF16)
        gv_out[:, out_narrow] = gv[own_rows, pair_cols(pair)].astype(BF16)

    def loop(low, high, body):
        def step(n, carry):
            body(n)
            return carry

        lax.fori_loop(low, high, step, 0)

    loop(0, 4, states)
    loop(0, 2, intra)
    combine_first()
    loop(2, 4, intra)
    combine_second()
    loop(0, 4, cross)

    lane = lax.broadcasted_iota(jnp.int32, (8, 256), 1)
    tail = suffix(drift[...], lane)
    drift[...] = tail
    bs_out = remote(small.at[:, :], bs.at[pl.ds(48, 8), :], last_send.at[1], last_recv.at[1], seq_2=other)
    tile = lax.broadcasted_iota(jnp.int32, (8, 128), 1)
    head_total = jnp.broadcast_to(tail[:, 0:1], (8, 128))
    head_square = jnp.broadcast_to(jnp.sum(tail * tail, axis=1, keepdims=True), (8, 128))
    head_sum = jnp.broadcast_to(jnp.sum(tail, axis=1, keepdims=True), (8, 128))
    a_buf[chip] = jnp.where(tile == 0, head_total, jnp.where(tile == 1, head_square, head_sum))

    def a_copy(step):
        peer = (chip + step) % 16
        return remote(
            a_buf.at[chip], a_buf.at[chip], a_send.at[peer], a_recv.at[chip],
            seq_0=peer // 4, seq_1=peer % 4,
        )

    for step in range(1, 16):
        a_copy(step).start()
    small[...] = drift[:, other_rows]
    for level in range(6):
        ss_rows = slice(8 * level, 8 * level + 8)
        ys[y, 1, ss_rows] = glw[level, :, other_rows]
    glw_copy = remote(
        ys.at[y, 1, pl.ds(0, 48)], bs.at[pl.ds(0, 48), :], last_send.at[0], last_recv.at[0],
        seq_2=other,
    )
    glw_copy.start()
    bs_out.start()
    for level in range(6):
        glw_out[level, own_heads, :] = glw[level, :, own_rows]

    for pair in range(4):
        for kind in range(3):
            back_copy(pair, kind).wait_recv()
    other_q = pl.ds(pl.multiple_of(other * 1024, 1024), 1024)
    other_v = pl.ds(pl.multiple_of(other * 512, 512), 512)
    gq_out[:, other_q] = bq[...].astype(BF16)
    gk_out[:, other_q] = bk[...].astype(BF16)
    gv_out[:, other_v] = bv[...].astype(BF16)
    glw_copy.wait_recv()
    for level in range(6):
        glw_out[level, other_heads, :] = bs[8 * level : 8 * level + 8, :]

    for step in range(1, 16):
        peer = (chip + step) % 16
        remote(
            a_buf.at[chip], a_buf.at[peer], a_send.at[peer], a_recv.at[peer],
            seq_0=peer // 4, seq_1=peer % 4,
        ).wait_recv()
    run = jnp.zeros((8, 1), F32)
    later = jnp.zeros((8, 1), F32)
    squares = jnp.zeros((8, 1), F32)
    for at in range(15, -1, -1):
        now = a_buf[at]
        later = later + run * (chip == at).astype(F32)
        squares = squares + now[:, 1:2] + run * (2.0 * now[:, 2:3] + 256.0 * run)
        run = run + now[:, 0:1]
    whole = jnp.broadcast_to(jnp.sum(squares, axis=0, keepdims=True), (8, 128))
    b_buf[group] = jnp.where(tile < 64, jnp.broadcast_to(later, (8, 128)), whole)

    def b_peer(step):
        peer = (group + step) % 8
        return peer, {"head": peer // 2, "seq_2": peer % 2}

    for step in range(1, 8):
        peer, to = b_peer(step)
        remote(
            b_buf.at[group], b_buf.at[group], b_send.at[peer], b_recv.at[group], **to
        ).start()
    for step in range(1, 8):
        peer, to = b_peer(step)
        remote(
            b_buf.at[group], b_buf.at[peer], b_send.at[peer], b_recv.at[peer], **to
        ).wait_recv()
    total_square = jnp.zeros((8, 128), F32)
    for at in range(8):
        total_square = total_square + b_buf[at]
    factor = jnp.minimum(1.0, lax.rsqrt(total_square[:, 64:65] / (64 * 4096) + 1e-06))
    glg_out[own_heads, :] = (drift[:, own_rows] + later) * factor
    bs_out.wait_recv()
    glg_out[other_heads, :] = (bs[48:56, :] + b_buf[z * 2 + other][:, 0:1]) * factor

    for swap in swaps:
        swap.wait_send()
    for pair in range(4):
        for kind in range(4):

            @pl.when((y != pair) & sent(kind, y))
            def _():
                y1_copy(pair, kind, y).wait_send()

            back = (pair % 2 == 1, pair >= 2, x > 0, True)[kind]
            if back is not False:

                @pl.when((y != pair) & back)
                def _():
                    y2_copy(pair, kind, y2_source(pair, kind)).wait_send()

        @pl.when(pair != x)
        def _():
            x_copy(pair, 0).wait_send()

        for kind in range(3):
            back_copy(pair, kind).wait_send()
    glw_copy.wait_send()
    bs_out.wait_send()
    for step in range(1, 16):
        a_copy(step).wait_send()
    for step in range(1, 8):
        peer, to = b_peer(step)
        remote(
            b_buf.at[group], b_buf.at[group], b_send.at[peer], b_recv.at[group], **to
        ).wait_send()


def shards(queries, keys, values, out_grad, log_gate, level_weight, doc_start):
    vmem = pl.BlockSpec(memory_space=pltpu.VMEM)
    scratch = (
        [(128, 1024), (128, 1024), (128, 512), (128, 512), (64, 128)] * 2
    )
    scratch = [pltpu.VMEM(s, F32) for s in scratch]
    scratch += [pltpu.VMEM(s, BF16) for s in ((256, 1024), (256, 1024), (256, 512), (256, 512))]
    scratch += [pltpu.VMEM((4, 128, 256), F32)] * 2
    scratch += [pltpu.VMEM((8, 256), F32)] * 5
    scratch += [pltpu.VMEM((6, 8, 256), F32), pltpu.VMEM((8, 256, 128), F32)]
    scratch += [pltpu.VMEM((256, 256), F32), pltpu.VMEM((256, 256), BF16), pltpu.VMEM((256, 256), BF16)]
    scratch += [pltpu.VMEM((256, 1024), F32), pltpu.VMEM((256, 1024), F32), pltpu.VMEM((256, 512), F32)]
    scratch += [pltpu.VMEM((4, 128, 256), F32), pltpu.VMEM((6, 8, 256), F32)]
    scratch += [pltpu.VMEM((8, 256), F32), pltpu.VMEM((8, 128), F32)]
    scratch += [pltpu.VMEM((4, 4, 136, 128), F32)] * 2 + [pltpu.VMEM((4, 4, 128, 128), F32)] * 2
    scratch += [pltpu.VMEM((2, 136, 128), F32), pltpu.VMEM((4, 136, 128), F32)]
    scratch += [pltpu.VMEM((128, 128), F32)] * 2
    scratch += [pltpu.VMEM((128, 1024), F32), pltpu.VMEM((128, 1024), F32), pltpu.VMEM((128, 512), F32)]
    scratch += [pltpu.VMEM((56, 128), F32)]
    scratch += [pltpu.VMEM((16, 8, 128), F32), pltpu.VMEM((8, 8, 128), F32)]
    sems = [(5,), (5,), (4, 4), (4, 4), (4, 4), (4, 4), (4,), (4,), (4, 3), (4, 3), (2,), (2,)]
    sems += [(16,), (16,), (8,), (8,)]
    scratch += [pltpu.SemaphoreType.DMA(s) for s in sems]
    return pl.pallas_call(
        kernel,
        out_shape=(
            jax.ShapeDtypeStruct(queries.shape, BF16),
            jax.ShapeDtypeStruct(keys.shape, BF16),
            jax.ShapeDtypeStruct(values.shape, BF16),
            jax.ShapeDtypeStruct(level_weight.shape, F32),
            jax.ShapeDtypeStruct(log_gate.shape, F32),
        ),
        in_specs=[vmem] * 7,
        out_specs=[vmem] * 5,
        scratch_shapes=scratch,
        compiler_params=pltpu.CompilerParams(
            collective_id=0, has_side_effects=True, vmem_limit_bytes=56 * 2**20
        ),
    )(queries, keys, values, out_grad, log_gate, level_weight, doc_start.reshape(1, -1))


def solution(mesh):
    finer = Mesh(
        mesh.devices.reshape(4, 4, 2, mesh.shape["head"]), ("seq_0", "seq_1", "seq_2", "head")
    )
    wide = P(SEQ, "head")
    return jax.shard_map(
        shards,
        mesh=finer,
        in_specs=(wide, wide, wide, wide, P("head", SEQ), P(None, "head", SEQ), P(SEQ)),
        out_specs=(wide, wide, wide, P(None, "head", SEQ), P("head", SEQ)),
        check_vma=False,
    )
```

```python
import functools

import jax
import jax.numpy as jnp
from jax import lax
from jax.experimental import pallas as pl
from jax.experimental.pallas import tpu as pltpu
from jax.sharding import Mesh
from jax.sharding import PartitionSpec as P

SEQ = ("seq_0", "seq_1", "seq_2")
MESH = pl.DeviceIdType.MESH
F32 = jnp.float32
BF16 = jnp.bfloat16
NEG = -1e30

NN = (((1,), (0,)), ((), ()))
NT = (((1,), (1,)), ((), ()))
TN = (((0,), (0,)), ((), ()))


def dot(a, b, dims):
    return lax.dot_general(a, b, dims, preferred_element_type=F32)


def split(a):
    hi = a.astype(BF16)
    return hi, (a - hi.astype(F32)).astype(BF16)


def prefix(a, lane):
    shift = 1
    while shift < a.shape[1]:
        a = a + jnp.where(lane >= shift, pltpu.roll(a, shift, 1), 0.0)
        shift *= 2
    return a


def suffix(a, lane):
    size = a.shape[1]
    shift = 1
    while shift < size:
        a = a + jnp.where(lane < size - shift, pltpu.roll(a, size - shift, 1), 0.0)
        shift *= 2
    return a


def kernel(
    q_hbm, k_hbm, v_hbm, g_hbm, lg_hbm, lw_hbm, ds_hbm,
    gq_hbm, gk_hbm, gv_hbm, glw_hbm, glg_hbm,
    q_in, k_in, v_in, g_in, lg_in, lw_in, ds_in,
    gq_out, gk_out, gv_out, glw_out, glg_out, load_sem, store_sem,
    sq, sk, sv, sg, ss, rq, rk, rv, rg, rs,
    qb, kb, vb, gb, vt, gt,
    gates, doc, cum, fs, de, wts, cm, bias, pt, rt,
    gq, gk, gv, gvt, glw, drift, small,
    ys, yr, zs, zr, xs, xr, ein, xin,
    bq, bk, bv, bs,
    a_buf, b_buf,
    in_send, in_recv, y1_send, y1_recv, y2_send, y2_recv, x_send, x_recv,
    out_send, out_recv, last_send, last_recv, a_send, a_recv, b_send, b_recv,
):
    x, y, c, z = (lax.axis_index(n) for n in ("seq_0", "seq_1", "seq_2", "head"))
    other = 1 - c
    chip = x * 4 + y
    group = z * 2 + c

    def remote(src, dst, send, recv, **to):
        return pltpu.make_async_remote_copy(
            src_ref=src, dst_ref=dst, send_sem=send, recv_sem=recv,
            device_id=to, device_id_type=MESH,
        )

    loads = [
        pltpu.make_async_copy(src, dst, load_sem.at[n])
        for n, (src, dst) in enumerate((
            (ds_hbm, ds_in), (lg_hbm, lg_in), (lw_hbm, lw_in), (k_hbm, k_in),
            (v_hbm, v_in), (g_hbm, g_in), (q_hbm, q_in),
        ))
    ]
    for load in loads:
        load.start()

    barrier = pltpu.get_barrier_semaphore()
    for step in range(1, 16):
        peer = (chip + step) % 16
        pl.semaphore_signal(
            barrier, inc=1, device_id={"seq_0": peer // 4, "seq_1": peer % 4}, device_id_type=MESH
        )
    for step in range(1, 8):
        peer = (group + step) % 8
        pl.semaphore_signal(
            barrier, inc=1, device_id={"head": peer // 2, "seq_2": peer % 2}, device_id_type=MESH
        )

    q_cols = pl.ds(pl.multiple_of(other * 1024, 1024), 1024)
    v_cols = pl.ds(pl.multiple_of(other * 512, 512), 512)
    own_q = pl.ds(pl.multiple_of(c * 1024, 1024), 1024)
    own_v = pl.ds(pl.multiple_of(c * 512, 512), 512)
    own_rows = pl.ds(pl.multiple_of(c * 128, 128), 128)
    other_rows = pl.ds(pl.multiple_of(other * 128, 128), 128)
    own_heads = pl.ds(pl.multiple_of(c * 8, 8), 8)
    other_heads = pl.ds(pl.multiple_of(other * 8, 8), 8)
    for load in loads[:3]:
        load.wait()
    ds_row = jnp.broadcast_to(ds_in[...].astype(F32), (8, 128))
    ss[0:8, :] = lg_in[other_heads, :]
    for level in range(6):
        ss[8 + 8 * level : 16 + 8 * level, :] = lw_in[level, other_heads, :]
    ss[56:64, :] = ds_row
    loads[3].wait()
    sk[...] = k_in[:, q_cols].astype(F32)
    loads[4].wait()
    sv[...] = v_in[:, v_cols].astype(F32)
    loads[5].wait()
    sg[...] = g_in[:, v_cols].astype(F32)
    loads[6].wait()
    sq[...] = q_in[:, q_cols].astype(F32)

    pl.semaphore_wait(barrier, 22)
    swaps = [
        remote(src, dst, in_send.at[n], in_recv.at[n], seq_2=other)
        for n, (src, dst) in enumerate(((ss, rs), (sk, rk), (sv, rv), (sg, rg), (sq, rq)))
    ]
    for swap in swaps:
        swap.start()

    kb[own_rows, :] = k_in[:, own_q]
    vb[own_rows, :] = v_in[:, own_v]
    gb[own_rows, :] = g_in[:, own_v]
    qb[own_rows, :] = q_in[:, own_q]
    gates[:, own_rows] = lg_in[own_heads, :]
    for level in range(6):
        wts[level, :, own_rows] = lw_in[level, own_heads, :]
    doc[:, own_rows] = ds_row
    ein[...] = jnp.zeros_like(ein)
    xin[...] = jnp.zeros_like(xin)
    pt[128:256, 0:128] = jnp.zeros((128, 128), BF16)
    rt[128:256, 0:128] = jnp.zeros((128, 128), BF16)

    zero_slab = jnp.zeros((128, 128), F32)
    for level, absent in ((0, y % 2 == 0), (1, y < 2), (2, x == 0)):

        @pl.when(absent)
        def _():
            for pair in range(4):
                zr[pair, level] = zero_slab

    swaps[0].wait_recv()
    gates[:, other_rows] = rs[0:8, :]
    for level in range(6):
        wts[level, :, other_rows] = rs[8 + 8 * level : 16 + 8 * level, :]
    doc[:, other_rows] = rs[56:64, :]
    lane = lax.broadcasted_iota(jnp.int32, (8, 256), 1)
    cum_now = prefix(gates[...], lane)
    reset = prefix(doc[...], lane)
    total = cum_now[:, 255:256]
    reset_total = reset[:, 255:256]
    cum[...] = cum_now
    fs[...] = jnp.where(reset == 0.0, jnp.exp(cum_now), 0.0)
    de[...] = jnp.where(reset == reset_total, jnp.exp(total - cum_now), 0.0)
    decay = jnp.broadcast_to(jnp.where(reset_total == 0.0, jnp.exp(total), 0.0), (8, 128))
    small[...] = decay
    columns = jnp.transpose(
        jnp.concatenate([cum_now, reset, jnp.zeros((112, 256), F32)], axis=0)
    )
    for head in range(8):
        cm[head] = jnp.broadcast_to(columns[:, head : head + 1], (256, 128))
    reset_col = jnp.broadcast_to(columns[:, 8:9], (256, 128))
    for half in range(2):
        reset_row = jnp.broadcast_to(reset[0:1, 128 * half : 128 * half + 128], (256, 128))
        s_pos = lax.broadcasted_iota(jnp.int32, (256, 128), 0)
        t_pos = lax.broadcasted_iota(jnp.int32, (256, 128), 1) + 128 * half
        bias[:, 128 * half : 128 * half + 128] = jnp.where(
            (t_pos >= s_pos) & (reset_col == reset_row), 0.0, NEG
        )

    swaps[1].wait_recv()
    kb[other_rows, :] = rk[...].astype(BF16)
    swaps[2].wait_recv()
    vb[other_rows, :] = rv[...].astype(BF16)
    swaps[3].wait_recv()
    gb[other_rows, :] = rg[...].astype(BF16)
    swaps[4].wait_recv()
    qb[other_rows, :] = rq[...].astype(BF16)

    def head_cols(pair, i):
        return pl.ds(pl.multiple_of(pair * 256 + i * 128, 128), 128)

    def pair_cols(pair):
        return pl.ds(pl.multiple_of(pair * 128, 128), 128)

    def sent(kind, at_y):
        return (True, x > 0, at_y % 2 == 1, at_y >= 2)[kind]

    def y1_copy(pair, kind, at_y):
        rows = 136 if kind == 0 else 128
        return remote(
            ys.at[pair, kind, pl.ds(0, rows)], yr.at[at_y, kind, pl.ds(0, rows)],
            y1_send.at[pair, kind], y1_recv.at[at_y, kind], seq_1=pair,
        )

    def place(pair, kind, i, slab):
        rows = pl.ds(64 * i, 64)

        @pl.when(pair == y)
        def _():
            yr[y, kind, rows] = slab

        @pl.when(pair != y)
        def _():
            ys[pair, kind, rows] = slab

    def hand_over(pair, kind):
        @pl.when((pair != y) & sent(kind, y))
        def _():
            y1_copy(pair, kind, y).start()

    def state_fwd(pair):
        vt[pair] = jnp.transpose(vb[:, pair_cols(pair)].astype(F32))
        for i in range(2):
            head = pl.ds(pair * 2 + i, 1)
            value_hi, value_lo = split(vt[pair, pl.ds(64 * i, 64)] * de[head, :])
            state = dot(
                jnp.concatenate([value_hi, value_lo], axis=0), kb[:, head_cols(pair, i)], NN
            )
            place(pair, 0, i, state[0:64] + state[64:128])
            row = small[head, :]

            @pl.when(pair == y)
            def _():
                yr[y, 0, 128 + i : 129 + i] = row

            @pl.when(pair != y)
            def _():
                ys[pair, 0, 128 + i : 129 + i] = row

        hand_over(pair, 0)

    def state_back(pair):
        gt[pair] = jnp.transpose(gb[:, pair_cols(pair)].astype(F32))
        for i in range(2):
            head = pl.ds(pair * 2 + i, 1)
            hi, lo = split(gt[pair, pl.ds(64 * i, 64)] * (fs[head, :] * wts[5, head, :]))
            back = dot(jnp.concatenate([hi, lo], axis=0), qb[:, head_cols(pair, i)], NN)
            place(pair, 1, i, back[0:64] + back[64:128])
        hand_over(pair, 1)

    def state_near(pair):
        for i in range(2):
            head = pl.ds(pair * 2 + i, 1)
            grad = gt[pair, pl.ds(64 * i, 64)]
            parts = [split(grad * (fs[head, :] * wts[level, head, :])) for level in (3, 4)]
            back = dot(
                jnp.concatenate([p[0] for p in parts] + [p[1] for p in parts], axis=0),
                qb[:, head_cols(pair, i)], NN,
            )
            for n in range(2):
                place(
                    pair, 2 + n, i, back[64 * n : 64 * n + 64] + back[128 + 64 * n : 192 + 64 * n]
                )
        hand_over(pair, 2)
        hand_over(pair, 3)

    def intra(pair):
        for i in range(2):
            number = pair * 2 + i
            head = pl.ds(number, 1)
            rows = pl.ds(64 * i, 64)
            query = qb[:, head_cols(pair, i)]
            key = kb[:, head_cols(pair, i)]
            grad = gb[:, pair_cols(pair)]
            value = vb[:, pair_cols(pair)]
            mine = lax.broadcasted_iota(jnp.int32, (64, 128), 1) // 64 == i
            weight = [wts[level, head, :] for level in range(3)]
            span = lax.broadcasted_iota(jnp.int32, (1, 256), 1) // 64
            cum_row = cum[head, :]
            level_rows = [jnp.zeros((1, 256), F32) for level in range(3)]
            drift_row = jnp.zeros((1, 256), F32)
            for b in range(4):
                low = 0 if b < 2 else 128
                blk = slice(64 * b, 64 * b + 64)
                score = dot(key[blk], query[low:256], NT)
                pair_dot = dot(
                    jnp.where(mine, value[blk], jnp.zeros((64, 128), BF16)), grad[low:256], NT
                )
                col = cm[number, blk, :]
                if low == 0:
                    col = jnp.concatenate([col, col], axis=1)
                decayed = jnp.exp((cum_row[:, low:256] - col) + bias[blk, low:256])
                at = span[:, low:256]
                near = (at == b).astype(jnp.int32), ((at ^ 1) == b).astype(jnp.int32)
                mix = jnp.where(
                    near[0] == 1, weight[0][:, low:256],
                    jnp.where(near[1] == 1, weight[1][:, low:256], weight[2][:, low:256]),
                )
                scored = decayed * score
                joint = jnp.sum(scored * pair_dot, axis=0, keepdims=True)
                prob = (scored * mix).astype(BF16)
                pt[blk, low:256] = prob
                rt[blk, low:256] = (decayed * mix * pair_dot).astype(BF16)
                drifted = jnp.sum(prob.astype(F32) * pair_dot, axis=0, keepdims=True)
                if low:
                    pad = jnp.zeros((1, 128), F32)
                    joint = jnp.concatenate([pad, joint], axis=1)
                    drifted = jnp.concatenate([pad, drifted], axis=1)
                drift_row = drift_row + drifted
                level_rows[0] = level_rows[0] + jnp.where(span == b, joint, 0.0)
                level_rows[1] = level_rows[1] + jnp.where((span ^ 1) == b, joint, 0.0)
                level_rows[2] = level_rows[2] + jnp.where(
                    (span != b) & ((span ^ 1) != b), joint, 0.0
                )
            for level in range(3):
                glw[level, head, :] = level_rows[level]
            drift[head, :] = drift_row
            gvt[pair, rows] = dot(gt[pair, rows].astype(BF16), pt[...], NT)
            gk[:, head_cols(pair, i)] = dot(rt[...], query, NN)
            gq[:, head_cols(pair, i)] = dot(rt[...], key, TN)

    def y2_copy(to_y, kind, src):
        return remote(
            src, zr.at[y, kind], y2_send.at[to_y, kind], y2_recv.at[y, kind], seq_1=to_y
        )

    def y2_source(to_y, kind):
        if kind == 0:
            return yr.at[to_y - 1, 0, pl.ds(0, 128)]
        return zs.at[to_y, kind]

    def hand_back(to_y, kind):
        def go():
            @pl.when(to_y != y)
            def _():
                y2_copy(to_y, kind, y2_source(to_y, kind)).start()

            @pl.when(to_y == y)
            def _():
                zr[y, kind] = y2_source(to_y, kind)[...]

        if kind == 2:
            pl.when(x > 0)(go)
        else:
            go()

    def y1_wait(kind):
        for at_y in range(4):
            here = sent(kind, at_y)
            if here is False:
                continue

            @pl.when((y != at_y) & here)
            def _():
                y1_copy(y, kind, at_y).wait_recv()

    def x_copy(to_x, kind):
        return remote(xs.at[kind], xr.at[x], x_send.at[to_x], x_recv.at[x], seq_0=to_x)

    def decays(i):
        return [yr[n, 0, 128 + i : 129 + i] for n in range(4)]

    def combine_fwd():
        y1_wait(0)
        for i in range(2):
            rows = slice(64 * i, 64 * i + 64)
            dec = decays(i)
            both = dec[1] * yr[0, 0, rows] + yr[1, 0, rows]
            zs[2, 1, rows] = both
            after = dec[2] * both
            zs[3, 1, rows] = after
            xs[0, rows] = dec[3] * (after + yr[2, 0, rows]) + yr[3, 0, rows]
            all_decay = dec[0] * dec[1] * (dec[2] * dec[3])
            xs[0, 128 + i : 129 + i] = all_decay
            xs[1, 128 + i : 129 + i] = all_decay
        for to_x in range(4):

            @pl.when(to_x > x)
            def _():
                x_copy(to_x, 0).start()

    def combine_back():
        y1_wait(1)

        @pl.when(x > 0)
        def _():
            for i in range(2):
                rows = slice(64 * i, 64 * i + 64)
                dec = decays(i)
                back = yr[2, 1, rows] + dec[2] * yr[3, 1, rows]
                back = yr[1, 1, rows] + dec[1] * back
                xs[1, rows] = yr[0, 1, rows] + dec[0] * back

        for to_x in range(4):

            @pl.when(to_x < x)
            def _():
                x_copy(to_x, 1).start()

        hand_back(1, 0)
        hand_back(3, 0)
        hand_back(2, 1)
        hand_back(3, 1)

    def take(acc, at_x):
        remote(
            xs.at[0], xr.at[at_x], x_send.at[at_x], x_recv.at[at_x], seq_0=at_x
        ).wait_recv()
        for i in range(2):
            rows = slice(64 * i, 64 * i + 64)
            acc[rows] = xr[at_x, 128 + i : 129 + i] * acc[rows] + xr[at_x, rows]

    def enter_far():
        for at_x in range(4):
            pl.when(at_x < x)(functools.partial(take, ein, at_x))
        for i in range(2):
            rows = slice(64 * i, 64 * i + 64)
            dec = decays(i)
            into = ein[rows]
            for at_y in range(4):
                zs[at_y, 2, rows] = into
                into = dec[at_y] * into
        for at_y in range(4):
            hand_back(at_y, 2)

    def leave_far():
        y1_wait(2)
        y1_wait(3)
        for at_x in range(3, -1, -1):
            pl.when(at_x > x)(functools.partial(take, xin, at_x))
        for i in range(2):
            rows = slice(64 * i, 64 * i + 64)
            dec = decays(i)
            late = xin[rows]
            zs[3, 3, rows] = late
            late = dec[3] * late
            zs[2, 3, rows] = late + yr[3, 2, rows]
            late = dec[2] * late + (yr[2, 3, rows] + dec[2] * yr[3, 3, rows])
            zs[1, 3, rows] = late
            zs[0, 3, rows] = dec[1] * late + yr[1, 2, rows]
        for at_y in range(4):
            hand_back(at_y, 3)

    def back_copy(pair, kind):
        if kind == 2:
            cols, src, dst = pair_cols(pair), gv, bv
        else:
            cols = pl.ds(pl.multiple_of(pair * 256, 256), 256)
            src, dst = ((gq, bq), (gk, bk))[kind]
        return remote(
            src.at[other_rows, cols], dst.at[:, cols],
            out_send.at[pair, kind], out_recv.at[pair, kind], seq_2=other,
        )

    def cross(pair):
        for kind in range(4):
            here = (y % 2 == 1, y >= 2, x > 0, True)[kind]

            @pl.when((pair != y) & here)
            def _():
                remote(
                    zs.at[0, kind], zr.at[pair, kind], y2_send.at[0, kind],
                    y2_recv.at[pair, kind], seq_1=pair,
                ).wait_recv()

        for i in range(2):
            head = pl.ds(pair * 2 + i, 1)
            rows = pl.ds(64 * i, 64)
            grad = gt[pair, rows]
            value = vt[pair, rows]
            enter_hi, enter_lo = split(
                jnp.concatenate([zr[pair, n, rows] for n in range(3)], axis=0)
            )
            mixed = dot(
                jnp.concatenate([enter_hi, enter_lo], axis=0), qb[:, head_cols(pair, i)], NT
            )
            drift_row = drift[head, :]
            for n in range(3):
                state_row = mixed[64 * n : 64 * n + 64] + mixed[192 + 64 * n : 256 + 64 * n]
                level_row = fs[head, :] * jnp.sum(state_row * grad, axis=0, keepdims=True)
                glw[3 + n, head, :] = level_row
                drift_row = drift_row + wts[3 + n, head, :] * level_row
            leave_hi, leave_lo = split(zr[pair, 3, rows])
            left = dot(
                jnp.concatenate([leave_hi, leave_lo], axis=0), kb[:, head_cols(pair, i)], NT
            )
            value_grad = gvt[pair, rows] + de[head, :] * (left[0:64] + left[64:128])
            gvt[pair, rows] = value_grad
            drift[head, :] = drift_row - jnp.sum(value * value_grad, axis=0, keepdims=True)

    def cross_grad(pair):
        for i in range(2):
            head = pl.ds(pair * 2 + i, 1)
            rows = pl.ds(64 * i, 64)
            enter_hi, enter_lo = split(
                jnp.concatenate([zr[pair, n, rows] for n in range(3)], axis=0)
            )
            grad = gt[pair, rows]
            weighted_hi, weighted_lo = split(
                jnp.concatenate(
                    [grad * (fs[head, :] * wts[3 + n, head, :]) for n in range(3)], axis=0
                )
            )
            gq[:, head_cols(pair, i)] = gq[:, head_cols(pair, i)] + dot(
                jnp.concatenate([weighted_hi, weighted_lo, weighted_hi], axis=0),
                jnp.concatenate([enter_hi, enter_hi, enter_lo], axis=0), TN,
            )
            leave_hi, leave_lo = split(zr[pair, 3, rows])
            ended_hi, ended_lo = split(vt[pair, rows] * de[head, :])
            gk[:, head_cols(pair, i)] = gk[:, head_cols(pair, i)] + dot(
                jnp.concatenate([ended_hi, ended_lo, ended_hi], axis=0),
                jnp.concatenate([leave_hi, leave_hi, leave_lo], axis=0), TN,
            )
        gv[:, pair_cols(pair)] = jnp.transpose(gvt[pair])
        for kind in range(3):
            back_copy(pair, kind).start()
        wide = pl.ds(pl.multiple_of(pair * 256, 256), 256)
        out_wide = pl.ds(pl.multiple_of(c * 1024 + pair * 256, 256), 256)
        out_narrow = pl.ds(pl.multiple_of(c * 512 + pair * 128, 128), 128)
        gq_out[:, out_wide] = gq[own_rows, wide].astype(BF16)
        gk_out[:, out_wide] = gk[own_rows, wide].astype(BF16)
        gv_out[:, out_narrow] = gv[own_rows, pair_cols(pair)].astype(BF16)

    def loop(low, high, body):
        def step(n, carry):
            body(n)
            return carry

        lax.fori_loop(low, high, step, 0)

    def toward(n):
        return (y + jnp.where(n == 2, 3, jnp.where(n == 3, 0, 2 - n))) % 4

    def nearby(n):
        return (y + jnp.where(n == 2, 3, jnp.where(n == 3, 2, n))) % 4

    loop(0, 4, lambda n: state_fwd(toward(n)))
    loop(0, 4, lambda n: state_back(toward(n)))
    loop(0, 4, lambda n: state_near(toward(n)))
    loop(0, 2, intra)
    combine_fwd()
    loop(2, 3, intra)
    combine_back()
    loop(3, 4, intra)
    enter_far()
    leave_far()
    loop(0, 4, lambda n: cross(nearby(n)))
    lane = lax.broadcasted_iota(jnp.int32, (8, 256), 1)
    tail = suffix(drift[...], lane)
    drift[...] = tail
    bs_out = remote(small.at[:, :], bs.at[pl.ds(48, 8), :], last_send.at[1], last_recv.at[1], seq_2=other)
    tile = lax.broadcasted_iota(jnp.int32, (8, 128), 1)
    head_total = jnp.broadcast_to(tail[:, 0:1], (8, 128))
    head_square = jnp.broadcast_to(jnp.sum(tail * tail, axis=1, keepdims=True), (8, 128))
    head_sum = jnp.broadcast_to(jnp.sum(tail, axis=1, keepdims=True), (8, 128))
    a_buf[chip] = jnp.where(tile == 0, head_total, jnp.where(tile == 1, head_square, head_sum))

    def a_copy(step):
        peer = (chip + step) % 16
        return remote(
            a_buf.at[chip], a_buf.at[chip], a_send.at[peer], a_recv.at[chip],
            seq_0=peer // 4, seq_1=peer % 4,
        )

    for step in range(1, 16):
        a_copy(step).start()
    small[...] = drift[:, other_rows]
    for level in range(6):
        ss_rows = slice(8 * level, 8 * level + 8)
        ys[y, 1, ss_rows] = glw[level, :, other_rows]
    glw_copy = remote(
        ys.at[y, 1, pl.ds(0, 48)], bs.at[pl.ds(0, 48), :], last_send.at[0], last_recv.at[0],
        seq_2=other,
    )
    glw_copy.start()
    bs_out.start()
    for level in range(6):
        glw_out[level, own_heads, :] = glw[level, :, own_rows]

    loop(0, 4, cross_grad)
    for pair in range(4):
        for kind in range(3):
            back_copy(pair, kind).wait_recv()
    other_q = pl.ds(pl.multiple_of(other * 1024, 1024), 1024)
    other_v = pl.ds(pl.multiple_of(other * 512, 512), 512)
    gq_out[:, other_q] = bq[...].astype(BF16)
    gk_out[:, other_q] = bk[...].astype(BF16)
    gv_out[:, other_v] = bv[...].astype(BF16)
    glw_copy.wait_recv()
    for level in range(6):
        glw_out[level, other_heads, :] = bs[8 * level : 8 * level + 8, :]
    stores = [
        pltpu.make_async_copy(src, dst, store_sem.at[n])
        for n, (src, dst) in enumerate((
            (gq_out, gq_hbm), (gk_out, gk_hbm), (gv_out, gv_hbm), (glw_out, glw_hbm),
            (glg_out, glg_hbm),
        ))
    ]
    for store in stores[:4]:
        store.start()

    for step in range(1, 16):
        peer = (chip + step) % 16
        remote(
            a_buf.at[chip], a_buf.at[peer], a_send.at[peer], a_recv.at[peer],
            seq_0=peer // 4, seq_1=peer % 4,
        ).wait_recv()
    run = jnp.zeros((8, 1), F32)
    later = jnp.zeros((8, 1), F32)
    squares = jnp.zeros((8, 1), F32)
    for at in range(15, -1, -1):
        now = a_buf[at]
        later = later + run * (chip == at).astype(F32)
        squares = squares + now[:, 1:2] + run * (2.0 * now[:, 2:3] + 256.0 * run)
        run = run + now[:, 0:1]
    whole = jnp.broadcast_to(jnp.sum(squares, axis=0, keepdims=True), (8, 128))
    b_buf[group] = jnp.where(tile < 64, jnp.broadcast_to(later, (8, 128)), whole)

    def b_peer(step):
        peer = (group + step) % 8
        return peer, {"head": peer // 2, "seq_2": peer % 2}

    for step in range(1, 8):
        peer, to = b_peer(step)
        remote(
            b_buf.at[group], b_buf.at[group], b_send.at[peer], b_recv.at[group], **to
        ).start()
    for step in range(1, 8):
        peer, to = b_peer(step)
        remote(
            b_buf.at[group], b_buf.at[peer], b_send.at[peer], b_recv.at[peer], **to
        ).wait_recv()
    total_square = jnp.zeros((8, 128), F32)
    for at in range(8):
        total_square = total_square + b_buf[at]
    factor = jnp.minimum(1.0, lax.rsqrt(total_square[:, 64:65] / (64 * 4096) + 1e-06))
    glg_out[own_heads, :] = (drift[:, own_rows] + later) * factor
    bs_out.wait_recv()
    glg_out[other_heads, :] = (bs[48:56, :] + b_buf[z * 2 + other][:, 0:1]) * factor

    stores[4].start()
    for swap in swaps:
        swap.wait_send()
    for pair in range(4):
        for kind in range(4):

            @pl.when((y != pair) & sent(kind, y))
            def _():
                y1_copy(pair, kind, y).wait_send()

            back = (pair % 2 == 1, pair >= 2, x > 0, True)[kind]
            if back is not False:

                @pl.when((y != pair) & back)
                def _():
                    y2_copy(pair, kind, y2_source(pair, kind)).wait_send()

        @pl.when(pair != x)
        def _():
            x_copy(pair, 0).wait_send()

        for kind in range(3):
            back_copy(pair, kind).wait_send()
    glw_copy.wait_send()
    bs_out.wait_send()
    for step in range(1, 16):
        a_copy(step).wait_send()
    for step in range(1, 8):
        peer, to = b_peer(step)
        remote(
            b_buf.at[group], b_buf.at[group], b_send.at[peer], b_recv.at[group], **to
        ).wait_send()
    for store in stores:
        store.wait()


def settle(*refs):
    count = (len(refs) - 2) // 3
    source, target, held = (refs[n * count : n * count + count] for n in range(3))
    load_sem, store_sem = refs[3 * count :]
    pieces = []
    for n in range(count):
        cuts = 4 if n < 2 else 2 if n == 2 else 1
        rows = source[n].shape[0] // cuts
        pieces += [(n, pl.ds(rows * cut, rows)) for cut in range(cuts)]
    loads = [
        pltpu.make_async_copy(source[n].at[at], held[n].at[at], load_sem.at[m])
        for m, (n, at) in enumerate(pieces)
    ]
    stores = [
        pltpu.make_async_copy(held[n].at[at], target[n].at[at], store_sem.at[m])
        for m, (n, at) in enumerate(pieces)
    ]
    for load in loads:
        load.start()
    for load, store in zip(loads, stores):
        load.wait()
        store.start()
    for store in stores:
        store.wait()


def shards(queries, keys, values, out_grad, log_gate, level_weight, doc_start):
    args = (queries, keys, values, out_grad, log_gate, level_weight, doc_start.reshape(1, -1))
    anywhere = pl.BlockSpec(memory_space=pl.ANY)
    results = tuple(
        jax.ShapeDtypeStruct(a.shape, a.dtype)
        for a in (queries, keys, values, level_weight, log_gate)
    )
    held = [pltpu.VMEM(r.shape, r.dtype) for r in results]
    scratch = [pltpu.VMEM(a.shape, a.dtype) for a in args] + held
    scratch += [pltpu.SemaphoreType.DMA((7,)), pltpu.SemaphoreType.DMA((5,))]
    swap = [(128, 1024), (128, 1024), (128, 512), (128, 512), (64, 128)]
    scratch += [pltpu.VMEM(s, F32) for s in swap * 2]
    scratch += [pltpu.VMEM(s, BF16) for s in ((256, 1024), (256, 1024), (256, 512), (256, 512))]
    scratch += [pltpu.VMEM((4, 128, 256), F32)] * 2
    scratch += [pltpu.VMEM((8, 256), F32)] * 5
    scratch += [pltpu.VMEM((6, 8, 256), F32), pltpu.VMEM((8, 256, 128), F32)]
    scratch += [pltpu.VMEM((256, 256), F32), pltpu.VMEM((256, 256), BF16), pltpu.VMEM((256, 256), BF16)]
    scratch += [pltpu.VMEM((256, 1024), F32), pltpu.VMEM((256, 1024), F32), pltpu.VMEM((256, 512), F32)]
    scratch += [pltpu.VMEM((4, 128, 256), F32), pltpu.VMEM((6, 8, 256), F32)]
    scratch += [pltpu.VMEM((8, 256), F32), pltpu.VMEM((8, 128), F32)]
    scratch += [pltpu.VMEM((4, 4, 136, 128), F32)] * 2 + [pltpu.VMEM((4, 4, 128, 128), F32)] * 2
    scratch += [pltpu.VMEM((2, 136, 128), F32), pltpu.VMEM((4, 136, 128), F32)]
    scratch += [pltpu.VMEM((128, 128), F32)] * 2
    scratch += [pltpu.VMEM((128, 1024), F32), pltpu.VMEM((128, 1024), F32), pltpu.VMEM((128, 512), F32)]
    scratch += [pltpu.VMEM((56, 128), F32)]
    scratch += [pltpu.VMEM((16, 8, 128), F32), pltpu.VMEM((8, 8, 128), F32)]
    sems = [(5,), (5,), (4, 4), (4, 4), (4, 4), (4, 4), (4,), (4,), (4, 3), (4, 3), (2,), (2,)]
    sems += [(16,), (16,), (8,), (8,)]
    scratch += [pltpu.SemaphoreType.DMA(s) for s in sems]
    outs = pl.pallas_call(
        kernel,
        out_shape=results,
        in_specs=[anywhere] * 7,
        out_specs=[anywhere] * 5,
        scratch_shapes=scratch,
        compiler_params=pltpu.CompilerParams(
            collective_id=0, has_side_effects=True, vmem_limit_bytes=56 * 2**20
        ),
    )(*args)
    return pl.pallas_call(
        settle,
        out_shape=results,
        in_specs=[anywhere] * 5,
        out_specs=[anywhere] * 5,
        scratch_shapes=held + [pltpu.SemaphoreType.DMA((12,)), pltpu.SemaphoreType.DMA((12,))],
        compiler_params=pltpu.CompilerParams(vmem_limit_bytes=56 * 2**20),
    )(*outs)


def solution(mesh):
    finer = Mesh(
        mesh.devices.reshape(4, 4, 2, mesh.shape["head"]), ("seq_0", "seq_1", "seq_2", "head")
    )
    wide = P(SEQ, "head")
    return jax.shard_map(
        shards,
        mesh=finer,
        in_specs=(wide, wide, wide, wide, P("head", SEQ), P(None, "head", SEQ), P(SEQ)),
        out_specs=(wide, wide, wide, P(None, "head", SEQ), P("head", SEQ)),
        check_vma=False,
    )
```

```python
import functools

import jax
import jax.numpy as jnp
from jax import lax
from jax.experimental import pallas as pl
from jax.experimental.pallas import tpu as pltpu
from jax.sharding import Mesh
from jax.sharding import PartitionSpec as P

SEQ = ("seq_0", "seq_1", "seq_2")
MESH = pl.DeviceIdType.MESH
F32 = jnp.float32
BF16 = jnp.bfloat16
NEG = -1e30

NN = (((1,), (0,)), ((), ()))
NT = (((1,), (1,)), ((), ()))
TN = (((0,), (0,)), ((), ()))


def dot(a, b, dims):
    return lax.dot_general(a, b, dims, preferred_element_type=F32)


def split(a):
    hi = a.astype(BF16)
    return hi, (a - hi.astype(F32)).astype(BF16)


def prefix(a, lane):
    shift = 1
    while shift < a.shape[1]:
        a = a + jnp.where(lane >= shift, pltpu.roll(a, shift, 1), 0.0)
        shift *= 2
    return a


def suffix(a, lane):
    size = a.shape[1]
    shift = 1
    while shift < size:
        a = a + jnp.where(lane < size - shift, pltpu.roll(a, size - shift, 1), 0.0)
        shift *= 2
    return a


def kernel(
    q_hbm, k_hbm, v_hbm, g_hbm, lg_hbm, lw_hbm, ds_hbm,
    gq_out, gk_out, gv_out, glw_out, glg_out,
    q_in, k_in, v_in, g_in, lg_in, lw_in, ds_in, load_sem,
    sq, sk, sv, sg, ss, rq, rk, rv, rg, rs,
    qb, kb, vb, gb, vt, gt,
    gates, doc, cum, resets, fs, de, wts, cm, bias, pt, rt,
    gq, gk, gv, gvt, glw, drift, small,
    ys, yr, zs, zr, xs, xr, ein, xin,
    bq, bk, bv, bs,
    a_buf, b_buf,
    in_send, in_recv, y1_send, y1_recv, y2_send, y2_recv, x_send, x_recv,
    out_send, out_recv, last_send, last_recv, a_send, a_recv, b_send, b_recv,
):
    x, y, c, z = (lax.axis_index(n) for n in ("seq_0", "seq_1", "seq_2", "head"))
    other = 1 - c
    chip = x * 4 + y
    group = z * 2 + c

    def remote(src, dst, send, recv, **to):
        return pltpu.make_async_remote_copy(
            src_ref=src, dst_ref=dst, send_sem=send, recv_sem=recv,
            device_id=to, device_id_type=MESH,
        )

    loads = [
        pltpu.make_async_copy(src, dst, load_sem.at[n])
        for n, (src, dst) in enumerate((
            (ds_hbm, ds_in), (lg_hbm, lg_in), (lw_hbm, lw_in), (k_hbm, k_in),
            (v_hbm, v_in), (g_hbm, g_in), (q_hbm, q_in),
        ))
    ]
    for load in loads:
        load.start()

    barrier = pltpu.get_barrier_semaphore()
    for step in range(1, 16):
        peer = (chip + step) % 16
        pl.semaphore_signal(
            barrier, inc=1, device_id={"seq_0": peer // 4, "seq_1": peer % 4}, device_id_type=MESH
        )
    for step in range(1, 8):
        peer = (group + step) % 8
        pl.semaphore_signal(
            barrier, inc=1, device_id={"head": peer // 2, "seq_2": peer % 2}, device_id_type=MESH
        )

    q_cols = pl.ds(pl.multiple_of(other * 1024, 1024), 1024)
    v_cols = pl.ds(pl.multiple_of(other * 512, 512), 512)
    own_q = pl.ds(pl.multiple_of(c * 1024, 1024), 1024)
    own_v = pl.ds(pl.multiple_of(c * 512, 512), 512)
    own_rows = pl.ds(pl.multiple_of(c * 128, 128), 128)
    other_rows = pl.ds(pl.multiple_of(other * 128, 128), 128)
    own_heads = pl.ds(pl.multiple_of(c * 8, 8), 8)
    other_heads = pl.ds(pl.multiple_of(other * 8, 8), 8)
    for load in loads[:3]:
        load.wait()
    ds_row = jnp.broadcast_to(ds_in[...].astype(F32), (8, 128))
    ss[0:8, :] = lg_in[other_heads, :]
    for level in range(6):
        ss[8 + 8 * level : 16 + 8 * level, :] = lw_in[level, other_heads, :]
    ss[56:64, :] = ds_row
    loads[3].wait()
    sk[...] = k_in[:, q_cols].astype(F32)
    loads[4].wait()
    sv[...] = v_in[:, v_cols].astype(F32)
    loads[5].wait()
    sg[...] = g_in[:, v_cols].astype(F32)
    loads[6].wait()
    sq[...] = q_in[:, q_cols].astype(F32)

    pl.semaphore_wait(barrier, 22)
    swaps = [
        remote(src, dst, in_send.at[n], in_recv.at[n], seq_2=other)
        for n, (src, dst) in enumerate(((ss, rs), (sk, rk), (sv, rv), (sg, rg), (sq, rq)))
    ]
    for swap in swaps:
        swap.start()

    kb[own_rows, :] = k_in[:, own_q]
    vb[own_rows, :] = v_in[:, own_v]
    gb[own_rows, :] = g_in[:, own_v]
    qb[own_rows, :] = q_in[:, own_q]
    gates[:, own_rows] = lg_in[own_heads, :]
    for level in range(6):
        wts[level, :, own_rows] = lw_in[level, own_heads, :]
    doc[:, own_rows] = ds_row
    ein[...] = jnp.zeros_like(ein)
    xin[...] = jnp.zeros_like(xin)
    pt[128:256, 0:128] = jnp.zeros((128, 128), BF16)
    rt[128:256, 0:128] = jnp.zeros((128, 128), BF16)

    zero_slab = jnp.zeros((128, 128), F32)
    for level, absent in ((0, y % 2 == 0), (1, y < 2), (2, x == 0)):

        @pl.when(absent)
        def _():
            for pair in range(4):
                zr[pair, level] = zero_slab

    swaps[0].wait_recv()
    gates[:, other_rows] = rs[0:8, :]
    for level in range(6):
        wts[level, :, other_rows] = rs[8 + 8 * level : 16 + 8 * level, :]
    doc[:, other_rows] = rs[56:64, :]
    lane = lax.broadcasted_iota(jnp.int32, (8, 256), 1)
    cum_now = prefix(gates[...], lane)
    reset = prefix(doc[...], lane)
    total = cum_now[:, 255:256]
    reset_total = reset[:, 255:256]
    cum[...] = cum_now
    resets[...] = reset
    fs[...] = jnp.where(reset == 0.0, jnp.exp(cum_now), 0.0)
    de[...] = jnp.where(reset == reset_total, jnp.exp(total - cum_now), 0.0)
    decay = jnp.broadcast_to(jnp.where(reset_total == 0.0, jnp.exp(total), 0.0), (8, 128))
    small[...] = decay
    def masks():
        columns = jnp.transpose(
            jnp.concatenate([cum[...], resets[...], jnp.zeros((112, 256), F32)], axis=0)
        )
        for head in range(8):
            cm[head] = jnp.broadcast_to(columns[:, head : head + 1], (256, 128))
        reset_col = jnp.broadcast_to(columns[:, 8:9], (256, 128))
        for half in range(2):
            reset_row = jnp.broadcast_to(resets[0:1, 128 * half : 128 * half + 128], (256, 128))
            s_pos = lax.broadcasted_iota(jnp.int32, (256, 128), 0)
            t_pos = lax.broadcasted_iota(jnp.int32, (256, 128), 1) + 128 * half
            bias[:, 128 * half : 128 * half + 128] = jnp.where(
                (t_pos >= s_pos) & (reset_col == reset_row), 0.0, NEG
            )

    def head_cols(pair, i):
        return pl.ds(pl.multiple_of(pair * 256 + i * 128, 128), 128)

    def pair_cols(pair):
        return pl.ds(pl.multiple_of(pair * 128, 128), 128)

    def sent(kind, at_y):
        return (True, x > 0, at_y % 2 == 1, at_y >= 2)[kind]

    def y1_copy(pair, kind, at_y):
        rows = 136 if kind == 0 else 128
        return remote(
            ys.at[pair, kind, pl.ds(0, rows)], yr.at[at_y, kind, pl.ds(0, rows)],
            y1_send.at[pair, kind], y1_recv.at[at_y, kind], seq_1=pair,
        )

    def place(pair, kind, i, slab):
        rows = pl.ds(64 * i, 64)

        @pl.when(pair == y)
        def _():
            yr[y, kind, rows] = slab

        @pl.when(pair != y)
        def _():
            ys[pair, kind, rows] = slab

    def hand_over(pair, kind):
        @pl.when((pair != y) & sent(kind, y))
        def _():
            y1_copy(pair, kind, y).start()

    def state_fwd(pair):
        vt[pair] = jnp.transpose(vb[:, pair_cols(pair)].astype(F32))
        for i in range(2):
            head = pl.ds(pair * 2 + i, 1)
            value_hi, value_lo = split(vt[pair, pl.ds(64 * i, 64)] * de[head, :])
            state = dot(
                jnp.concatenate([value_hi, value_lo], axis=0), kb[:, head_cols(pair, i)], NN
            )
            place(pair, 0, i, state[0:64] + state[64:128])
            row = small[head, :]

            @pl.when(pair == y)
            def _():
                yr[y, 0, 128 + i : 129 + i] = row

            @pl.when(pair != y)
            def _():
                ys[pair, 0, 128 + i : 129 + i] = row

        hand_over(pair, 0)

    def state_back(pair):
        gt[pair] = jnp.transpose(gb[:, pair_cols(pair)].astype(F32))
        for i in range(2):
            head = pl.ds(pair * 2 + i, 1)
            hi, lo = split(gt[pair, pl.ds(64 * i, 64)] * (fs[head, :] * wts[5, head, :]))
            back = dot(jnp.concatenate([hi, lo], axis=0), qb[:, head_cols(pair, i)], NN)
            place(pair, 1, i, back[0:64] + back[64:128])
        hand_over(pair, 1)

    def state_near(pair):
        for i in range(2):
            head = pl.ds(pair * 2 + i, 1)
            grad = gt[pair, pl.ds(64 * i, 64)]
            parts = [split(grad * (fs[head, :] * wts[level, head, :])) for level in (3, 4)]
            back = dot(
                jnp.concatenate([p[0] for p in parts] + [p[1] for p in parts], axis=0),
                qb[:, head_cols(pair, i)], NN,
            )
            for n in range(2):
                place(
                    pair, 2 + n, i, back[64 * n : 64 * n + 64] + back[128 + 64 * n : 192 + 64 * n]
                )
        hand_over(pair, 2)
        hand_over(pair, 3)

    def intra(pair):
        for i in range(2):
            number = pair * 2 + i
            head = pl.ds(number, 1)
            rows = pl.ds(64 * i, 64)
            query = qb[:, head_cols(pair, i)]
            key = kb[:, head_cols(pair, i)]
            grad = gb[:, pair_cols(pair)]
            value = vb[:, pair_cols(pair)]
            mine = lax.broadcasted_iota(jnp.int32, (64, 128), 1) // 64 == i
            weight = [wts[level, head, :] for level in range(3)]
            span = lax.broadcasted_iota(jnp.int32, (1, 256), 1) // 64
            cum_row = cum[head, :]
            level_rows = [jnp.zeros((1, 256), F32) for level in range(3)]
            drift_row = jnp.zeros((1, 256), F32)
            for b in range(4):
                low = 0 if b < 2 else 128
                blk = slice(64 * b, 64 * b + 64)
                score = dot(key[blk], query[low:256], NT)
                pair_dot = dot(
                    jnp.where(mine, value[blk], jnp.zeros((64, 128), BF16)), grad[low:256], NT
                )
                col = cm[number, blk, :]
                if low == 0:
                    col = jnp.concatenate([col, col], axis=1)
                decayed = jnp.exp((cum_row[:, low:256] - col) + bias[blk, low:256])
                at = span[:, low:256]
                near = (at == b).astype(jnp.int32), ((at ^ 1) == b).astype(jnp.int32)
                mix = jnp.where(
                    near[0] == 1, weight[0][:, low:256],
                    jnp.where(near[1] == 1, weight[1][:, low:256], weight[2][:, low:256]),
                )
                scored = decayed * score
                joint = jnp.sum(scored * pair_dot, axis=0, keepdims=True)
                prob = (scored * mix).astype(BF16)
                pt[blk, low:256] = prob
                rt[blk, low:256] = (decayed * mix * pair_dot).astype(BF16)
                drifted = jnp.sum(prob.astype(F32) * pair_dot, axis=0, keepdims=True)
                if low:
                    pad = jnp.zeros((1, 128), F32)
                    joint = jnp.concatenate([pad, joint], axis=1)
                    drifted = jnp.concatenate([pad, drifted], axis=1)
                drift_row = drift_row + drifted
                level_rows[0] = level_rows[0] + jnp.where(span == b, joint, 0.0)
                level_rows[1] = level_rows[1] + jnp.where((span ^ 1) == b, joint, 0.0)
                level_rows[2] = level_rows[2] + jnp.where(
                    (span != b) & ((span ^ 1) != b), joint, 0.0
                )
            for level in range(3):
                glw[level, head, :] = level_rows[level]
            drift[head, :] = drift_row
            gvt[pair, rows] = dot(gt[pair, rows].astype(BF16), pt[...], NT)
            gk[:, head_cols(pair, i)] = dot(rt[...], query, NN)
            gq[:, head_cols(pair, i)] = dot(rt[...], key, TN)

    def y2_copy(to_y, kind, src):
        return remote(
            src, zr.at[y, kind], y2_send.at[to_y, kind], y2_recv.at[y, kind], seq_1=to_y
        )

    def y2_source(to_y, kind):
        if kind == 0:
            return yr.at[to_y - 1, 0, pl.ds(0, 128)]
        return zs.at[to_y, kind]

    def hand_back(to_y, kind):
        def go():
            @pl.when(to_y != y)
            def _():
                y2_copy(to_y, kind, y2_source(to_y, kind)).start()

            @pl.when(to_y == y)
            def _():
                zr[y, kind] = y2_source(to_y, kind)[...]

        if kind == 2:
            pl.when(x > 0)(go)
        else:
            go()

    def y1_wait(kind):
        for at_y in range(4):
            here = sent(kind, at_y)
            if here is False:
                continue

            @pl.when((y != at_y) & here)
            def _():
                y1_copy(y, kind, at_y).wait_recv()

    def x_copy(to_x, kind):
        return remote(xs.at[kind], xr.at[x], x_send.at[to_x], x_recv.at[x], seq_0=to_x)

    def decays(i):
        return [yr[n, 0, 128 + i : 129 + i] for n in range(4)]

    def combine_fwd():
        y1_wait(0)
        for i in range(2):
            rows = slice(64 * i, 64 * i + 64)
            dec = decays(i)
            both = dec[1] * yr[0, 0, rows] + yr[1, 0, rows]
            zs[2, 1, rows] = both
            after = dec[2] * both
            zs[3, 1, rows] = after
            xs[0, rows] = dec[3] * (after + yr[2, 0, rows]) + yr[3, 0, rows]
            all_decay = dec[0] * dec[1] * (dec[2] * dec[3])
            xs[0, 128 + i : 129 + i] = all_decay
            xs[1, 128 + i : 129 + i] = all_decay
        for to_x in range(4):

            @pl.when(to_x > x)
            def _():
                x_copy(to_x, 0).start()

    def combine_back():
        y1_wait(1)

        @pl.when(x > 0)
        def _():
            for i in range(2):
                rows = slice(64 * i, 64 * i + 64)
                dec = decays(i)
                back = yr[2, 1, rows] + dec[2] * yr[3, 1, rows]
                back = yr[1, 1, rows] + dec[1] * back
                xs[1, rows] = yr[0, 1, rows] + dec[0] * back

        for to_x in range(4):

            @pl.when(to_x < x)
            def _():
                x_copy(to_x, 1).start()

        hand_back(1, 0)
        hand_back(3, 0)
        hand_back(2, 1)
        hand_back(3, 1)

    def take(acc, at_x):
        remote(
            xs.at[0], xr.at[at_x], x_send.at[at_x], x_recv.at[at_x], seq_0=at_x
        ).wait_recv()
        for i in range(2):
            rows = slice(64 * i, 64 * i + 64)
            acc[rows] = xr[at_x, 128 + i : 129 + i] * acc[rows] + xr[at_x, rows]

    def enter_far():
        for at_x in range(4):
            pl.when(at_x < x)(functools.partial(take, ein, at_x))
        for i in range(2):
            rows = slice(64 * i, 64 * i + 64)
            dec = decays(i)
            into = ein[rows]
            for at_y in range(4):
                zs[at_y, 2, rows] = into
                into = dec[at_y] * into
        for step in (2, 1, 3, 0):
            hand_back((y + step) % 4, 2)

    def leave_far():
        y1_wait(2)
        y1_wait(3)
        for at_x in range(3, -1, -1):
            pl.when(at_x > x)(functools.partial(take, xin, at_x))
        for i in range(2):
            rows = slice(64 * i, 64 * i + 64)
            dec = decays(i)
            late = xin[rows]
            zs[3, 3, rows] = late
            late = dec[3] * late
            zs[2, 3, rows] = late + yr[3, 2, rows]
            late = dec[2] * late + (yr[2, 3, rows] + dec[2] * yr[3, 3, rows])
            zs[1, 3, rows] = late
            zs[0, 3, rows] = dec[1] * late + yr[1, 2, rows]
        for step in (2, 1, 3, 0):
            hand_back((y + step) % 4, 3)

    def back_copy(pair, kind):
        if kind == 2:
            cols, src, dst = pair_cols(pair), gv, bv
        else:
            cols = pl.ds(pl.multiple_of(pair * 256, 256), 256)
            src, dst = ((gq, bq), (gk, bk))[kind]
        return remote(
            src.at[other_rows, cols], dst.at[:, cols],
            out_send.at[kind], out_recv.at[kind], seq_2=other,
        )

    def y2_wait(pair, kinds):
        for kind in kinds:
            here = (y % 2 == 1, y >= 2, x > 0, True)[kind]

            @pl.when((pair != y) & here)
            def _():
                remote(
                    zs.at[0, kind], zr.at[pair, kind], y2_send.at[0, kind],
                    y2_recv.at[pair, kind], seq_1=pair,
                ).wait_recv()

    def cross_in(pair):
        y2_wait(pair, (0, 1, 2))
        for i in range(2):
            head = pl.ds(pair * 2 + i, 1)
            rows = pl.ds(64 * i, 64)
            grad = gt[pair, rows]
            enter_hi, enter_lo = split(
                jnp.concatenate([zr[pair, n, rows] for n in range(3)], axis=0)
            )
            mixed = dot(
                jnp.concatenate([enter_hi, enter_lo], axis=0), qb[:, head_cols(pair, i)], NT
            )
            drift_row = drift[head, :]
            for n in range(3):
                state_row = mixed[64 * n : 64 * n + 64] + mixed[192 + 64 * n : 256 + 64 * n]
                level_row = fs[head, :] * jnp.sum(state_row * grad, axis=0, keepdims=True)
                glw[3 + n, head, :] = level_row
                drift_row = drift_row + wts[3 + n, head, :] * level_row
            drift[head, :] = drift_row
            weighted_hi, weighted_lo = split(
                jnp.concatenate(
                    [grad * (fs[head, :] * wts[3 + n, head, :]) for n in range(3)], axis=0
                )
            )
            gq[:, head_cols(pair, i)] = gq[:, head_cols(pair, i)] + dot(
                jnp.concatenate([weighted_hi, weighted_lo, weighted_hi], axis=0),
                jnp.concatenate([enter_hi, enter_hi, enter_lo], axis=0), TN,
            )
        back_copy(pair, 0).start()
        wide = pl.ds(pl.multiple_of(pair * 256, 256), 256)
        out_wide = pl.ds(pl.multiple_of(c * 1024 + pair * 256, 256), 256)
        gq_out[:, out_wide] = gq[own_rows, wide].astype(BF16)

    def cross_out(pair):
        y2_wait(pair, (3,))
        for i in range(2):
            head = pl.ds(pair * 2 + i, 1)
            rows = pl.ds(64 * i, 64)
            leave_hi, leave_lo = split(zr[pair, 3, rows])
            left = dot(
                jnp.concatenate([leave_hi, leave_lo], axis=0), kb[:, head_cols(pair, i)], NT
            )
            value_grad = gvt[pair, rows] + de[head, :] * (left[0:64] + left[64:128])
            gvt[pair, rows] = value_grad
            drift[head, :] = drift[head, :] - jnp.sum(
                vt[pair, rows] * value_grad, axis=0, keepdims=True
            )

    def cross_grad(pair):
        for i in range(2):
            head = pl.ds(pair * 2 + i, 1)
            rows = pl.ds(64 * i, 64)
            leave_hi, leave_lo = split(zr[pair, 3, rows])
            ended_hi, ended_lo = split(vt[pair, rows] * de[head, :])
            gk[:, head_cols(pair, i)] = gk[:, head_cols(pair, i)] + dot(
                jnp.concatenate([ended_hi, ended_lo, ended_hi], axis=0),
                jnp.concatenate([leave_hi, leave_hi, leave_lo], axis=0), TN,
            )
        gv[:, pair_cols(pair)] = jnp.transpose(gvt[pair])
        back_copy(pair, 1).start()
        back_copy(pair, 2).start()
        wide = pl.ds(pl.multiple_of(pair * 256, 256), 256)
        out_wide = pl.ds(pl.multiple_of(c * 1024 + pair * 256, 256), 256)
        out_narrow = pl.ds(pl.multiple_of(c * 512 + pair * 128, 128), 128)
        gk_out[:, out_wide] = gk[own_rows, wide].astype(BF16)
        gv_out[:, out_narrow] = gv[own_rows, pair_cols(pair)].astype(BF16)

    def loop(low, high, body):
        def step(n, carry):
            body(n)
            return carry

        lax.fori_loop(low, high, step, 0)

    def toward(n):
        return (y + jnp.where(n == 2, 3, jnp.where(n == 3, 0, 2 - n))) % 4

    def nearby(n):
        return (y + jnp.where(n == 2, 3, jnp.where(n == 3, 2, n))) % 4

    swaps[1].wait_recv()
    kb[other_rows, :] = rk[...].astype(BF16)
    swaps[2].wait_recv()
    vb[other_rows, :] = rv[...].astype(BF16)
    loop(0, 4, lambda n: state_fwd(toward(n)))
    swaps[3].wait_recv()
    gb[other_rows, :] = rg[...].astype(BF16)
    swaps[4].wait_recv()
    qb[other_rows, :] = rq[...].astype(BF16)
    loop(0, 4, lambda n: state_back(toward(n)))
    masks()
    loop(0, 1, intra)
    combine_fwd()
    loop(0, 4, lambda n: state_near(toward(n)))
    combine_back()
    loop(1, 3, intra)
    enter_far()
    loop(3, 4, intra)
    leave_far()
    loop(0, 4, lambda n: cross_in(nearby(n)))
    loop(0, 4, lambda n: cross_out(nearby(n)))
    lane = lax.broadcasted_iota(jnp.int32, (8, 256), 1)
    tail = suffix(drift[...], lane)
    drift[...] = tail
    bs_out = remote(small.at[:, :], bs.at[pl.ds(48, 8), :], last_send.at[1], last_recv.at[1], seq_2=other)
    tile = lax.broadcasted_iota(jnp.int32, (8, 128), 1)
    head_total = jnp.broadcast_to(tail[:, 0:1], (8, 128))
    head_square = jnp.broadcast_to(jnp.sum(tail * tail, axis=1, keepdims=True), (8, 128))
    head_sum = jnp.broadcast_to(jnp.sum(tail, axis=1, keepdims=True), (8, 128))
    a_buf[chip] = jnp.where(tile == 0, head_total, jnp.where(tile == 1, head_square, head_sum))

    def a_copy(step):
        peer = (chip + step) % 16
        return remote(
            a_buf.at[chip], a_buf.at[chip], a_send.at[0], a_recv.at[0],
            seq_0=peer // 4, seq_1=peer % 4,
        )

    for step in range(1, 16):
        a_copy(step).start()
    small[...] = drift[:, other_rows]
    for level in range(6):
        ss_rows = slice(8 * level, 8 * level + 8)
        ys[y, 1, ss_rows] = glw[level, :, other_rows]
    glw_copy = remote(
        ys.at[y, 1, pl.ds(0, 48)], bs.at[pl.ds(0, 48), :], last_send.at[0], last_recv.at[0],
        seq_2=other,
    )
    glw_copy.start()
    bs_out.start()
    for level in range(6):
        glw_out[level, own_heads, :] = glw[level, :, own_rows]

    loop(0, 4, cross_grad)
    def back_whole(kind):
        src, dst = ((gq, bq), (gk, bk), (gv, bv))[kind]
        return remote(
            src.at[other_rows, :], dst, out_send.at[kind], out_recv.at[kind], seq_2=other
        )

    for kind in range(3):
        back_whole(kind).wait_recv()
    other_q = pl.ds(pl.multiple_of(other * 1024, 1024), 1024)
    other_v = pl.ds(pl.multiple_of(other * 512, 512), 512)
    gq_out[:, other_q] = bq[...].astype(BF16)
    gk_out[:, other_q] = bk[...].astype(BF16)
    gv_out[:, other_v] = bv[...].astype(BF16)
    glw_copy.wait_recv()
    for level in range(6):
        glw_out[level, other_heads, :] = bs[8 * level : 8 * level + 8, :]

    a_whole = remote(
        a_buf.at[pl.ds(0, 15)], a_buf.at[pl.ds(0, 15)], a_send.at[0], a_recv.at[0], seq_2=other
    )
    a_whole.wait_recv()
    run = jnp.zeros((8, 1), F32)
    later = jnp.zeros((8, 1), F32)
    squares = jnp.zeros((8, 1), F32)
    for at in range(15, -1, -1):
        now = a_buf[at]
        later = later + run * (chip == at).astype(F32)
        squares = squares + now[:, 1:2] + run * (2.0 * now[:, 2:3] + 256.0 * run)
        run = run + now[:, 0:1]
    whole = jnp.broadcast_to(jnp.sum(squares, axis=0, keepdims=True), (8, 128))
    b_buf[group] = jnp.where(tile < 64, jnp.broadcast_to(later, (8, 128)), whole)

    def b_peer(step):
        peer = (group + step) % 8
        return {"head": peer // 2, "seq_2": peer % 2}

    for step in range(1, 8):
        to = b_peer(step)
        remote(
            b_buf.at[group], b_buf.at[group], b_send.at[0], b_recv.at[0], **to
        ).start()
    b_whole = remote(
        b_buf.at[pl.ds(0, 7)], b_buf.at[pl.ds(0, 7)], b_send.at[0], b_recv.at[0], seq_2=other
    )
    b_whole.wait_recv()
    total_square = jnp.zeros((8, 128), F32)
    for at in range(8):
        total_square = total_square + b_buf[at]
    factor = jnp.minimum(1.0, lax.rsqrt(total_square[:, 64:65] / (64 * 4096) + 1e-06))
    glg_out[own_heads, :] = (drift[:, own_rows] + later) * factor
    bs_out.wait_recv()
    glg_out[other_heads, :] = (bs[48:56, :] + b_buf[z * 2 + other][:, 0:1]) * factor

    for swap in swaps:
        swap.wait_send()
    for pair in range(4):
        for kind in range(4):

            @pl.when((y != pair) & sent(kind, y))
            def _():
                y1_copy(pair, kind, y).wait_send()

            back = (pair % 2 == 1, pair >= 2, x > 0, True)[kind]
            if back is not False:

                @pl.when((y != pair) & back)
                def _():
                    y2_copy(pair, kind, y2_source(pair, kind)).wait_send()

        @pl.when(pair != x)
        def _():
            x_copy(pair, 0).wait_send()

    for kind in range(3):
        back_whole(kind).wait_send()
    glw_copy.wait_send()
    bs_out.wait_send()
    a_whole.wait_send()
    b_whole.wait_send()


def settle(*refs):
    source, target, sem = refs[:5], refs[5:10], refs[10]
    stores = []
    for n in range(5):
        cuts = 4 if n < 2 else 2 if n == 2 else 1
        rows = source[n].shape[0] // cuts
        for m in range(cuts):
            at = pl.ds(rows * m, rows)
            stores.append(
                pltpu.make_async_copy(source[n].at[at], target[n].at[at], sem.at[len(stores)])
            )
    for store in stores:
        store.start()
    for store in stores:
        store.wait()


def shards(queries, keys, values, out_grad, log_gate, level_weight, doc_start):
    args = (queries, keys, values, out_grad, log_gate, level_weight, doc_start.reshape(1, -1))
    anywhere = pl.BlockSpec(memory_space=pl.ANY)
    results = tuple(
        jax.ShapeDtypeStruct(a.shape, a.dtype)
        for a in (queries, keys, values, level_weight, log_gate)
    )
    held = tuple(pltpu.VMEM(r.shape, r.dtype) for r in results)
    scratch = [pltpu.VMEM(a.shape, a.dtype) for a in args] + [pltpu.SemaphoreType.DMA((7,))]
    swap = [(128, 1024), (128, 1024), (128, 512), (128, 512), (64, 128)]
    scratch += [pltpu.VMEM(s, F32) for s in swap * 2]
    scratch += [pltpu.VMEM(s, BF16) for s in ((256, 1024), (256, 1024), (256, 512), (256, 512))]
    scratch += [pltpu.VMEM((4, 128, 256), F32)] * 2
    scratch += [pltpu.VMEM((8, 256), F32)] * 6
    scratch += [pltpu.VMEM((6, 8, 256), F32), pltpu.VMEM((8, 256, 128), F32)]
    scratch += [pltpu.VMEM((256, 256), F32), pltpu.VMEM((256, 256), BF16), pltpu.VMEM((256, 256), BF16)]
    scratch += [pltpu.VMEM((256, 1024), F32), pltpu.VMEM((256, 1024), F32), pltpu.VMEM((256, 512), F32)]
    scratch += [pltpu.VMEM((4, 128, 256), F32), pltpu.VMEM((6, 8, 256), F32)]
    scratch += [pltpu.VMEM((8, 256), F32), pltpu.VMEM((8, 128), F32)]
    scratch += [pltpu.VMEM((4, 4, 136, 128), F32)] * 2 + [pltpu.VMEM((4, 4, 128, 128), F32)] * 2
    scratch += [pltpu.VMEM((2, 136, 128), F32), pltpu.VMEM((4, 136, 128), F32)]
    scratch += [pltpu.VMEM((128, 128), F32)] * 2
    scratch += [pltpu.VMEM((128, 1024), F32), pltpu.VMEM((128, 1024), F32), pltpu.VMEM((128, 512), F32)]
    scratch += [pltpu.VMEM((56, 128), F32)]
    scratch += [pltpu.VMEM((16, 8, 128), F32), pltpu.VMEM((8, 8, 128), F32)]
    sems = [(5,), (5,), (4, 4), (4, 4), (4, 4), (4, 4), (4,), (4,), (3,), (3,), (2,), (2,)]
    sems += [(1,)] * 4
    scratch += [pltpu.SemaphoreType.DMA(s) for s in sems]
    outs = pl.pallas_call(
        kernel,
        out_shape=held,
        in_specs=[anywhere] * 7,
        out_specs=[pl.BlockSpec(memory_space=pltpu.VMEM)] * 5,
        scratch_shapes=scratch,
        compiler_params=pltpu.CompilerParams(
            collective_id=0, has_side_effects=True, vmem_limit_bytes=60 * 2**20
        ),
    )(*args)
    return pl.pallas_call(
        settle,
        out_shape=results,
        in_specs=[anywhere] * 5,
        out_specs=[anywhere] * 5,
        scratch_shapes=[pltpu.SemaphoreType.DMA((12,))],
        compiler_params=pltpu.CompilerParams(vmem_limit_bytes=48 * 2**20),
    )(*outs)


def solution(mesh):
    finer = Mesh(
        mesh.devices.reshape(4, 4, 2, mesh.shape["head"]), ("seq_0", "seq_1", "seq_2", "head")
    )
    wide = P(SEQ, "head")
    return jax.shard_map(
        shards,
        mesh=finer,
        in_specs=(wide, wide, wide, wide, P("head", SEQ), P(None, "head", SEQ), P(SEQ)),
        out_specs=(wide, wide, wide, P(None, "head", SEQ), P("head", SEQ)),
        check_vma=False,
    )
```

```python
import functools

import jax
import jax.numpy as jnp
from jax import lax
from jax.experimental import pallas as pl
from jax.experimental.pallas import tpu as pltpu
from jax.sharding import Mesh
from jax.sharding import PartitionSpec as P

SEQ = ("seq_0", "seq_1", "seq_2")
MESH = pl.DeviceIdType.MESH
F32 = jnp.float32
BF16 = jnp.bfloat16
NEG = -1e30

NN = (((1,), (0,)), ((), ()))
NT = (((1,), (1,)), ((), ()))
TN = (((0,), (0,)), ((), ()))


def dot(a, b, dims):
    return lax.dot_general(a, b, dims, preferred_element_type=F32)


def split(a):
    hi = a.astype(BF16)
    return hi, (a - hi.astype(F32)).astype(BF16)


def prefix(a, lane):
    shift = 1
    while shift < a.shape[1]:
        a = a + jnp.where(lane >= shift, pltpu.roll(a, shift, 1), 0.0)
        shift *= 2
    return a


def suffix(a, lane):
    size = a.shape[1]
    shift = 1
    while shift < size:
        a = a + jnp.where(lane < size - shift, pltpu.roll(a, size - shift, 1), 0.0)
        shift *= 2
    return a


def kernel(
    q_hbm, k_hbm, v_hbm, g_hbm, lg_hbm, lw_hbm, ds_hbm,
    gq_out, gk_out, gv_out, glw_out, glg_out,
    q_in, k_in, v_in, g_in, lg_in, lw_in, ds_in, load_sem,
    sq, sk, sv, sg, ss, rq, rk, rv, rg, rs,
    qb, kb, vb, gb, vt, gt,
    gates, doc, cum, resets, fs, de, wts, cm, bias, pt, rt,
    gq, gk, gv, gvt, glw, drift, small,
    ys, yr, zs, zr, xs, xr, ein, xin,
    bq, bk, bv, bs,
    a_buf, b_buf,
    in_send, in_recv, y1_send, y1_recv, y2_send, y2_recv, x_send, x_recv,
    out_send, out_recv, last_send, last_recv, a_send, a_recv, b_send, b_recv,
):
    x, y, c, z = (lax.axis_index(n) for n in ("seq_0", "seq_1", "seq_2", "head"))
    other = 1 - c
    chip = x * 4 + y
    group = z * 2 + c

    def remote(src, dst, send, recv, **to):
        return pltpu.make_async_remote_copy(
            src_ref=src, dst_ref=dst, send_sem=send, recv_sem=recv,
            device_id=to, device_id_type=MESH,
        )

    loads = [
        pltpu.make_async_copy(src, dst, load_sem.at[n])
        for n, (src, dst) in enumerate((
            (ds_hbm, ds_in), (lg_hbm, lg_in), (lw_hbm, lw_in), (k_hbm, k_in),
            (v_hbm, v_in), (g_hbm, g_in), (q_hbm, q_in),
        ))
    ]
    for load in loads:
        load.start()

    barrier = pltpu.get_barrier_semaphore()
    for step in range(1, 4):
        for axis, place in (("seq_1", y), ("seq_0", x)):
            pl.semaphore_signal(
                barrier, inc=1, device_id={axis: (place + step) % 4}, device_id_type=MESH
            )
    for step in range(1, 8):
        peer = (group + step) % 8
        pl.semaphore_signal(
            barrier, inc=1, device_id={"head": peer // 2, "seq_2": peer % 2}, device_id_type=MESH
        )

    q_cols = pl.ds(pl.multiple_of(other * 1024, 1024), 1024)
    v_cols = pl.ds(pl.multiple_of(other * 512, 512), 512)
    own_q = pl.ds(pl.multiple_of(c * 1024, 1024), 1024)
    own_v = pl.ds(pl.multiple_of(c * 512, 512), 512)
    own_rows = pl.ds(pl.multiple_of(c * 128, 128), 128)
    other_rows = pl.ds(pl.multiple_of(other * 128, 128), 128)
    own_heads = pl.ds(pl.multiple_of(c * 8, 8), 8)
    other_heads = pl.ds(pl.multiple_of(other * 8, 8), 8)
    for load in loads[:3]:
        load.wait()
    ds_row = jnp.broadcast_to(ds_in[...].astype(F32), (8, 128))
    ss[0:8, :] = lg_in[other_heads, :]
    for level in range(6):
        ss[8 + 8 * level : 16 + 8 * level, :] = lw_in[level, other_heads, :]
    ss[56:64, :] = ds_row
    loads[3].wait()
    sk[...] = k_in[:, q_cols].astype(F32)
    loads[4].wait()
    sv[...] = v_in[:, v_cols].astype(F32)
    loads[5].wait()
    sg[...] = g_in[:, v_cols].astype(F32)
    loads[6].wait()
    sq[...] = q_in[:, q_cols].astype(F32)

    pl.semaphore_wait(barrier, 13)
    swaps = [
        remote(src, dst, in_send.at[n], in_recv.at[n], seq_2=other)
        for n, (src, dst) in enumerate(((ss, rs), (sk, rk), (sv, rv), (sg, rg), (sq, rq)))
    ]
    for swap in swaps:
        swap.start()

    kb[own_rows, :] = k_in[:, own_q]
    vb[own_rows, :] = v_in[:, own_v]
    gb[own_rows, :] = g_in[:, own_v]
    qb[own_rows, :] = q_in[:, own_q]
    gates[:, own_rows] = lg_in[own_heads, :]
    for level in range(6):
        wts[level, :, own_rows] = lw_in[level, own_heads, :]
    doc[:, own_rows] = ds_row
    ein[...] = jnp.zeros_like(ein)
    xin[...] = jnp.zeros_like(xin)
    pt[128:256, 0:128] = jnp.zeros((128, 128), BF16)
    rt[128:256, 0:128] = jnp.zeros((128, 128), BF16)

    zero_slab = jnp.zeros((128, 128), F32)
    for level, absent in ((0, y % 2 == 0), (1, y < 2), (2, x == 0)):

        @pl.when(absent)
        def _():
            for pair in range(4):
                zr[pair, level] = zero_slab

    swaps[0].wait_recv()
    gates[:, other_rows] = rs[0:8, :]
    for level in range(6):
        wts[level, :, other_rows] = rs[8 + 8 * level : 16 + 8 * level, :]
    doc[:, other_rows] = rs[56:64, :]
    lane = lax.broadcasted_iota(jnp.int32, (8, 256), 1)
    cum_now = prefix(gates[...], lane)
    reset = prefix(doc[...], lane)
    total = cum_now[:, 255:256]
    reset_total = reset[:, 255:256]
    cum[...] = cum_now
    resets[...] = reset
    fs[...] = jnp.where(reset == 0.0, jnp.exp(cum_now), 0.0)
    de[...] = jnp.where(reset == reset_total, jnp.exp(total - cum_now), 0.0)
    decay = jnp.broadcast_to(jnp.where(reset_total == 0.0, jnp.exp(total), 0.0), (8, 128))
    small[...] = decay
    def masks():
        columns = jnp.transpose(
            jnp.concatenate([cum[...], resets[...], jnp.zeros((112, 256), F32)], axis=0)
        )
        for head in range(8):
            cm[head] = jnp.broadcast_to(columns[:, head : head + 1], (256, 128))
        reset_col = jnp.broadcast_to(columns[:, 8:9], (256, 128))
        for half in range(2):
            reset_row = jnp.broadcast_to(resets[0:1, 128 * half : 128 * half + 128], (256, 128))
            s_pos = lax.broadcasted_iota(jnp.int32, (256, 128), 0)
            t_pos = lax.broadcasted_iota(jnp.int32, (256, 128), 1) + 128 * half
            bias[:, 128 * half : 128 * half + 128] = jnp.where(
                (t_pos >= s_pos) & (reset_col == reset_row), 0.0, NEG
            )

    def head_cols(pair, i):
        return pl.ds(pl.multiple_of(pair * 256 + i * 128, 128), 128)

    def pair_cols(pair):
        return pl.ds(pl.multiple_of(pair * 128, 128), 128)

    def sent(kind, at_y):
        return (True, x > 0, at_y % 2 == 1, at_y >= 2)[kind]

    def y1_copy(pair, kind, at_y):
        rows = 136 if kind == 0 else 128
        return remote(
            ys.at[pair, kind, pl.ds(0, rows)], yr.at[at_y, kind, pl.ds(0, rows)],
            y1_send.at[pair, kind], y1_recv.at[at_y, kind], seq_1=pair,
        )

    def place(pair, kind, i, slab):
        rows = pl.ds(64 * i, 64)

        @pl.when(pair == y)
        def _():
            yr[y, kind, rows] = slab

        @pl.when(pair != y)
        def _():
            ys[pair, kind, rows] = slab

    def hand_over(pair, kind):
        @pl.when((pair != y) & sent(kind, y))
        def _():
            y1_copy(pair, kind, y).start()

    def state_fwd(pair):
        vt[pair] = jnp.transpose(vb[:, pair_cols(pair)].astype(F32))
        for i in range(2):
            head = pl.ds(pair * 2 + i, 1)
            value_hi, value_lo = split(vt[pair, pl.ds(64 * i, 64)] * de[head, :])
            state = dot(
                jnp.concatenate([value_hi, value_lo], axis=0), kb[:, head_cols(pair, i)], NN
            )
            place(pair, 0, i, state[0:64] + state[64:128])
            row = small[head, :]

            @pl.when(pair == y)
            def _():
                yr[y, 0, 128 + i : 129 + i] = row

            @pl.when(pair != y)
            def _():
                ys[pair, 0, 128 + i : 129 + i] = row

        hand_over(pair, 0)

    def state_back(pair):
        gt[pair] = jnp.transpose(gb[:, pair_cols(pair)].astype(F32))
        for i in range(2):
            head = pl.ds(pair * 2 + i, 1)
            hi, lo = split(gt[pair, pl.ds(64 * i, 64)] * (fs[head, :] * wts[5, head, :]))
            back = dot(jnp.concatenate([hi, lo], axis=0), qb[:, head_cols(pair, i)], NN)
            place(pair, 1, i, back[0:64] + back[64:128])
        hand_over(pair, 1)

    def state_near(pair):
        for i in range(2):
            head = pl.ds(pair * 2 + i, 1)
            grad = gt[pair, pl.ds(64 * i, 64)]
            parts = [split(grad * (fs[head, :] * wts[level, head, :])) for level in (3, 4)]
            back = dot(
                jnp.concatenate([p[0] for p in parts] + [p[1] for p in parts], axis=0),
                qb[:, head_cols(pair, i)], NN,
            )
            for n in range(2):
                place(
                    pair, 2 + n, i, back[64 * n : 64 * n + 64] + back[128 + 64 * n : 192 + 64 * n]
                )
        hand_over(pair, 2)
        hand_over(pair, 3)

    def intra(pair):
        for i in range(2):
            number = pair * 2 + i
            head = pl.ds(number, 1)
            rows = pl.ds(64 * i, 64)
            query = qb[:, head_cols(pair, i)]
            key = kb[:, head_cols(pair, i)]
            grad = gb[:, pair_cols(pair)]
            value = vb[:, pair_cols(pair)]
            mine = lax.broadcasted_iota(jnp.int32, (64, 128), 1) // 64 == i
            weight = [wts[level, head, :] for level in range(3)]
            span = lax.broadcasted_iota(jnp.int32, (1, 256), 1) // 64
            cum_row = cum[head, :]
            level_rows = [jnp.zeros((1, 256), F32) for level in range(3)]
            drift_row = jnp.zeros((1, 256), F32)
            for b in range(4):
                low = 0 if b < 2 else 128
                blk = slice(64 * b, 64 * b + 64)
                score = dot(key[blk], query[low:256], NT)
                pair_dot = dot(
                    jnp.where(mine, value[blk], jnp.zeros((64, 128), BF16)), grad[low:256], NT
                )
                col = cm[number, blk, :]
                if low == 0:
                    col = jnp.concatenate([col, col], axis=1)
                decayed = jnp.exp((cum_row[:, low:256] - col) + bias[blk, low:256])
                at = span[:, low:256]
                near = (at == b).astype(jnp.int32), ((at ^ 1) == b).astype(jnp.int32)
                mix = jnp.where(
                    near[0] == 1, weight[0][:, low:256],
                    jnp.where(near[1] == 1, weight[1][:, low:256], weight[2][:, low:256]),
                )
                scored = decayed * score
                joint = jnp.sum(scored * pair_dot, axis=0, keepdims=True)
                prob = (scored * mix).astype(BF16)
                pt[blk, low:256] = prob
                rt[blk, low:256] = (decayed * mix * pair_dot).astype(BF16)
                drifted = jnp.sum(prob.astype(F32) * pair_dot, axis=0, keepdims=True)
                if low:
                    pad = jnp.zeros((1, 128), F32)
                    joint = jnp.concatenate([pad, joint], axis=1)
                    drifted = jnp.concatenate([pad, drifted], axis=1)
                drift_row = drift_row + drifted
                level_rows[0] = level_rows[0] + jnp.where(span == b, joint, 0.0)
                level_rows[1] = level_rows[1] + jnp.where((span ^ 1) == b, joint, 0.0)
                level_rows[2] = level_rows[2] + jnp.where(
                    (span != b) & ((span ^ 1) != b), joint, 0.0
                )
            for level in range(3):
                glw[level, head, :] = level_rows[level]
            drift[head, :] = drift_row
            gvt[pair, rows] = dot(gt[pair, rows].astype(BF16), pt[...], NT)
            gk[:, head_cols(pair, i)] = dot(rt[...], query, NN)
            gq[:, head_cols(pair, i)] = dot(rt[...], key, TN)

    def y2_copy(to_y, kind, src):
        return remote(
            src, zr.at[y, kind], y2_send.at[to_y, kind], y2_recv.at[y, kind], seq_1=to_y
        )

    def y2_source(to_y, kind):
        if kind == 0:
            return yr.at[to_y - 1, 0, pl.ds(0, 128)]
        return zs.at[to_y, kind]

    def hand_back(to_y, kind):
        def go():
            @pl.when(to_y != y)
            def _():
                y2_copy(to_y, kind, y2_source(to_y, kind)).start()

            @pl.when(to_y == y)
            def _():
                zr[y, kind] = y2_source(to_y, kind)[...]

        if kind == 2:
            pl.when(x > 0)(go)
        else:
            go()

    def y1_wait(kind):
        for at_y in range(4):
            here = sent(kind, at_y)
            if here is False:
                continue

            @pl.when((y != at_y) & here)
            def _():
                y1_copy(y, kind, at_y).wait_recv()

    def x_copy(to_x, kind):
        return remote(xs.at[kind], xr.at[x], x_send.at[to_x], x_recv.at[x], seq_0=to_x)

    def decays(i):
        return [yr[n, 0, 128 + i : 129 + i] for n in range(4)]

    def combine_fwd():
        y1_wait(0)
        for i in range(2):
            rows = slice(64 * i, 64 * i + 64)
            dec = decays(i)
            both = dec[1] * yr[0, 0, rows] + yr[1, 0, rows]
            zs[2, 1, rows] = both
            after = dec[2] * both
            zs[3, 1, rows] = after
            xs[0, rows] = dec[3] * (after + yr[2, 0, rows]) + yr[3, 0, rows]
            all_decay = dec[0] * dec[1] * (dec[2] * dec[3])
            xs[0, 128 + i : 129 + i] = all_decay
            xs[1, 128 + i : 129 + i] = all_decay
        for to_x in range(4):

            @pl.when(to_x > x)
            def _():
                x_copy(to_x, 0).start()

        hand_back(1, 0)
        hand_back(3, 0)
        hand_back(2, 1)
        hand_back(3, 1)

    def combine_back():
        y1_wait(1)

        @pl.when(x > 0)
        def _():
            for i in range(2):
                rows = slice(64 * i, 64 * i + 64)
                dec = decays(i)
                back = yr[2, 1, rows] + dec[2] * yr[3, 1, rows]
                back = yr[1, 1, rows] + dec[1] * back
                xs[1, rows] = yr[0, 1, rows] + dec[0] * back

        for to_x in range(4):

            @pl.when(to_x < x)
            def _():
                x_copy(to_x, 1).start()


    def take(acc, at_x):
        remote(
            xs.at[0], xr.at[at_x], x_send.at[at_x], x_recv.at[at_x], seq_0=at_x
        ).wait_recv()
        for i in range(2):
            rows = slice(64 * i, 64 * i + 64)
            acc[rows] = xr[at_x, 128 + i : 129 + i] * acc[rows] + xr[at_x, rows]

    def enter_far():
        for at_x in range(4):
            pl.when(at_x < x)(functools.partial(take, ein, at_x))
        for i in range(2):
            rows = slice(64 * i, 64 * i + 64)
            dec = decays(i)
            into = ein[rows]
            for at_y in range(4):
                zs[at_y, 2, rows] = into
                into = dec[at_y] * into
        for step in (2, 1, 3, 0):
            hand_back((y + step) % 4, 2)

    def leave_far():
        y1_wait(2)
        y1_wait(3)
        for at_x in range(3, -1, -1):
            pl.when(at_x > x)(functools.partial(take, xin, at_x))
        for i in range(2):
            rows = slice(64 * i, 64 * i + 64)
            dec = decays(i)
            late = xin[rows]
            zs[3, 3, rows] = late
            late = dec[3] * late
            zs[2, 3, rows] = late + yr[3, 2, rows]
            late = dec[2] * late + (yr[2, 3, rows] + dec[2] * yr[3, 3, rows])
            zs[1, 3, rows] = late
            zs[0, 3, rows] = dec[1] * late + yr[1, 2, rows]
        for step in (2, 1, 3, 0):
            hand_back((y + step) % 4, 3)

    def back_copy(pair, kind):
        if kind == 2:
            cols, src, dst = pair_cols(pair), gv, bv
        else:
            cols = pl.ds(pl.multiple_of(pair * 256, 256), 256)
            src, dst = ((gq, bq), (gk, bk))[kind]
        return remote(
            src.at[other_rows, cols], dst.at[:, cols],
            out_send.at[kind], out_recv.at[kind], seq_2=other,
        )

    def y2_wait(pair, kinds):
        for kind in kinds:
            here = (y % 2 == 1, y >= 2, x > 0, True)[kind]

            @pl.when((pair != y) & here)
            def _():
                remote(
                    zs.at[0, kind], zr.at[pair, kind], y2_send.at[0, kind],
                    y2_recv.at[pair, kind], seq_1=pair,
                ).wait_recv()

    def cross_in(pair):
        y2_wait(pair, (0, 1, 2))
        for i in range(2):
            head = pl.ds(pair * 2 + i, 1)
            rows = pl.ds(64 * i, 64)
            grad = gt[pair, rows]
            enter_hi, enter_lo = split(
                jnp.concatenate([zr[pair, n, rows] for n in range(3)], axis=0)
            )
            mixed = dot(
                jnp.concatenate([enter_hi, enter_lo], axis=0), qb[:, head_cols(pair, i)], NT
            )
            drift_row = drift[head, :]
            for n in range(3):
                state_row = mixed[64 * n : 64 * n + 64] + mixed[192 + 64 * n : 256 + 64 * n]
                level_row = fs[head, :] * jnp.sum(state_row * grad, axis=0, keepdims=True)
                glw[3 + n, head, :] = level_row
                drift_row = drift_row + wts[3 + n, head, :] * level_row
            drift[head, :] = drift_row
            weighted_hi, weighted_lo = split(
                jnp.concatenate(
                    [grad * (fs[head, :] * wts[3 + n, head, :]) for n in range(3)], axis=0
                )
            )
            gq[:, head_cols(pair, i)] = gq[:, head_cols(pair, i)] + dot(
                jnp.concatenate([weighted_hi, weighted_lo, weighted_hi], axis=0),
                jnp.concatenate([enter_hi, enter_hi, enter_lo], axis=0), TN,
            )
        back_copy(pair, 0).start()
        wide = pl.ds(pl.multiple_of(pair * 256, 256), 256)
        out_wide = pl.ds(pl.multiple_of(c * 1024 + pair * 256, 256), 256)
        gq_out[:, out_wide] = gq[own_rows, wide].astype(BF16)

    def cross_out(pair):
        y2_wait(pair, (3,))
        for i in range(2):
            head = pl.ds(pair * 2 + i, 1)
            rows = pl.ds(64 * i, 64)
            leave_hi, leave_lo = split(zr[pair, 3, rows])
            left = dot(
                jnp.concatenate([leave_hi, leave_lo], axis=0), kb[:, head_cols(pair, i)], NT
            )
            value_grad = gvt[pair, rows] + de[head, :] * (left[0:64] + left[64:128])
            gvt[pair, rows] = value_grad
            drift[head, :] = drift[head, :] - jnp.sum(
                vt[pair, rows] * value_grad, axis=0, keepdims=True
            )

    def cross_grad(pair):
        for i in range(2):
            head = pl.ds(pair * 2 + i, 1)
            rows = pl.ds(64 * i, 64)
            leave_hi, leave_lo = split(zr[pair, 3, rows])
            ended_hi, ended_lo = split(vt[pair, rows] * de[head, :])
            gk[:, head_cols(pair, i)] = gk[:, head_cols(pair, i)] + dot(
                jnp.concatenate([ended_hi, ended_lo, ended_hi], axis=0),
                jnp.concatenate([leave_hi, leave_hi, leave_lo], axis=0), TN,
            )
        gv[:, pair_cols(pair)] = jnp.transpose(gvt[pair])
        back_copy(pair, 1).start()
        back_copy(pair, 2).start()
        wide = pl.ds(pl.multiple_of(pair * 256, 256), 256)
        out_wide = pl.ds(pl.multiple_of(c * 1024 + pair * 256, 256), 256)
        out_narrow = pl.ds(pl.multiple_of(c * 512 + pair * 128, 128), 128)
        gk_out[:, out_wide] = gk[own_rows, wide].astype(BF16)
        gv_out[:, out_narrow] = gv[own_rows, pair_cols(pair)].astype(BF16)

    def loop(low, high, body):
        def step(n, carry):
            body(n)
            return carry

        lax.fori_loop(low, high, step, 0)

    def toward(n):
        return (y + jnp.where(n == 2, 3, jnp.where(n == 3, 0, 2 - n))) % 4

    def nearby(n):
        return (y + jnp.where(n == 2, 3, jnp.where(n == 3, 2, n))) % 4

    swaps[1].wait_recv()
    kb[other_rows, :] = rk[...].astype(BF16)
    swaps[2].wait_recv()
    vb[other_rows, :] = rv[...].astype(BF16)
    loop(0, 4, lambda n: state_fwd(toward(n)))
    swaps[3].wait_recv()
    gb[other_rows, :] = rg[...].astype(BF16)
    swaps[4].wait_recv()
    qb[other_rows, :] = rq[...].astype(BF16)
    loop(0, 4, lambda n: state_back(toward(n)))
    loop(0, 4, lambda n: state_near(toward(n)))
    combine_fwd()
    masks()
    loop(0, 1, intra)
    combine_back()
    loop(1, 3, intra)
    enter_far()
    loop(3, 4, intra)
    leave_far()
    loop(0, 4, lambda n: cross_in(nearby(n)))
    loop(0, 4, lambda n: cross_out(nearby(n)))
    lane = lax.broadcasted_iota(jnp.int32, (8, 256), 1)
    tail = suffix(drift[...], lane)
    drift[...] = tail
    bs_out = remote(small.at[:, :], bs.at[pl.ds(48, 8), :], last_send.at[1], last_recv.at[1], seq_2=other)
    tile = lax.broadcasted_iota(jnp.int32, (8, 128), 1)
    head_total = jnp.broadcast_to(tail[:, 0:1], (8, 128))
    head_square = jnp.broadcast_to(jnp.sum(tail * tail, axis=1, keepdims=True), (8, 128))
    head_sum = jnp.broadcast_to(jnp.sum(tail, axis=1, keepdims=True), (8, 128))
    a_buf[chip] = jnp.where(tile == 0, head_total, jnp.where(tile == 1, head_square, head_sum))

    def a_copy(step):
        peer = (chip + step) % 16
        return remote(
            a_buf.at[chip], a_buf.at[chip], a_send.at[0], a_recv.at[0],
            seq_0=peer // 4, seq_1=peer % 4,
        )

    for step in range(1, 16):
        a_copy(step).start()
    small[...] = drift[:, other_rows]
    for level in range(6):
        ss_rows = slice(8 * level, 8 * level + 8)
        ys[y, 1, ss_rows] = glw[level, :, other_rows]
    glw_copy = remote(
        ys.at[y, 1, pl.ds(0, 48)], bs.at[pl.ds(0, 48), :], last_send.at[0], last_recv.at[0],
        seq_2=other,
    )
    glw_copy.start()
    bs_out.start()
    for level in range(6):
        glw_out[level, own_heads, :] = glw[level, :, own_rows]

    loop(0, 4, cross_grad)
    def back_whole(kind):
        src, dst = ((gq, bq), (gk, bk), (gv, bv))[kind]
        return remote(
            src.at[other_rows, :], dst, out_send.at[kind], out_recv.at[kind], seq_2=other
        )

    for kind in range(3):
        back_whole(kind).wait_recv()
    other_q = pl.ds(pl.multiple_of(other * 1024, 1024), 1024)
    other_v = pl.ds(pl.multiple_of(other * 512, 512), 512)
    gq_out[:, other_q] = bq[...].astype(BF16)
    gk_out[:, other_q] = bk[...].astype(BF16)
    gv_out[:, other_v] = bv[...].astype(BF16)
    glw_copy.wait_recv()
    for level in range(6):
        glw_out[level, other_heads, :] = bs[8 * level : 8 * level + 8, :]

    a_whole = remote(
        a_buf.at[pl.ds(0, 15)], a_buf.at[pl.ds(0, 15)], a_send.at[0], a_recv.at[0], seq_2=other
    )
    a_whole.wait_recv()
    run = jnp.zeros((8, 1), F32)
    later = jnp.zeros((8, 1), F32)
    squares = jnp.zeros((8, 1), F32)
    for at in range(15, -1, -1):
        now = a_buf[at]
        later = later + run * (chip == at).astype(F32)
        squares = squares + now[:, 1:2] + run * (2.0 * now[:, 2:3] + 256.0 * run)
        run = run + now[:, 0:1]
    whole = jnp.broadcast_to(jnp.sum(squares, axis=0, keepdims=True), (8, 128))
    b_buf[group] = jnp.where(tile < 64, jnp.broadcast_to(later, (8, 128)), whole)

    def b_peer(step):
        peer = (group + step) % 8
        return {"head": peer // 2, "seq_2": peer % 2}

    for step in range(1, 8):
        to = b_peer(step)
        remote(
            b_buf.at[group], b_buf.at[group], b_send.at[0], b_recv.at[0], **to
        ).start()
    b_whole = remote(
        b_buf.at[pl.ds(0, 7)], b_buf.at[pl.ds(0, 7)], b_send.at[0], b_recv.at[0], seq_2=other
    )
    b_whole.wait_recv()
    total_square = jnp.zeros((8, 128), F32)
    for at in range(8):
        total_square = total_square + b_buf[at]
    factor = jnp.minimum(1.0, lax.rsqrt(total_square[:, 64:65] / (64 * 4096) + 1e-06))
    glg_out[own_heads, :] = (drift[:, own_rows] + later) * factor
    bs_out.wait_recv()
    glg_out[other_heads, :] = (bs[48:56, :] + b_buf[z * 2 + other][:, 0:1]) * factor

    for swap in swaps:
        swap.wait_send()
    for pair in range(4):
        for kind in range(4):

            @pl.when((y != pair) & sent(kind, y))
            def _():
                y1_copy(pair, kind, y).wait_send()

            back = (pair % 2 == 1, pair >= 2, x > 0, True)[kind]
            if back is not False:

                @pl.when((y != pair) & back)
                def _():
                    y2_copy(pair, kind, y2_source(pair, kind)).wait_send()

        @pl.when(pair != x)
        def _():
            x_copy(pair, 0).wait_send()

    for kind in range(3):
        back_whole(kind).wait_send()
    glw_copy.wait_send()
    bs_out.wait_send()
    a_whole.wait_send()
    b_whole.wait_send()


def settle(*refs):
    source, target, sem = refs[:5], refs[5:10], refs[10]
    stores = []
    for n in range(5):
        cuts = 4 if n < 2 else 2 if n == 2 else 1
        rows = source[n].shape[0] // cuts
        for m in range(cuts):
            at = pl.ds(rows * m, rows)
            stores.append(
                pltpu.make_async_copy(source[n].at[at], target[n].at[at], sem.at[len(stores)])
            )
    for store in stores:
        store.start()
    for store in stores:
        store.wait()


def shards(queries, keys, values, out_grad, log_gate, level_weight, doc_start):
    args = (queries, keys, values, out_grad, log_gate, level_weight, doc_start.reshape(1, -1))
    anywhere = pl.BlockSpec(memory_space=pl.ANY)
    results = tuple(
        jax.ShapeDtypeStruct(a.shape, a.dtype)
        for a in (queries, keys, values, level_weight, log_gate)
    )
    held = tuple(pltpu.VMEM(r.shape, r.dtype) for r in results)
    scratch = [pltpu.VMEM(a.shape, a.dtype) for a in args] + [pltpu.SemaphoreType.DMA((7,))]
    swap = [(128, 1024), (128, 1024), (128, 512), (128, 512), (64, 128)]
    scratch += [pltpu.VMEM(s, F32) for s in swap * 2]
    scratch += [pltpu.VMEM(s, BF16) for s in ((256, 1024), (256, 1024), (256, 512), (256, 512))]
    scratch += [pltpu.VMEM((4, 128, 256), F32)] * 2
    scratch += [pltpu.VMEM((8, 256), F32)] * 6
    scratch += [pltpu.VMEM((6, 8, 256), F32), pltpu.VMEM((8, 256, 128), F32)]
    scratch += [pltpu.VMEM((256, 256), F32), pltpu.VMEM((256, 256), BF16), pltpu.VMEM((256, 256), BF16)]
    scratch += [pltpu.VMEM((256, 1024), F32), pltpu.VMEM((256, 1024), F32), pltpu.VMEM((256, 512), F32)]
    scratch += [pltpu.VMEM((4, 128, 256), F32), pltpu.VMEM((6, 8, 256), F32)]
    scratch += [pltpu.VMEM((8, 256), F32), pltpu.VMEM((8, 128), F32)]
    scratch += [pltpu.VMEM((4, 4, 136, 128), F32)] * 2 + [pltpu.VMEM((4, 4, 128, 128), F32)] * 2
    scratch += [pltpu.VMEM((2, 136, 128), F32), pltpu.VMEM((4, 136, 128), F32)]
    scratch += [pltpu.VMEM((128, 128), F32)] * 2
    scratch += [pltpu.VMEM((128, 1024), F32), pltpu.VMEM((128, 1024), F32), pltpu.VMEM((128, 512), F32)]
    scratch += [pltpu.VMEM((56, 128), F32)]
    scratch += [pltpu.VMEM((16, 8, 128), F32), pltpu.VMEM((8, 8, 128), F32)]
    sems = [(5,), (5,), (4, 4), (4, 4), (4, 4), (4, 4), (4,), (4,), (3,), (3,), (2,), (2,)]
    sems += [(1,)] * 4
    scratch += [pltpu.SemaphoreType.DMA(s) for s in sems]
    outs = pl.pallas_call(
        kernel,
        out_shape=held,
        in_specs=[anywhere] * 7,
        out_specs=[pl.BlockSpec(memory_space=pltpu.VMEM)] * 5,
        scratch_shapes=scratch,
        compiler_params=pltpu.CompilerParams(
            collective_id=0, has_side_effects=True, vmem_limit_bytes=60 * 2**20
        ),
    )(*args)
    return pl.pallas_call(
        settle,
        out_shape=results,
        in_specs=[anywhere] * 5,
        out_specs=[anywhere] * 5,
        scratch_shapes=[pltpu.SemaphoreType.DMA((12,))],
        compiler_params=pltpu.CompilerParams(vmem_limit_bytes=48 * 2**20),
    )(*outs)


def solution(mesh):
    finer = Mesh(
        mesh.devices.reshape(4, 4, 2, mesh.shape["head"]), ("seq_0", "seq_1", "seq_2", "head")
    )
    wide = P(SEQ, "head")
    return jax.shard_map(
        shards,
        mesh=finer,
        in_specs=(wide, wide, wide, wide, P("head", SEQ), P(None, "head", SEQ), P(SEQ)),
        out_specs=(wide, wide, wide, P(None, "head", SEQ), P("head", SEQ)),
        check_vma=False,
    )
```

```python
import functools

import jax
import jax.numpy as jnp
from jax import lax
from jax.experimental import pallas as pl
from jax.experimental.pallas import tpu as pltpu
from jax.sharding import Mesh
from jax.sharding import PartitionSpec as P

SEQ = ("seq_0", "seq_1", "seq_2")
MESH = pl.DeviceIdType.MESH
F32 = jnp.float32
BF16 = jnp.bfloat16
NEG = -1e30

NN = (((1,), (0,)), ((), ()))
NT = (((1,), (1,)), ((), ()))
TN = (((0,), (0,)), ((), ()))


def dot(a, b, dims):
    return lax.dot_general(a, b, dims, preferred_element_type=F32)


def split(a):
    hi = a.astype(BF16)
    return hi, (a - hi.astype(F32)).astype(BF16)


def prefix(a, lane):
    shift = 1
    while shift < a.shape[1]:
        a = a + jnp.where(lane >= shift, pltpu.roll(a, shift, 1), 0.0)
        shift *= 2
    return a


def suffix(a, lane):
    size = a.shape[1]
    shift = 1
    while shift < size:
        a = a + jnp.where(lane < size - shift, pltpu.roll(a, size - shift, 1), 0.0)
        shift *= 2
    return a


def kernel(
    q_hbm, k_hbm, v_hbm, g_hbm, lg_hbm, lw_hbm, ds_hbm,
    gq_out, gk_out, gv_out, glw_out, glg_out,
    q_in, k_in, v_in, g_in, lg_in, lw_in, ds_in, load_sem,
    sq, sk, sv, sg, ss, rq, rk, rv, rg, rs,
    qb, kb, vb, gb, vt, gt,
    gates, doc, cum, resets, fs, de, wts, cm, bias, pt, rt,
    gq, gk, gv, gvt, glw, drift, small,
    ys, yr, zs, zr, xs, xr, ein, xin,
    bq, bk, bv, bs,
    a_buf,
    in_send, in_recv, y1_send, y1_recv, y2_send, y2_recv, x_send, x_recv,
    out_send, out_recv, last_send, last_recv, a_send, a_recv,
):
    x, y, c, z = (lax.axis_index(n) for n in ("seq_0", "seq_1", "seq_2", "head"))
    other = 1 - c
    chip = x * 4 + y
    group = z * 2 + c

    def remote(src, dst, send, recv, **to):
        return pltpu.make_async_remote_copy(
            src_ref=src, dst_ref=dst, send_sem=send, recv_sem=recv,
            device_id=to, device_id_type=MESH,
        )

    loads = [
        pltpu.make_async_copy(src, dst, load_sem.at[n])
        for n, (src, dst) in enumerate((
            (ds_hbm, ds_in), (lg_hbm, lg_in), (lw_hbm, lw_in), (k_hbm, k_in),
            (v_hbm, v_in), (g_hbm, g_in), (q_hbm, q_in),
        ))
    ]
    for load in loads:
        load.start()

    barrier = pltpu.get_barrier_semaphore()
    for step in range(1, 4):
        for axis, place in (("seq_1", y), ("seq_0", x)):
            pl.semaphore_signal(
                barrier, inc=1, device_id={axis: (place + step) % 4}, device_id_type=MESH
            )
    for step in range(1, 8):
        peer = (group + step) % 8
        pl.semaphore_signal(
            barrier, inc=1, device_id={"head": peer // 2, "seq_2": peer % 2}, device_id_type=MESH
        )

    q_cols = pl.ds(pl.multiple_of(other * 1024, 1024), 1024)
    v_cols = pl.ds(pl.multiple_of(other * 512, 512), 512)
    own_q = pl.ds(pl.multiple_of(c * 1024, 1024), 1024)
    own_v = pl.ds(pl.multiple_of(c * 512, 512), 512)
    own_rows = pl.ds(pl.multiple_of(c * 128, 128), 128)
    other_rows = pl.ds(pl.multiple_of(other * 128, 128), 128)
    own_heads = pl.ds(pl.multiple_of(c * 8, 8), 8)
    other_heads = pl.ds(pl.multiple_of(other * 8, 8), 8)
    swaps = [
        remote(src, dst, in_send.at[n], in_recv.at[n], seq_2=other)
        for n, (src, dst) in enumerate(((ss, rs), (sk, rk), (sv, rv), (sg, rg), (sq, rq)))
    ]
    for load in loads[:3]:
        load.wait()
    ds_row = jnp.broadcast_to(ds_in[...].astype(F32), (8, 128))
    ss[0:8, :] = lg_in[other_heads, :]
    for level in range(6):
        ss[8 + 8 * level : 16 + 8 * level, :] = lw_in[level, other_heads, :]
    ss[56:64, :] = ds_row
    loads[3].wait()
    sk[...] = k_in[:, q_cols].astype(F32)
    loads[4].wait()
    sv[...] = v_in[:, v_cols].astype(F32)
    pl.semaphore_wait(barrier, 13)
    for swap in swaps[:3]:
        swap.start()
    loads[5].wait()
    sg[...] = g_in[:, v_cols].astype(F32)
    loads[6].wait()
    sq[...] = q_in[:, q_cols].astype(F32)
    for swap in swaps[3:]:
        swap.start()
    kb[own_rows, :] = k_in[:, own_q]
    vb[own_rows, :] = v_in[:, own_v]
    gb[own_rows, :] = g_in[:, own_v]
    qb[own_rows, :] = q_in[:, own_q]
    gates[:, own_rows] = lg_in[own_heads, :]
    for level in range(6):
        wts[level, :, own_rows] = lw_in[level, own_heads, :]
    doc[:, own_rows] = ds_row
    ein[...] = jnp.zeros_like(ein)
    xin[...] = jnp.zeros_like(xin)
    pt[128:256, 0:128] = jnp.zeros((128, 128), BF16)
    rt[128:256, 0:128] = jnp.zeros((128, 128), BF16)

    zero_slab = jnp.zeros((128, 128), F32)
    for level, absent in ((0, y % 2 == 0), (1, y < 2), (2, x == 0)):

        @pl.when(absent)
        def _():
            for pair in range(4):
                zr[pair, level] = zero_slab

    swaps[0].wait_recv()
    gates[:, other_rows] = rs[0:8, :]
    for level in range(6):
        wts[level, :, other_rows] = rs[8 + 8 * level : 16 + 8 * level, :]
    doc[:, other_rows] = rs[56:64, :]
    lane = lax.broadcasted_iota(jnp.int32, (8, 256), 1)
    cum_now = prefix(gates[...], lane)
    reset = prefix(doc[...], lane)
    total = cum_now[:, 255:256]
    reset_total = reset[:, 255:256]
    cum[...] = cum_now
    resets[...] = reset
    fs[...] = jnp.where(reset == 0.0, jnp.exp(cum_now), 0.0)
    de[...] = jnp.where(reset == reset_total, jnp.exp(total - cum_now), 0.0)
    decay = jnp.broadcast_to(jnp.where(reset_total == 0.0, jnp.exp(total), 0.0), (8, 128))
    small[...] = decay
    def masks():
        columns = jnp.transpose(
            jnp.concatenate([cum[...], resets[...], jnp.zeros((112, 256), F32)], axis=0)
        )
        for head in range(8):
            cm[head] = jnp.broadcast_to(columns[:, head : head + 1], (256, 128))
        reset_col = jnp.broadcast_to(columns[:, 8:9], (256, 128))
        for half in range(2):
            reset_row = jnp.broadcast_to(resets[0:1, 128 * half : 128 * half + 128], (256, 128))
            s_pos = lax.broadcasted_iota(jnp.int32, (256, 128), 0)
            t_pos = lax.broadcasted_iota(jnp.int32, (256, 128), 1) + 128 * half
            bias[:, 128 * half : 128 * half + 128] = jnp.where(
                (t_pos >= s_pos) & (reset_col == reset_row), 0.0, NEG
            )

    def head_cols(pair, i):
        return pl.ds(pl.multiple_of(pair * 256 + i * 128, 128), 128)

    def pair_cols(pair):
        return pl.ds(pl.multiple_of(pair * 128, 128), 128)

    def sent(kind, at_y):
        return (True, x > 0, at_y % 2 == 1, at_y >= 2)[kind]

    def y1_copy(pair, kind, at_y):
        rows = 136 if kind == 0 else 128
        return remote(
            ys.at[pair, kind, pl.ds(0, rows)], yr.at[at_y, kind, pl.ds(0, rows)],
            y1_send.at[pair, kind], y1_recv.at[at_y, kind], seq_1=pair,
        )

    def place(pair, kind, i, slab):
        rows = pl.ds(64 * i, 64)

        @pl.when(pair == y)
        def _():
            yr[y, kind, rows] = slab

        @pl.when(pair != y)
        def _():
            ys[pair, kind, rows] = slab

    def hand_over(pair, kind):
        @pl.when((pair != y) & sent(kind, y))
        def _():
            y1_copy(pair, kind, y).start()

    def state_fwd(pair):
        vt[pair] = jnp.transpose(vb[:, pair_cols(pair)].astype(F32))
        for i in range(2):
            head = pl.ds(pair * 2 + i, 1)
            value_hi, value_lo = split(vt[pair, pl.ds(64 * i, 64)] * de[head, :])
            state = dot(
                jnp.concatenate([value_hi, value_lo], axis=0), kb[:, head_cols(pair, i)], NN
            )
            place(pair, 0, i, state[0:64] + state[64:128])
            row = small[head, :]

            @pl.when(pair == y)
            def _():
                yr[y, 0, 128 + i : 129 + i] = row

            @pl.when(pair != y)
            def _():
                ys[pair, 0, 128 + i : 129 + i] = row

        hand_over(pair, 0)

    def state_back(pair):
        gt[pair] = jnp.transpose(gb[:, pair_cols(pair)].astype(F32))
        for i in range(2):
            head = pl.ds(pair * 2 + i, 1)
            hi, lo = split(gt[pair, pl.ds(64 * i, 64)] * (fs[head, :] * wts[5, head, :]))
            back = dot(jnp.concatenate([hi, lo], axis=0), qb[:, head_cols(pair, i)], NN)
            place(pair, 1, i, back[0:64] + back[64:128])
        hand_over(pair, 1)

    def state_near(pair):
        for i in range(2):
            head = pl.ds(pair * 2 + i, 1)
            grad = gt[pair, pl.ds(64 * i, 64)]
            parts = [split(grad * (fs[head, :] * wts[level, head, :])) for level in (3, 4)]
            back = dot(
                jnp.concatenate([p[0] for p in parts] + [p[1] for p in parts], axis=0),
                qb[:, head_cols(pair, i)], NN,
            )
            for n in range(2):
                place(
                    pair, 2 + n, i, back[64 * n : 64 * n + 64] + back[128 + 64 * n : 192 + 64 * n]
                )
        hand_over(pair, 2)
        hand_over(pair, 3)

    def intra(pair):
        for i in range(2):
            number = pair * 2 + i
            head = pl.ds(number, 1)
            rows = pl.ds(64 * i, 64)
            query = qb[:, head_cols(pair, i)]
            key = kb[:, head_cols(pair, i)]
            grad = gb[:, pair_cols(pair)]
            value = vb[:, pair_cols(pair)]
            mine = lax.broadcasted_iota(jnp.int32, (64, 128), 1) // 64 == i
            weight = [wts[level, head, :] for level in range(3)]
            span = lax.broadcasted_iota(jnp.int32, (1, 256), 1) // 64
            cum_row = cum[head, :]
            level_rows = [jnp.zeros((1, 256), F32) for level in range(3)]
            drift_row = jnp.zeros((1, 256), F32)
            for b in range(4):
                low = 0 if b < 2 else 128
                blk = slice(64 * b, 64 * b + 64)
                score = dot(key[blk], query[low:256], NT)
                pair_dot = dot(
                    jnp.where(mine, value[blk], jnp.zeros((64, 128), BF16)), grad[low:256], NT
                )
                col = cm[number, blk, :]
                if low == 0:
                    col = jnp.concatenate([col, col], axis=1)
                decayed = jnp.exp((cum_row[:, low:256] - col) + bias[blk, low:256])
                at = span[:, low:256]
                near = (at == b).astype(jnp.int32), ((at ^ 1) == b).astype(jnp.int32)
                mix = jnp.where(
                    near[0] == 1, weight[0][:, low:256],
                    jnp.where(near[1] == 1, weight[1][:, low:256], weight[2][:, low:256]),
                )
                scored = decayed * score
                joint = jnp.sum(scored * pair_dot, axis=0, keepdims=True)
                prob = (scored * mix).astype(BF16)
                pt[blk, low:256] = prob
                rt[blk, low:256] = (decayed * mix * pair_dot).astype(BF16)
                drifted = jnp.sum(prob.astype(F32) * pair_dot, axis=0, keepdims=True)
                if low:
                    pad = jnp.zeros((1, 128), F32)
                    joint = jnp.concatenate([pad, joint], axis=1)
                    drifted = jnp.concatenate([pad, drifted], axis=1)
                drift_row = drift_row + drifted
                level_rows[0] = level_rows[0] + jnp.where(span == b, joint, 0.0)
                level_rows[1] = level_rows[1] + jnp.where((span ^ 1) == b, joint, 0.0)
                level_rows[2] = level_rows[2] + jnp.where(
                    (span != b) & ((span ^ 1) != b), joint, 0.0
                )
            for level in range(3):
                glw[level, head, :] = level_rows[level]
            drift[head, :] = drift_row
            gvt[pair, rows] = dot(gt[pair, rows].astype(BF16), pt[...], NT)
            gk[:, head_cols(pair, i)] = dot(rt[...], query, NN)
            gq[:, head_cols(pair, i)] = dot(rt[...], key, TN)

    def y2_copy(to_y, kind, src):
        return remote(
            src, zr.at[y, kind], y2_send.at[to_y, kind], y2_recv.at[y, kind], seq_1=to_y
        )

    def y2_source(to_y, kind):
        if kind == 0:
            return yr.at[to_y - 1, 0, pl.ds(0, 128)]
        return zs.at[to_y, kind]

    def hand_back(to_y, kind):
        def go():
            @pl.when(to_y != y)
            def _():
                y2_copy(to_y, kind, y2_source(to_y, kind)).start()

            @pl.when(to_y == y)
            def _():
                zr[y, kind] = y2_source(to_y, kind)[...]

        if kind == 2:
            pl.when(x > 0)(go)
        else:
            go()

    def y1_wait(kind):
        for at_y in range(4):
            here = sent(kind, at_y)
            if here is False:
                continue

            @pl.when((y != at_y) & here)
            def _():
                y1_copy(y, kind, at_y).wait_recv()

    def x_copy(to_x, kind):
        return remote(xs.at[kind], xr.at[x], x_send.at[to_x], x_recv.at[x], seq_0=to_x)

    def decays(i):
        return [yr[n, 0, 128 + i : 129 + i] for n in range(4)]

    def combine_fwd():
        y1_wait(0)
        for i in range(2):
            rows = slice(64 * i, 64 * i + 64)
            dec = decays(i)
            both = dec[1] * yr[0, 0, rows] + yr[1, 0, rows]
            zs[2, 1, rows] = both
            after = dec[2] * both
            zs[3, 1, rows] = after
            xs[0, rows] = dec[3] * (after + yr[2, 0, rows]) + yr[3, 0, rows]
            all_decay = dec[0] * dec[1] * (dec[2] * dec[3])
            xs[0, 128 + i : 129 + i] = all_decay
            xs[1, 128 + i : 129 + i] = all_decay
        for to_x in range(4):

            @pl.when(to_x > x)
            def _():
                x_copy(to_x, 0).start()

        hand_back(1, 0)
        hand_back(3, 0)
        hand_back(2, 1)
        hand_back(3, 1)

    def combine_back():
        y1_wait(1)

        @pl.when(x > 0)
        def _():
            for i in range(2):
                rows = slice(64 * i, 64 * i + 64)
                dec = decays(i)
                back = yr[2, 1, rows] + dec[2] * yr[3, 1, rows]
                back = yr[1, 1, rows] + dec[1] * back
                xs[1, rows] = yr[0, 1, rows] + dec[0] * back

        for to_x in range(4):

            @pl.when(to_x < x)
            def _():
                x_copy(to_x, 1).start()


    def take(acc, at_x):
        remote(
            xs.at[0], xr.at[at_x], x_send.at[at_x], x_recv.at[at_x], seq_0=at_x
        ).wait_recv()
        for i in range(2):
            rows = slice(64 * i, 64 * i + 64)
            acc[rows] = xr[at_x, 128 + i : 129 + i] * acc[rows] + xr[at_x, rows]

    def enter_far():
        for at_x in range(4):
            pl.when(at_x < x)(functools.partial(take, ein, at_x))
        for i in range(2):
            rows = slice(64 * i, 64 * i + 64)
            dec = decays(i)
            into = ein[rows]
            for at_y in range(4):
                zs[at_y, 2, rows] = into
                into = dec[at_y] * into
        for step in (2, 1, 3, 0):
            hand_back((y + step) % 4, 2)

    def leave_far():
        y1_wait(2)
        y1_wait(3)
        for at_x in range(3, -1, -1):
            pl.when(at_x > x)(functools.partial(take, xin, at_x))
        for i in range(2):
            rows = slice(64 * i, 64 * i + 64)
            dec = decays(i)
            late = xin[rows]
            zs[3, 3, rows] = late
            late = dec[3] * late
            zs[2, 3, rows] = late + yr[3, 2, rows]
            late = dec[2] * late + (yr[2, 3, rows] + dec[2] * yr[3, 3, rows])
            zs[1, 3, rows] = late
            zs[0, 3, rows] = dec[1] * late + yr[1, 2, rows]
        for step in (2, 1, 3, 0):
            hand_back((y + step) % 4, 3)

    def back_copy(pair, kind):
        if kind == 2:
            cols, src, dst = pair_cols(pair), gv, bv
        else:
            cols = pl.ds(pl.multiple_of(pair * 256, 256), 256)
            src, dst = ((gq, bq), (gk, bk))[kind]
        return remote(
            src.at[other_rows, cols], dst.at[:, cols],
            out_send.at[kind], out_recv.at[kind], seq_2=other,
        )

    def y2_wait(pair, kinds):
        for kind in kinds:
            here = (y % 2 == 1, y >= 2, x > 0, True)[kind]

            @pl.when((pair != y) & here)
            def _():
                remote(
                    zs.at[0, kind], zr.at[pair, kind], y2_send.at[0, kind],
                    y2_recv.at[pair, kind], seq_1=pair,
                ).wait_recv()

    def cross_in(pair):
        y2_wait(pair, (0, 1, 2))
        for i in range(2):
            head = pl.ds(pair * 2 + i, 1)
            rows = pl.ds(64 * i, 64)
            grad = gt[pair, rows]
            enter_hi, enter_lo = split(
                jnp.concatenate([zr[pair, n, rows] for n in range(3)], axis=0)
            )
            mixed = dot(
                jnp.concatenate([enter_hi, enter_lo], axis=0), qb[:, head_cols(pair, i)], NT
            )
            drift_row = drift[head, :]
            for n in range(3):
                state_row = mixed[64 * n : 64 * n + 64] + mixed[192 + 64 * n : 256 + 64 * n]
                level_row = fs[head, :] * jnp.sum(state_row * grad, axis=0, keepdims=True)
                glw[3 + n, head, :] = level_row
                drift_row = drift_row + wts[3 + n, head, :] * level_row
            drift[head, :] = drift_row
            weighted_hi, weighted_lo = split(
                jnp.concatenate(
                    [grad * (fs[head, :] * wts[3 + n, head, :]) for n in range(3)], axis=0
                )
            )
            gq[:, head_cols(pair, i)] = gq[:, head_cols(pair, i)] + dot(
                jnp.concatenate([weighted_hi, weighted_lo, weighted_hi], axis=0),
                jnp.concatenate([enter_hi, enter_hi, enter_lo], axis=0), TN,
            )
        back_copy(pair, 0).start()
        wide = pl.ds(pl.multiple_of(pair * 256, 256), 256)
        out_wide = pl.ds(pl.multiple_of(c * 1024 + pair * 256, 256), 256)
        gq_out[:, out_wide] = gq[own_rows, wide].astype(BF16)

    def cross_out(pair):
        y2_wait(pair, (3,))
        for i in range(2):
            head = pl.ds(pair * 2 + i, 1)
            rows = pl.ds(64 * i, 64)
            leave_hi, leave_lo = split(zr[pair, 3, rows])
            left = dot(
                jnp.concatenate([leave_hi, leave_lo], axis=0), kb[:, head_cols(pair, i)], NT
            )
            value_grad = gvt[pair, rows] + de[head, :] * (left[0:64] + left[64:128])
            gvt[pair, rows] = value_grad
            drift[head, :] = drift[head, :] - jnp.sum(
                vt[pair, rows] * value_grad, axis=0, keepdims=True
            )

    def cross_grad(pair):
        for i in range(2):
            head = pl.ds(pair * 2 + i, 1)
            rows = pl.ds(64 * i, 64)
            leave_hi, leave_lo = split(zr[pair, 3, rows])
            ended_hi, ended_lo = split(vt[pair, rows] * de[head, :])
            gk[:, head_cols(pair, i)] = gk[:, head_cols(pair, i)] + dot(
                jnp.concatenate([ended_hi, ended_lo, ended_hi], axis=0),
                jnp.concatenate([leave_hi, leave_hi, leave_lo], axis=0), TN,
            )
        gv[:, pair_cols(pair)] = jnp.transpose(gvt[pair])
        back_copy(pair, 1).start()
        back_copy(pair, 2).start()
        wide = pl.ds(pl.multiple_of(pair * 256, 256), 256)
        out_wide = pl.ds(pl.multiple_of(c * 1024 + pair * 256, 256), 256)
        out_narrow = pl.ds(pl.multiple_of(c * 512 + pair * 128, 128), 128)
        gk_out[:, out_wide] = gk[own_rows, wide].astype(BF16)
        gv_out[:, out_narrow] = gv[own_rows, pair_cols(pair)].astype(BF16)

    def loop(low, high, body):
        def step(n, carry):
            body(n)
            return carry

        lax.fori_loop(low, high, step, 0)

    def toward(n):
        return (y + jnp.where(n == 2, 3, jnp.where(n == 3, 0, 2 - n))) % 4

    def nearby(n):
        return (y + jnp.where(n == 2, 3, jnp.where(n == 3, 2, n))) % 4

    swaps[1].wait_recv()
    kb[other_rows, :] = rk[...].astype(BF16)
    swaps[2].wait_recv()
    vb[other_rows, :] = rv[...].astype(BF16)
    loop(0, 4, lambda n: state_fwd(toward(n)))
    swaps[3].wait_recv()
    gb[other_rows, :] = rg[...].astype(BF16)
    swaps[4].wait_recv()
    qb[other_rows, :] = rq[...].astype(BF16)
    loop(0, 4, lambda n: state_back(toward(n)))
    loop(0, 4, lambda n: state_near(toward(n)))
    combine_fwd()
    masks()
    loop(0, 1, intra)
    combine_back()
    loop(1, 3, intra)
    enter_far()
    loop(3, 4, intra)
    leave_far()
    loop(0, 4, lambda n: cross_in(nearby(n)))
    loop(0, 4, lambda n: cross_out(nearby(n)))
    lane = lax.broadcasted_iota(jnp.int32, (8, 256), 1)
    tail = suffix(drift[...], lane)
    drift[...] = tail
    bs_out = remote(small.at[:, :], bs.at[pl.ds(48, 8), :], last_send.at[1], last_recv.at[1], seq_2=other)
    tile = lax.broadcasted_iota(jnp.int32, (8, 128), 1)
    mine = lax.broadcasted_iota(jnp.int32, (8, 128), 0)
    head_total = tail[:, 0:1]
    head_square = jnp.sum(tail * tail, axis=1, keepdims=True)
    head_sum = jnp.sum(tail, axis=1, keepdims=True)
    slots = [
        jnp.where(tile == mine + 8 * n, jnp.broadcast_to(part, (8, 128)), 0.0)
        for n, part in enumerate((head_total, head_square, head_sum))
    ]
    place_here = chip * 8 + group
    a_buf[place_here] = jnp.sum(slots[0] + slots[1] + slots[2], axis=0, keepdims=True)

    def a_copy(dx, dy, dz, dc):
        return remote(
            a_buf.at[place_here], a_buf.at[place_here], a_send.at[0], a_recv.at[0],
            seq_0=(x + dx) % 4, seq_1=(y + dy) % 4, seq_2=(c + dc) % 2, head=(z + dz) % 4,
        )

    def hops(move):
        return -(sum(min(d, 4 - d) for d in move[:3]) + 0.5 * move[3])

    moves = [(dx, dy, dz, dc) for dx in range(4) for dy in range(4) for dz in range(4) for dc in (0, 1)]
    for move in sorted(moves, key=hops):
        if any(move):
            a_copy(*move).start()
    small[...] = drift[:, other_rows]
    for level in range(6):
        ss_rows = slice(8 * level, 8 * level + 8)
        ys[y, 1, ss_rows] = glw[level, :, other_rows]
    glw_copy = remote(
        ys.at[y, 1, pl.ds(0, 48)], bs.at[pl.ds(0, 48), :], last_send.at[0], last_recv.at[0],
        seq_2=other,
    )
    glw_copy.start()
    bs_out.start()
    for level in range(6):
        glw_out[level, own_heads, :] = glw[level, :, own_rows]

    loop(0, 4, cross_grad)
    def back_whole(kind):
        src, dst = ((gq, bq), (gk, bk), (gv, bv))[kind]
        return remote(
            src.at[other_rows, :], dst, out_send.at[kind], out_recv.at[kind], seq_2=other
        )

    for kind in range(3):
        back_whole(kind).wait_recv()
    other_q = pl.ds(pl.multiple_of(other * 1024, 1024), 1024)
    other_v = pl.ds(pl.multiple_of(other * 512, 512), 512)
    gq_out[:, other_q] = bq[...].astype(BF16)
    gk_out[:, other_q] = bk[...].astype(BF16)
    gv_out[:, other_v] = bv[...].astype(BF16)
    glw_copy.wait_recv()
    for level in range(6):
        glw_out[level, other_heads, :] = bs[8 * level : 8 * level + 8, :]

    a_whole = remote(
        a_buf.at[pl.ds(0, 127)], a_buf.at[pl.ds(0, 127)], a_send.at[0], a_recv.at[0], seq_2=other
    )
    a_whole.wait_recv()
    run = jnp.zeros((8, 128), F32)
    later = jnp.zeros((8, 128), F32)
    squares = jnp.zeros((8, 128), F32)
    for at in range(15, -1, -1):
        now = a_buf[8 * at : 8 * at + 8, 0, :]
        later = later + run * (chip == at).astype(F32)
        square = pltpu.roll(now, 120, 1)
        total_of = pltpu.roll(now, 112, 1)
        squares = squares + square + run * (2.0 * total_of + 256.0 * run)
        run = run + now
    squares = jnp.where(tile < 8, squares, 0.0)
    total_square = jnp.sum(jnp.sum(squares, axis=1, keepdims=True), axis=0, keepdims=True)
    factor = jnp.minimum(1.0, lax.rsqrt(total_square / (64 * 4096) + 1e-06))

    def later_of(at_group):
        row = jnp.sum(jnp.where(mine == at_group, later, 0.0), axis=0, keepdims=True)
        return jnp.sum(
            jnp.where(tile == mine, jnp.broadcast_to(row, (8, 128)), 0.0), axis=1, keepdims=True
        )

    glg_out[own_heads, :] = (drift[:, own_rows] + later_of(group)) * factor
    bs_out.wait_recv()
    glg_out[other_heads, :] = (bs[48:56, :] + later_of(z * 2 + other)) * factor

    for swap in swaps:
        swap.wait_send()
    for pair in range(4):
        for kind in range(4):

            @pl.when((y != pair) & sent(kind, y))
            def _():
                y1_copy(pair, kind, y).wait_send()

            back = (pair % 2 == 1, pair >= 2, x > 0, True)[kind]
            if back is not False:

                @pl.when((y != pair) & back)
                def _():
                    y2_copy(pair, kind, y2_source(pair, kind)).wait_send()

        @pl.when(pair != x)
        def _():
            x_copy(pair, 0).wait_send()

    for kind in range(3):
        back_whole(kind).wait_send()
    glw_copy.wait_send()
    bs_out.wait_send()
    a_whole.wait_send()


def settle(*refs):
    source, target, sem = refs[:5], refs[5:10], refs[10]
    stores = []
    for n in range(5):
        cuts = 4 if n < 2 else 2 if n == 2 else 1
        rows = source[n].shape[0] // cuts
        for m in range(cuts):
            at = pl.ds(rows * m, rows)
            stores.append(
                pltpu.make_async_copy(source[n].at[at], target[n].at[at], sem.at[len(stores)])
            )
    for store in stores:
        store.start()
    for store in stores:
        store.wait()


def shards(queries, keys, values, out_grad, log_gate, level_weight, doc_start):
    args = (queries, keys, values, out_grad, log_gate, level_weight, doc_start.reshape(1, -1))
    anywhere = pl.BlockSpec(memory_space=pl.ANY)
    results = tuple(
        jax.ShapeDtypeStruct(a.shape, a.dtype)
        for a in (queries, keys, values, level_weight, log_gate)
    )
    held = tuple(pltpu.VMEM(r.shape, r.dtype) for r in results)
    scratch = [pltpu.VMEM(a.shape, a.dtype) for a in args] + [pltpu.SemaphoreType.DMA((7,))]
    swap = [(128, 1024), (128, 1024), (128, 512), (128, 512), (64, 128)]
    scratch += [pltpu.VMEM(s, F32) for s in swap * 2]
    scratch += [pltpu.VMEM(s, BF16) for s in ((256, 1024), (256, 1024), (256, 512), (256, 512))]
    scratch += [pltpu.VMEM((4, 128, 256), F32)] * 2
    scratch += [pltpu.VMEM((8, 256), F32)] * 6
    scratch += [pltpu.VMEM((6, 8, 256), F32), pltpu.VMEM((8, 256, 128), F32)]
    scratch += [pltpu.VMEM((256, 256), F32), pltpu.VMEM((256, 256), BF16), pltpu.VMEM((256, 256), BF16)]
    scratch += [pltpu.VMEM((256, 1024), F32), pltpu.VMEM((256, 1024), F32), pltpu.VMEM((256, 512), F32)]
    scratch += [pltpu.VMEM((4, 128, 256), F32), pltpu.VMEM((6, 8, 256), F32)]
    scratch += [pltpu.VMEM((8, 256), F32), pltpu.VMEM((8, 128), F32)]
    scratch += [pltpu.VMEM((4, 4, 136, 128), F32)] * 2 + [pltpu.VMEM((4, 4, 128, 128), F32)] * 2
    scratch += [pltpu.VMEM((2, 136, 128), F32), pltpu.VMEM((4, 136, 128), F32)]
    scratch += [pltpu.VMEM((128, 128), F32)] * 2
    scratch += [pltpu.VMEM((128, 1024), F32), pltpu.VMEM((128, 1024), F32), pltpu.VMEM((128, 512), F32)]
    scratch += [pltpu.VMEM((56, 128), F32)]
    scratch += [pltpu.VMEM((128, 1, 128), F32)]
    sems = [(5,), (5,), (4, 4), (4, 4), (4, 4), (4, 4), (4,), (4,), (3,), (3,), (2,), (2,)]
    sems += [(1,)] * 2
    scratch += [pltpu.SemaphoreType.DMA(s) for s in sems]
    outs = pl.pallas_call(
        kernel,
        out_shape=held,
        in_specs=[anywhere] * 7,
        out_specs=[pl.BlockSpec(memory_space=pltpu.VMEM)] * 5,
        scratch_shapes=scratch,
        compiler_params=pltpu.CompilerParams(
            collective_id=0, has_side_effects=True, vmem_limit_bytes=60 * 2**20
        ),
    )(*args)
    return pl.pallas_call(
        settle,
        out_shape=results,
        in_specs=[anywhere] * 5,
        out_specs=[anywhere] * 5,
        scratch_shapes=[pltpu.SemaphoreType.DMA((12,))],
        compiler_params=pltpu.CompilerParams(vmem_limit_bytes=48 * 2**20),
    )(*outs)


def solution(mesh):
    finer = Mesh(
        mesh.devices.reshape(4, 4, 2, mesh.shape["head"]), ("seq_0", "seq_1", "seq_2", "head")
    )
    wide = P(SEQ, "head")
    return jax.shard_map(
        shards,
        mesh=finer,
        in_specs=(wide, wide, wide, wide, P("head", SEQ), P(None, "head", SEQ), P(SEQ)),
        out_specs=(wide, wide, wide, P(None, "head", SEQ), P("head", SEQ)),
        check_vma=False,
    )
```

```python
import functools

import jax
import jax.numpy as jnp
from jax import lax
from jax.experimental import pallas as pl
from jax.experimental.pallas import tpu as pltpu
from jax.sharding import Mesh
from jax.sharding import PartitionSpec as P

SEQ = ("seq_0", "seq_1", "seq_2")
MESH = pl.DeviceIdType.MESH
F32 = jnp.float32
BF16 = jnp.bfloat16
NEG = -1e30

NN = (((1,), (0,)), ((), ()))
NT = (((1,), (1,)), ((), ()))
TN = (((0,), (0,)), ((), ()))


def dot(a, b, dims):
    return lax.dot_general(a, b, dims, preferred_element_type=F32)


def split(a):
    hi = a.astype(BF16)
    return hi, (a - hi.astype(F32)).astype(BF16)


def prefix(a, lane):
    shift = 1
    while shift < a.shape[1]:
        a = a + jnp.where(lane >= shift, pltpu.roll(a, shift, 1), 0.0)
        shift *= 2
    return a


def suffix(a, lane):
    size = a.shape[1]
    shift = 1
    while shift < size:
        a = a + jnp.where(lane < size - shift, pltpu.roll(a, size - shift, 1), 0.0)
        shift *= 2
    return a


def kernel(
    q_hbm, k_hbm, v_hbm, g_hbm, lg_hbm, lw_hbm, ds_hbm,
    gq_out, gk_out, gv_out, glw_out, glg_out,
    q_in, k_in, v_in, g_in, lg_in, lw_in, ds_in, load_sem,
    sq, sk, sv, sg, ss, rq, rk, rv, rg, rs,
    qb, kb, vb, gb, vt, gt,
    gates, doc, cum, resets, fs, de, wts, cm, bias, pt, rt,
    gq, gk, gv, gvt, glw, drift, small,
    ys, yr, zs, zr, xs, xr, ein, xin,
    bq, bk, bv, bs,
    a_buf,
    in_send, in_recv, kv_send, kv_recv, y1_send, y1_recv, y2_send, y2_recv, x_send, x_recv,
    out_send, out_recv, last_send, last_recv, a_send, a_recv,
):
    x, y, c, z = (lax.axis_index(n) for n in ("seq_0", "seq_1", "seq_2", "head"))
    other = 1 - c
    chip = x * 4 + y
    group = z * 2 + c

    def remote(src, dst, send, recv, **to):
        return pltpu.make_async_remote_copy(
            src_ref=src, dst_ref=dst, send_sem=send, recv_sem=recv,
            device_id=to, device_id_type=MESH,
        )

    loads = [
        pltpu.make_async_copy(src, dst, load_sem.at[n])
        for n, (src, dst) in enumerate((
            (ds_hbm, ds_in), (lg_hbm, lg_in), (lw_hbm, lw_in), (k_hbm, k_in),
            (v_hbm, v_in), (g_hbm, g_in), (q_hbm, q_in),
        ))
    ]
    for load in loads:
        load.start()

    barrier = pltpu.get_barrier_semaphore()
    for step in range(1, 4):
        for axis, place in (("seq_1", y), ("seq_0", x)):
            pl.semaphore_signal(
                barrier, inc=1, device_id={axis: (place + step) % 4}, device_id_type=MESH
            )
    for step in range(1, 8):
        peer = (group + step) % 8
        pl.semaphore_signal(
            barrier, inc=1, device_id={"head": peer // 2, "seq_2": peer % 2}, device_id_type=MESH
        )

    q_cols = pl.ds(pl.multiple_of(other * 1024, 1024), 1024)
    v_cols = pl.ds(pl.multiple_of(other * 512, 512), 512)
    own_q = pl.ds(pl.multiple_of(c * 1024, 1024), 1024)
    own_v = pl.ds(pl.multiple_of(c * 512, 512), 512)
    own_rows = pl.ds(pl.multiple_of(c * 128, 128), 128)
    other_rows = pl.ds(pl.multiple_of(other * 128, 128), 128)
    own_heads = pl.ds(pl.multiple_of(c * 8, 8), 8)
    other_heads = pl.ds(pl.multiple_of(other * 8, 8), 8)
    swaps = [
        remote(src, dst, in_send.at[n], in_recv.at[n], seq_2=other)
        for n, (src, dst) in enumerate(((ss, rs), (sg, rg), (sq, rq)))
    ]

    def toward(n):
        return (y + jnp.where(n == 2, 3, jnp.where(n == 3, 0, 2 - n))) % 4

    def nearby(n):
        return (y + jnp.where(n == 2, 3, jnp.where(n == 3, 2, n))) % 4

    def key_copy(pair):
        cols = pl.ds(pl.multiple_of(pair * 256, 256), 256)
        return remote(
            sk.at[:, cols], rk.at[:, cols], kv_send.at[0], kv_recv.at[0, pair], seq_2=other
        )

    def value_copy(pair):
        cols = pl.ds(pl.multiple_of(pair * 128, 128), 128)
        return remote(
            sv.at[:, cols], rv.at[:, cols], kv_send.at[1], kv_recv.at[1, pair], seq_2=other
        )

    for load in loads[:3]:
        load.wait()
    ds_row = jnp.broadcast_to(ds_in[...].astype(F32), (8, 128))
    ss[0:8, :] = lg_in[other_heads, :]
    for level in range(6):
        ss[8 + 8 * level : 16 + 8 * level, :] = lw_in[level, other_heads, :]
    ss[56:64, :] = ds_row
    loads[3].wait()
    sk[...] = k_in[:, q_cols].astype(F32)
    loads[4].wait()
    sv[...] = v_in[:, v_cols].astype(F32)
    pl.semaphore_wait(barrier, 13)
    swaps[0].start()
    for n in (2, 1, 3, 0):
        key_copy((y + n) % 4).start()
        value_copy((y + n) % 4).start()
    loads[5].wait()
    sg[...] = g_in[:, v_cols].astype(F32)
    loads[6].wait()
    sq[...] = q_in[:, q_cols].astype(F32)
    for swap in swaps[1:]:
        swap.start()
    kb[own_rows, :] = k_in[:, own_q]
    vb[own_rows, :] = v_in[:, own_v]
    gb[own_rows, :] = g_in[:, own_v]
    qb[own_rows, :] = q_in[:, own_q]
    gates[:, own_rows] = lg_in[own_heads, :]
    for level in range(6):
        wts[level, :, own_rows] = lw_in[level, own_heads, :]
    doc[:, own_rows] = ds_row
    ein[...] = jnp.zeros_like(ein)
    xin[...] = jnp.zeros_like(xin)
    pt[128:256, 0:128] = jnp.zeros((128, 128), BF16)
    rt[128:256, 0:128] = jnp.zeros((128, 128), BF16)

    zero_slab = jnp.zeros((128, 128), F32)
    for level, absent in ((0, y % 2 == 0), (1, y < 2), (2, x == 0)):

        @pl.when(absent)
        def _():
            for pair in range(4):
                zr[pair, level] = zero_slab

    swaps[0].wait_recv()
    gates[:, other_rows] = rs[0:8, :]
    for level in range(6):
        wts[level, :, other_rows] = rs[8 + 8 * level : 16 + 8 * level, :]
    doc[:, other_rows] = rs[56:64, :]
    lane = lax.broadcasted_iota(jnp.int32, (8, 256), 1)
    cum_now = prefix(gates[...], lane)
    reset = prefix(doc[...], lane)
    total = cum_now[:, 255:256]
    reset_total = reset[:, 255:256]
    cum[...] = cum_now
    resets[...] = reset
    fs[...] = jnp.where(reset == 0.0, jnp.exp(cum_now), 0.0)
    de[...] = jnp.where(reset == reset_total, jnp.exp(total - cum_now), 0.0)
    decay = jnp.broadcast_to(jnp.where(reset_total == 0.0, jnp.exp(total), 0.0), (8, 128))
    small[...] = decay
    def masks():
        columns = jnp.transpose(
            jnp.concatenate([cum[...], resets[...], jnp.zeros((112, 256), F32)], axis=0)
        )
        for head in range(8):
            cm[head] = jnp.broadcast_to(columns[:, head : head + 1], (256, 128))
        reset_col = jnp.broadcast_to(columns[:, 8:9], (256, 128))
        for half in range(2):
            reset_row = jnp.broadcast_to(resets[0:1, 128 * half : 128 * half + 128], (256, 128))
            s_pos = lax.broadcasted_iota(jnp.int32, (256, 128), 0)
            t_pos = lax.broadcasted_iota(jnp.int32, (256, 128), 1) + 128 * half
            bias[:, 128 * half : 128 * half + 128] = jnp.where(
                (t_pos >= s_pos) & (reset_col == reset_row), 0.0, NEG
            )

    def head_cols(pair, i):
        return pl.ds(pl.multiple_of(pair * 256 + i * 128, 128), 128)

    def pair_cols(pair):
        return pl.ds(pl.multiple_of(pair * 128, 128), 128)

    def sent(kind, at_y):
        return (True, x > 0, at_y % 2 == 1, at_y >= 2)[kind]

    def y1_copy(pair, kind, at_y):
        rows = 136 if kind == 0 else 128
        return remote(
            ys.at[pair, kind, pl.ds(0, rows)], yr.at[at_y, kind, pl.ds(0, rows)],
            y1_send.at[kind], y1_recv.at[kind], seq_1=pair,
        )

    def place(pair, kind, i, slab):
        rows = pl.ds(64 * i, 64)

        @pl.when(pair == y)
        def _():
            yr[y, kind, rows] = slab

        @pl.when(pair != y)
        def _():
            ys[pair, kind, rows] = slab

    def hand_over(pair, kind):
        @pl.when((pair != y) & sent(kind, y))
        def _():
            y1_copy(pair, kind, y).start()

    def state_fwd(pair):
        wide = pl.ds(pl.multiple_of(pair * 256, 256), 256)
        key_copy(pair).wait_recv()
        kb[other_rows, wide] = rk[:, wide].astype(BF16)
        value_copy(pair).wait_recv()
        vb[other_rows, pair_cols(pair)] = rv[:, pair_cols(pair)].astype(BF16)
        vt[pair] = jnp.transpose(vb[:, pair_cols(pair)].astype(F32))
        for i in range(2):
            head = pl.ds(pair * 2 + i, 1)
            value_hi, value_lo = split(vt[pair, pl.ds(64 * i, 64)] * de[head, :])
            state = dot(
                jnp.concatenate([value_hi, value_lo], axis=0), kb[:, head_cols(pair, i)], NN
            )
            place(pair, 0, i, state[0:64] + state[64:128])
            row = small[head, :]

            @pl.when(pair == y)
            def _():
                yr[y, 0, 128 + i : 129 + i] = row

            @pl.when(pair != y)
            def _():
                ys[pair, 0, 128 + i : 129 + i] = row

        hand_over(pair, 0)

    def state_back(pair):
        gt[pair] = jnp.transpose(gb[:, pair_cols(pair)].astype(F32))
        for i in range(2):
            head = pl.ds(pair * 2 + i, 1)
            hi, lo = split(gt[pair, pl.ds(64 * i, 64)] * (fs[head, :] * wts[5, head, :]))
            back = dot(jnp.concatenate([hi, lo], axis=0), qb[:, head_cols(pair, i)], NN)
            place(pair, 1, i, back[0:64] + back[64:128])
        hand_over(pair, 1)

    def state_near(pair):
        for i in range(2):
            head = pl.ds(pair * 2 + i, 1)
            grad = gt[pair, pl.ds(64 * i, 64)]
            parts = [split(grad * (fs[head, :] * wts[level, head, :])) for level in (3, 4)]
            back = dot(
                jnp.concatenate([p[0] for p in parts] + [p[1] for p in parts], axis=0),
                qb[:, head_cols(pair, i)], NN,
            )
            for n in range(2):
                place(
                    pair, 2 + n, i, back[64 * n : 64 * n + 64] + back[128 + 64 * n : 192 + 64 * n]
                )
        hand_over(pair, 2)
        hand_over(pair, 3)

    def intra(pair):
        for i in range(2):
            number = pair * 2 + i
            head = pl.ds(number, 1)
            rows = pl.ds(64 * i, 64)
            query = qb[:, head_cols(pair, i)]
            key = kb[:, head_cols(pair, i)]
            grad = gb[:, pair_cols(pair)]
            value = vb[:, pair_cols(pair)]
            mine = lax.broadcasted_iota(jnp.int32, (64, 128), 1) // 64 == i
            weight = [wts[level, head, :] for level in range(3)]
            span = lax.broadcasted_iota(jnp.int32, (1, 256), 1) // 64
            cum_row = cum[head, :]
            level_rows = [jnp.zeros((1, 256), F32) for level in range(3)]
            drift_row = jnp.zeros((1, 256), F32)
            for b in range(4):
                low = 0 if b < 2 else 128
                blk = slice(64 * b, 64 * b + 64)
                score = dot(key[blk], query[low:256], NT)
                pair_dot = dot(
                    jnp.where(mine, value[blk], jnp.zeros((64, 128), BF16)), grad[low:256], NT
                )
                col = cm[number, blk, :]
                if low == 0:
                    col = jnp.concatenate([col, col], axis=1)
                decayed = jnp.exp((cum_row[:, low:256] - col) + bias[blk, low:256])
                at = span[:, low:256]
                near = (at == b).astype(jnp.int32), ((at ^ 1) == b).astype(jnp.int32)
                mix = jnp.where(
                    near[0] == 1, weight[0][:, low:256],
                    jnp.where(near[1] == 1, weight[1][:, low:256], weight[2][:, low:256]),
                )
                scored = decayed * score
                joint = jnp.sum(scored * pair_dot, axis=0, keepdims=True)
                prob = (scored * mix).astype(BF16)
                pt[blk, low:256] = prob
                rt[blk, low:256] = (decayed * mix * pair_dot).astype(BF16)
                drifted = jnp.sum(prob.astype(F32) * pair_dot, axis=0, keepdims=True)
                if low:
                    pad = jnp.zeros((1, 128), F32)
                    joint = jnp.concatenate([pad, joint], axis=1)
                    drifted = jnp.concatenate([pad, drifted], axis=1)
                drift_row = drift_row + drifted
                level_rows[0] = level_rows[0] + jnp.where(span == b, joint, 0.0)
                level_rows[1] = level_rows[1] + jnp.where((span ^ 1) == b, joint, 0.0)
                level_rows[2] = level_rows[2] + jnp.where(
                    (span != b) & ((span ^ 1) != b), joint, 0.0
                )
            for level in range(3):
                glw[level, head, :] = level_rows[level]
            drift[head, :] = drift_row
            gvt[pair, rows] = dot(gt[pair, rows].astype(BF16), pt[...], NT)
            gk[:, head_cols(pair, i)] = dot(rt[...], query, NN)
            gq[:, head_cols(pair, i)] = dot(rt[...], key, TN)

    def y2_copy(to_y, kind, src):
        return remote(
            src, zr.at[y, kind], y2_send.at[kind], y2_recv.at[y, kind // 3], seq_1=to_y
        )

    def y2_source(to_y, kind):
        if kind == 0:
            return yr.at[to_y - 1, 0, pl.ds(0, 128)]
        return zs.at[to_y, kind]

    def hand_back(to_y, kind):
        def go():
            @pl.when(to_y != y)
            def _():
                y2_copy(to_y, kind, y2_source(to_y, kind)).start()

            @pl.when(to_y == y)
            def _():
                zr[y, kind] = y2_source(to_y, kind)[...]

        if kind == 2:
            pl.when(x > 0)(go)
        else:
            go()

    def several(buf, count, kind, send, recv):
        rows = pl.ds(0, 136 if kind == 0 and buf is ys else 128)
        return remote(
            buf.at[pl.ds(0, count), kind, rows], buf.at[pl.ds(0, count), kind, rows],
            send, recv, seq_2=other,
        )

    def in_turn(kind, here, act):
        pl.when(here)(lambda: act(1))
        pl.when(jnp.logical_not(here))(lambda: act(2))

    def y1_wait(kind):
        def act(count):
            several(ys, count, kind, y1_send.at[kind], y1_recv.at[kind]).wait_recv()

        if kind == 0:
            act(3)
        elif kind == 1:
            pl.when(x > 0)(lambda: act(3))
        else:
            in_turn(kind, y % 2 == 1 if kind == 2 else y >= 2, act)

    def x_copy(to_x, kind):
        return remote(xs.at[kind], xr.at[x], x_send.at[to_x], x_recv.at[x], seq_0=to_x)

    def decays(i):
        return [yr[n, 0, 128 + i : 129 + i] for n in range(4)]

    def combine_fwd():
        y1_wait(0)
        for i in range(2):
            rows = slice(64 * i, 64 * i + 64)
            dec = decays(i)
            both = dec[1] * yr[0, 0, rows] + yr[1, 0, rows]
            zs[2, 1, rows] = both
            after = dec[2] * both
            zs[3, 1, rows] = after
            xs[0, rows] = dec[3] * (after + yr[2, 0, rows]) + yr[3, 0, rows]
            all_decay = dec[0] * dec[1] * (dec[2] * dec[3])
            xs[0, 128 + i : 129 + i] = all_decay
            xs[1, 128 + i : 129 + i] = all_decay
        for to_x in range(4):

            @pl.when(to_x > x)
            def _():
                x_copy(to_x, 0).start()

        hand_back(1, 0)
        hand_back(3, 0)
        hand_back(2, 1)
        hand_back(3, 1)

    def combine_back():
        y1_wait(1)

        @pl.when(x > 0)
        def _():
            for i in range(2):
                rows = slice(64 * i, 64 * i + 64)
                dec = decays(i)
                back = yr[2, 1, rows] + dec[2] * yr[3, 1, rows]
                back = yr[1, 1, rows] + dec[1] * back
                xs[1, rows] = yr[0, 1, rows] + dec[0] * back

        for to_x in range(4):

            @pl.when(to_x < x)
            def _():
                x_copy(to_x, 1).start()


    def take(acc, at_x):
        remote(
            xs.at[0], xr.at[at_x], x_send.at[at_x], x_recv.at[at_x], seq_0=at_x
        ).wait_recv()
        for i in range(2):
            rows = slice(64 * i, 64 * i + 64)
            acc[rows] = xr[at_x, 128 + i : 129 + i] * acc[rows] + xr[at_x, rows]

    def enter_far():
        for at_x in range(4):
            pl.when(at_x < x)(functools.partial(take, ein, at_x))
        for i in range(2):
            rows = slice(64 * i, 64 * i + 64)
            dec = decays(i)
            into = ein[rows]
            for at_y in range(4):
                zs[at_y, 2, rows] = into
                into = dec[at_y] * into
        for step in (2, 1, 3, 0):
            hand_back((y + step) % 4, 2)

    def leave_far():
        y1_wait(2)
        y1_wait(3)
        for at_x in range(3, -1, -1):
            pl.when(at_x > x)(functools.partial(take, xin, at_x))
        for i in range(2):
            rows = slice(64 * i, 64 * i + 64)
            dec = decays(i)
            late = xin[rows]
            zs[3, 3, rows] = late
            late = dec[3] * late
            zs[2, 3, rows] = late + yr[3, 2, rows]
            late = dec[2] * late + (yr[2, 3, rows] + dec[2] * yr[3, 3, rows])
            zs[1, 3, rows] = late
            zs[0, 3, rows] = dec[1] * late + yr[1, 2, rows]
        for step in (2, 1, 3, 0):
            hand_back((y + step) % 4, 3)

    def back_copy(pair, kind):
        if kind == 2:
            cols, src, dst = pair_cols(pair), gv, bv
        else:
            cols = pl.ds(pl.multiple_of(pair * 256, 256), 256)
            src, dst = ((gq, bq), (gk, bk))[kind]
        return remote(
            src.at[other_rows, cols], dst.at[:, cols],
            out_send.at[kind], out_recv.at[kind], seq_2=other,
        )

    def y2_wait(pair, first, count):
        remote(
            zr.at[pair, pl.ds(0, count)], zr.at[pair, pl.ds(0, count)], y2_send.at[0],
            y2_recv.at[pair, first // 3], seq_1=pair,
        ).wait_recv()

    def cross_in(pair):
        levels_in = y % 2 + y // 2 + (x > 0).astype(jnp.int32)
        for count in range(1, 4):
            pl.when((pair != y) & (levels_in == count))(
                functools.partial(y2_wait, pair, 0, count)
            )
        for i in range(2):
            head = pl.ds(pair * 2 + i, 1)
            rows = pl.ds(64 * i, 64)
            grad = gt[pair, rows]
            enter_hi, enter_lo = split(
                jnp.concatenate([zr[pair, n, rows] for n in range(3)], axis=0)
            )
            mixed = dot(
                jnp.concatenate([enter_hi, enter_lo], axis=0), qb[:, head_cols(pair, i)], NT
            )
            drift_row = drift[head, :]
            for n in range(3):
                state_row = mixed[64 * n : 64 * n + 64] + mixed[192 + 64 * n : 256 + 64 * n]
                level_row = fs[head, :] * jnp.sum(state_row * grad, axis=0, keepdims=True)
                glw[3 + n, head, :] = level_row
                drift_row = drift_row + wts[3 + n, head, :] * level_row
            drift[head, :] = drift_row
            weighted_hi, weighted_lo = split(
                jnp.concatenate(
                    [grad * (fs[head, :] * wts[3 + n, head, :]) for n in range(3)], axis=0
                )
            )
            gq[:, head_cols(pair, i)] = gq[:, head_cols(pair, i)] + dot(
                jnp.concatenate([weighted_hi, weighted_lo, weighted_hi], axis=0),
                jnp.concatenate([enter_hi, enter_hi, enter_lo], axis=0), TN,
            )
        back_copy(pair, 0).start()
        wide = pl.ds(pl.multiple_of(pair * 256, 256), 256)
        out_wide = pl.ds(pl.multiple_of(c * 1024 + pair * 256, 256), 256)
        gq_out[:, out_wide] = gq[own_rows, wide].astype(BF16)

    def cross_out(pair):
        pl.when(pair != y)(functools.partial(y2_wait, pair, 3, 1))
        for i in range(2):
            head = pl.ds(pair * 2 + i, 1)
            rows = pl.ds(64 * i, 64)
            leave_hi, leave_lo = split(zr[pair, 3, rows])
            left = dot(
                jnp.concatenate([leave_hi, leave_lo], axis=0), kb[:, head_cols(pair, i)], NT
            )
            value_grad = gvt[pair, rows] + de[head, :] * (left[0:64] + left[64:128])
            gvt[pair, rows] = value_grad
            drift[head, :] = drift[head, :] - jnp.sum(
                vt[pair, rows] * value_grad, axis=0, keepdims=True
            )

    def cross_grad(pair):
        for i in range(2):
            head = pl.ds(pair * 2 + i, 1)
            rows = pl.ds(64 * i, 64)
            leave_hi, leave_lo = split(zr[pair, 3, rows])
            ended_hi, ended_lo = split(vt[pair, rows] * de[head, :])
            gk[:, head_cols(pair, i)] = gk[:, head_cols(pair, i)] + dot(
                jnp.concatenate([ended_hi, ended_lo, ended_hi], axis=0),
                jnp.concatenate([leave_hi, leave_hi, leave_lo], axis=0), TN,
            )
        gv[:, pair_cols(pair)] = jnp.transpose(gvt[pair])
        back_copy(pair, 1).start()
        back_copy(pair, 2).start()
        wide = pl.ds(pl.multiple_of(pair * 256, 256), 256)
        out_wide = pl.ds(pl.multiple_of(c * 1024 + pair * 256, 256), 256)
        out_narrow = pl.ds(pl.multiple_of(c * 512 + pair * 128, 128), 128)
        gk_out[:, out_wide] = gk[own_rows, wide].astype(BF16)
        gv_out[:, out_narrow] = gv[own_rows, pair_cols(pair)].astype(BF16)

    def loop(low, high, body):
        def step(n, carry):
            body(n)
            return carry

        lax.fori_loop(low, high, step, 0)

    loop(0, 4, lambda n: state_fwd(toward(n)))
    swaps[1].wait_recv()
    gb[other_rows, :] = rg[...].astype(BF16)
    swaps[2].wait_recv()
    qb[other_rows, :] = rq[...].astype(BF16)
    loop(0, 4, lambda n: state_back(toward(n)))
    loop(0, 4, lambda n: state_near(toward(n)))
    combine_fwd()
    masks()
    loop(0, 1, intra)
    combine_back()
    loop(1, 3, intra)
    enter_far()
    loop(3, 4, intra)
    leave_far()
    loop(0, 4, lambda n: cross_in(nearby(n)))
    loop(0, 4, lambda n: cross_out(nearby(n)))
    lane = lax.broadcasted_iota(jnp.int32, (8, 256), 1)
    tail = suffix(drift[...], lane)
    drift[...] = tail
    bs_out = remote(small.at[:, :], bs.at[pl.ds(48, 8), :], last_send.at[1], last_recv.at[1], seq_2=other)
    tile = lax.broadcasted_iota(jnp.int32, (8, 128), 1)
    mine = lax.broadcasted_iota(jnp.int32, (8, 128), 0)
    head_total = tail[:, 0:1]
    head_square = jnp.sum(tail * tail, axis=1, keepdims=True)
    head_sum = jnp.sum(tail, axis=1, keepdims=True)
    slots = [
        jnp.where(tile == mine + 8 * n, jnp.broadcast_to(part, (8, 128)), 0.0)
        for n, part in enumerate((head_total, head_square, head_sum))
    ]
    place_here = chip * 8 + group
    a_buf[place_here] = jnp.sum(slots[0] + slots[1] + slots[2], axis=0, keepdims=True)

    def a_copy(dx, dy, dz, dc):
        return remote(
            a_buf.at[place_here], a_buf.at[place_here], a_send.at[0], a_recv.at[0],
            seq_0=(x + dx) % 4, seq_1=(y + dy) % 4, seq_2=(c + dc) % 2, head=(z + dz) % 4,
        )

    def hops(move):
        return -(sum(min(d, 4 - d) for d in move[:3]) + 0.5 * move[3])

    moves = [(dx, dy, dz, dc) for dx in range(4) for dy in range(4) for dz in range(4) for dc in (0, 1)]
    for move in sorted(moves, key=hops):
        if any(move):
            a_copy(*move).start()
    small[...] = drift[:, other_rows]
    for level in range(6):
        ss_rows = slice(8 * level, 8 * level + 8)
        ys[y, 1, ss_rows] = glw[level, :, other_rows]
    glw_copy = remote(
        ys.at[y, 1, pl.ds(0, 48)], bs.at[pl.ds(0, 48), :], last_send.at[0], last_recv.at[0],
        seq_2=other,
    )
    glw_copy.start()
    bs_out.start()
    for level in range(6):
        glw_out[level, own_heads, :] = glw[level, :, own_rows]

    loop(0, 4, cross_grad)
    def back_whole(kind):
        src, dst = ((gq, bq), (gk, bk), (gv, bv))[kind]
        return remote(
            src.at[other_rows, :], dst, out_send.at[kind], out_recv.at[kind], seq_2=other
        )

    for kind in range(3):
        back_whole(kind).wait_recv()
    other_q = pl.ds(pl.multiple_of(other * 1024, 1024), 1024)
    other_v = pl.ds(pl.multiple_of(other * 512, 512), 512)
    gq_out[:, other_q] = bq[...].astype(BF16)
    gk_out[:, other_q] = bk[...].astype(BF16)
    gv_out[:, other_v] = bv[...].astype(BF16)
    glw_copy.wait_recv()
    for level in range(6):
        glw_out[level, other_heads, :] = bs[8 * level : 8 * level + 8, :]

    a_whole = remote(
        a_buf.at[pl.ds(0, 127)], a_buf.at[pl.ds(0, 127)], a_send.at[0], a_recv.at[0], seq_2=other
    )
    a_whole.wait_recv()
    run = jnp.zeros((8, 128), F32)
    later = jnp.zeros((8, 128), F32)
    squares = jnp.zeros((8, 128), F32)
    for at in range(15, -1, -1):
        now = a_buf[8 * at : 8 * at + 8, 0, :]
        later = later + run * (chip == at).astype(F32)
        square = pltpu.roll(now, 120, 1)
        total_of = pltpu.roll(now, 112, 1)
        squares = squares + square + run * (2.0 * total_of + 256.0 * run)
        run = run + now
    squares = jnp.where(tile < 8, squares, 0.0)
    total_square = jnp.sum(jnp.sum(squares, axis=1, keepdims=True), axis=0, keepdims=True)
    factor = jnp.minimum(1.0, lax.rsqrt(total_square / (64 * 4096) + 1e-06))

    def later_of(at_group):
        row = jnp.sum(jnp.where(mine == at_group, later, 0.0), axis=0, keepdims=True)
        return jnp.sum(
            jnp.where(tile == mine, jnp.broadcast_to(row, (8, 128)), 0.0), axis=1, keepdims=True
        )

    glg_out[own_heads, :] = (drift[:, own_rows] + later_of(group)) * factor
    bs_out.wait_recv()
    glg_out[other_heads, :] = (bs[48:56, :] + later_of(z * 2 + other)) * factor

    for swap in swaps:
        swap.wait_send()
    remote(sk, rk, kv_send.at[0], kv_recv.at[0, 0], seq_2=other).wait_send()
    remote(sv, rv, kv_send.at[1], kv_recv.at[1, 0], seq_2=other).wait_send()
    for kind in range(4):

        @pl.when(sent(kind, y))
        def _():
            several(ys, 3, kind, y1_send.at[kind], y1_recv.at[kind]).wait_send()

        def act(count):
            several(zs, count, kind, y2_send.at[kind], y2_recv.at[0, 0]).wait_send()

        if kind < 2:
            in_turn(kind, y % 2 == 1 if kind == 0 else y >= 2, act)
        else:
            pl.when(x > 0 if kind == 2 else y >= 0)(lambda: act(3))

    for pair in range(4):
        @pl.when(pair != x)
        def _():
            x_copy(pair, 0).wait_send()

    for kind in range(3):
        back_whole(kind).wait_send()
    glw_copy.wait_send()
    bs_out.wait_send()
    a_whole.wait_send()


def settle(*refs):
    source, target, sem = refs[:5], refs[5:10], refs[10]
    stores = []
    for n in range(5):
        cuts = 4 if n < 2 else 2 if n == 2 else 1
        rows = source[n].shape[0] // cuts
        for m in range(cuts):
            at = pl.ds(rows * m, rows)
            stores.append(
                pltpu.make_async_copy(source[n].at[at], target[n].at[at], sem.at[len(stores)])
            )
    for store in stores:
        store.start()
    for store in stores:
        store.wait()


def shards(queries, keys, values, out_grad, log_gate, level_weight, doc_start):
    args = (queries, keys, values, out_grad, log_gate, level_weight, doc_start.reshape(1, -1))
    anywhere = pl.BlockSpec(memory_space=pl.ANY)
    results = tuple(
        jax.ShapeDtypeStruct(a.shape, a.dtype)
        for a in (queries, keys, values, level_weight, log_gate)
    )
    held = tuple(pltpu.VMEM(r.shape, r.dtype) for r in results)
    scratch = [pltpu.VMEM(a.shape, a.dtype) for a in args] + [pltpu.SemaphoreType.DMA((7,))]
    swap = [(128, 1024), (128, 1024), (128, 512), (128, 512), (64, 128)]
    scratch += [pltpu.VMEM(s, F32) for s in swap * 2]
    scratch += [pltpu.VMEM(s, BF16) for s in ((256, 1024), (256, 1024), (256, 512), (256, 512))]
    scratch += [pltpu.VMEM((4, 128, 256), F32)] * 2
    scratch += [pltpu.VMEM((8, 256), F32)] * 6
    scratch += [pltpu.VMEM((6, 8, 256), F32), pltpu.VMEM((8, 256, 128), F32)]
    scratch += [pltpu.VMEM((256, 256), F32), pltpu.VMEM((256, 256), BF16), pltpu.VMEM((256, 256), BF16)]
    scratch += [pltpu.VMEM((256, 1024), F32), pltpu.VMEM((256, 1024), F32), pltpu.VMEM((256, 512), F32)]
    scratch += [pltpu.VMEM((4, 128, 256), F32), pltpu.VMEM((6, 8, 256), F32)]
    scratch += [pltpu.VMEM((8, 256), F32), pltpu.VMEM((8, 128), F32)]
    scratch += [pltpu.VMEM((4, 4, 136, 128), F32)] * 2 + [pltpu.VMEM((4, 4, 128, 128), F32)] * 2
    scratch += [pltpu.VMEM((2, 136, 128), F32), pltpu.VMEM((4, 136, 128), F32)]
    scratch += [pltpu.VMEM((128, 128), F32)] * 2
    scratch += [pltpu.VMEM((128, 1024), F32), pltpu.VMEM((128, 1024), F32), pltpu.VMEM((128, 512), F32)]
    scratch += [pltpu.VMEM((56, 128), F32)]
    scratch += [pltpu.VMEM((128, 1, 128), F32)]
    sems = [(3,), (3,), (2,), (2, 4), (4,), (4,), (4,), (4, 2), (4,), (4,), (3,), (3,), (2,), (2,)]
    sems += [(1,)] * 2
    scratch += [pltpu.SemaphoreType.DMA(s) for s in sems]
    outs = pl.pallas_call(
        kernel,
        out_shape=held,
        in_specs=[anywhere] * 7,
        out_specs=[pl.BlockSpec(memory_space=pltpu.VMEM)] * 5,
        scratch_shapes=scratch,
        compiler_params=pltpu.CompilerParams(
            collective_id=0, has_side_effects=True, vmem_limit_bytes=60 * 2**20
        ),
    )(*args)
    return pl.pallas_call(
        settle,
        out_shape=results,
        in_specs=[anywhere] * 5,
        out_specs=[anywhere] * 5,
        scratch_shapes=[pltpu.SemaphoreType.DMA((12,))],
        compiler_params=pltpu.CompilerParams(vmem_limit_bytes=48 * 2**20),
    )(*outs)


def solution(mesh):
    finer = Mesh(
        mesh.devices.reshape(4, 4, 2, mesh.shape["head"]), ("seq_0", "seq_1", "seq_2", "head")
    )
    wide = P(SEQ, "head")
    return jax.shard_map(
        shards,
        mesh=finer,
        in_specs=(wide, wide, wide, wide, P("head", SEQ), P(None, "head", SEQ), P(SEQ)),
        out_specs=(wide, wide, wide, P(None, "head", SEQ), P("head", SEQ)),
        check_vma=False,
    )
```

```python
import functools

import jax
import jax.numpy as jnp
from jax import lax
from jax.experimental import pallas as pl
from jax.experimental.pallas import tpu as pltpu
from jax.sharding import Mesh
from jax.sharding import PartitionSpec as P

SEQ = ("seq_0", "seq_1", "seq_2")
MESH = pl.DeviceIdType.MESH
F32 = jnp.float32
BF16 = jnp.bfloat16
NEG = -1e30

NN = (((1,), (0,)), ((), ()))
NT = (((1,), (1,)), ((), ()))
TN = (((0,), (0,)), ((), ()))


def dot(a, b, dims):
    return lax.dot_general(a, b, dims, preferred_element_type=F32)


def split(a):
    hi = a.astype(BF16)
    return hi, (a - hi.astype(F32)).astype(BF16)


def prefix(a, lane):
    shift = 1
    while shift < a.shape[1]:
        a = a + jnp.where(lane >= shift, pltpu.roll(a, shift, 1), 0.0)
        shift *= 2
    return a


def suffix(a, lane):
    size = a.shape[1]
    shift = 1
    while shift < size:
        a = a + jnp.where(lane < size - shift, pltpu.roll(a, size - shift, 1), 0.0)
        shift *= 2
    return a


def kernel(
    q_hbm, k_hbm, v_hbm, g_hbm, lg_hbm, lw_hbm, ds_hbm,
    gq_out, gk_out, gv_out, glw_out, glg_out,
    q_in, k_in, v_in, g_in, lg_in, lw_in, ds_in, load_sem,
    sq, sk, sv, sg, ss, rq, rk, rv, rg, rs,
    qb, kb, vb, gb, vt, gt,
    gates, doc, cum, resets, fs, de, wts, cm, bias, pt, rt,
    gq, gk, gv, gvt, glw, drift, small,
    ys, yr, zs, zr, xs, xr, ein, xin,
    bq, bk, bv, bs,
    a_buf,
    in_send, in_recv, kv_send, kv_recv, y1_send, y1_recv, y2_send, y2_recv, x_send, x_recv,
    out_send, out_recv, last_send, last_recv, a_send, a_recv,
):
    x, y, c, z = (lax.axis_index(n) for n in ("seq_0", "seq_1", "seq_2", "head"))
    other = 1 - c
    chip = x * 4 + y
    group = z * 2 + c

    def remote(src, dst, send, recv, **to):
        return pltpu.make_async_remote_copy(
            src_ref=src, dst_ref=dst, send_sem=send, recv_sem=recv,
            device_id=to, device_id_type=MESH,
        )

    loads = [
        pltpu.make_async_copy(src, dst, load_sem.at[n])
        for n, (src, dst) in enumerate((
            (ds_hbm, ds_in), (lg_hbm, lg_in), (lw_hbm, lw_in), (k_hbm, k_in),
            (v_hbm, v_in), (g_hbm, g_in), (q_hbm, q_in),
        ))
    ]
    for load in loads:
        load.start()

    barrier = pltpu.get_barrier_semaphore()
    for step in range(1, 4):
        for axis, place in (("seq_1", y), ("seq_0", x)):
            pl.semaphore_signal(
                barrier, inc=1, device_id={axis: (place + step) % 4}, device_id_type=MESH
            )
        pl.semaphore_signal(
            barrier, inc=1, device_id={"head": (z + step) % 4}, device_id_type=MESH
        )
    pl.semaphore_signal(barrier, inc=1, device_id={"seq_2": other}, device_id_type=MESH)

    q_cols = pl.ds(pl.multiple_of(other * 1024, 1024), 1024)
    v_cols = pl.ds(pl.multiple_of(other * 512, 512), 512)
    own_q = pl.ds(pl.multiple_of(c * 1024, 1024), 1024)
    own_v = pl.ds(pl.multiple_of(c * 512, 512), 512)
    own_rows = pl.ds(pl.multiple_of(c * 128, 128), 128)
    other_rows = pl.ds(pl.multiple_of(other * 128, 128), 128)
    own_heads = pl.ds(pl.multiple_of(c * 8, 8), 8)
    other_heads = pl.ds(pl.multiple_of(other * 8, 8), 8)
    swaps = [
        remote(src, dst, in_send.at[n], in_recv.at[n], seq_2=other)
        for n, (src, dst) in enumerate(((ss, rs), (sg, rg), (sq, rq)))
    ]

    def toward(n):
        return (y + jnp.where(n == 2, 3, jnp.where(n == 3, 0, 2 - n))) % 4

    def nearby(n):
        return (y + jnp.where(n == 2, 3, jnp.where(n == 3, 2, n))) % 4

    def key_copy(pair):
        cols = pl.ds(pl.multiple_of(pair * 256, 256), 256)
        return remote(
            sk.at[:, cols], rk.at[:, cols], kv_send.at[0], kv_recv.at[0, pair], seq_2=other
        )

    def value_copy(pair):
        cols = pl.ds(pl.multiple_of(pair * 128, 128), 128)
        return remote(
            sv.at[:, cols], rv.at[:, cols], kv_send.at[1], kv_recv.at[1, pair], seq_2=other
        )

    for load in loads[:3]:
        load.wait()
    ds_row = jnp.broadcast_to(ds_in[...].astype(F32), (8, 128))
    ss[0:8, :] = lg_in[other_heads, :]
    for level in range(6):
        ss[8 + 8 * level : 16 + 8 * level, :] = lw_in[level, other_heads, :]
    ss[56:64, :] = ds_row
    loads[3].wait()
    sk[...] = k_in[:, q_cols].astype(F32)
    loads[4].wait()
    sv[...] = v_in[:, v_cols].astype(F32)
    pl.semaphore_wait(barrier, 10)
    swaps[0].start()
    for n in (2, 1, 3, 0):
        key_copy((y + n) % 4).start()
        value_copy((y + n) % 4).start()
    loads[5].wait()
    sg[...] = g_in[:, v_cols].astype(F32)
    loads[6].wait()
    sq[...] = q_in[:, q_cols].astype(F32)
    for swap in swaps[1:]:
        swap.start()
    kb[own_rows, :] = k_in[:, own_q]
    vb[own_rows, :] = v_in[:, own_v]
    gb[own_rows, :] = g_in[:, own_v]
    qb[own_rows, :] = q_in[:, own_q]
    gates[:, own_rows] = lg_in[own_heads, :]
    for level in range(6):
        wts[level, :, own_rows] = lw_in[level, own_heads, :]
    doc[:, own_rows] = ds_row
    ein[...] = jnp.zeros_like(ein)
    xin[...] = jnp.zeros_like(xin)
    pt[128:256, 0:128] = jnp.zeros((128, 128), BF16)
    rt[128:256, 0:128] = jnp.zeros((128, 128), BF16)

    zero_slab = jnp.zeros((128, 128), F32)
    for level, absent in ((0, y % 2 == 0), (1, y < 2), (2, x == 0)):

        @pl.when(absent)
        def _():
            for pair in range(4):
                zr[pair, level] = zero_slab

    swaps[0].wait_recv()
    gates[:, other_rows] = rs[0:8, :]
    for level in range(6):
        wts[level, :, other_rows] = rs[8 + 8 * level : 16 + 8 * level, :]
    doc[:, other_rows] = rs[56:64, :]
    lane = lax.broadcasted_iota(jnp.int32, (8, 256), 1)
    cum_now = prefix(gates[...], lane)
    reset = prefix(doc[...], lane)
    total = cum_now[:, 255:256]
    reset_total = reset[:, 255:256]
    cum[...] = cum_now
    resets[...] = reset
    fs[...] = jnp.where(reset == 0.0, jnp.exp(cum_now), 0.0)
    de[...] = jnp.where(reset == reset_total, jnp.exp(total - cum_now), 0.0)
    decay = jnp.broadcast_to(jnp.where(reset_total == 0.0, jnp.exp(total), 0.0), (8, 128))
    small[...] = decay
    def masks():
        columns = jnp.transpose(
            jnp.concatenate([cum[...], resets[...], jnp.zeros((112, 256), F32)], axis=0)
        )
        for head in range(8):
            cm[head] = jnp.broadcast_to(columns[:, head : head + 1], (256, 128))
        reset_col = jnp.broadcast_to(columns[:, 8:9], (256, 128))
        for half in range(2):
            reset_row = jnp.broadcast_to(resets[0:1, 128 * half : 128 * half + 128], (256, 128))
            s_pos = lax.broadcasted_iota(jnp.int32, (256, 128), 0)
            t_pos = lax.broadcasted_iota(jnp.int32, (256, 128), 1) + 128 * half
            bias[:, 128 * half : 128 * half + 128] = jnp.where(
                (t_pos >= s_pos) & (reset_col == reset_row), 0.0, NEG
            )

    def head_cols(pair, i):
        return pl.ds(pl.multiple_of(pair * 256 + i * 128, 128), 128)

    def pair_cols(pair):
        return pl.ds(pl.multiple_of(pair * 128, 128), 128)

    def sent(kind, at_y):
        return (True, x > 0, at_y % 2 == 1, at_y >= 2)[kind]

    def y1_copy(pair, kind, at_y):
        rows = 136 if kind == 0 else 128
        return remote(
            ys.at[pair, kind, pl.ds(0, rows)], yr.at[at_y, kind, pl.ds(0, rows)],
            y1_send.at[kind], y1_recv.at[kind], seq_1=pair,
        )

    def place(pair, kind, i, slab):
        rows = pl.ds(64 * i, 64)

        @pl.when(pair == y)
        def _():
            yr[y, kind, rows] = slab

        @pl.when(pair != y)
        def _():
            ys[pair, kind, rows] = slab

    def hand_over(pair, kind):
        @pl.when((pair != y) & sent(kind, y))
        def _():
            y1_copy(pair, kind, y).start()

    def state_fwd(pair):
        wide = pl.ds(pl.multiple_of(pair * 256, 256), 256)
        key_copy(pair).wait_recv()
        kb[other_rows, wide] = rk[:, wide].astype(BF16)
        value_copy(pair).wait_recv()
        vb[other_rows, pair_cols(pair)] = rv[:, pair_cols(pair)].astype(BF16)
        vt[pair] = jnp.transpose(vb[:, pair_cols(pair)].astype(F32))
        for i in range(2):
            head = pl.ds(pair * 2 + i, 1)
            value_hi, value_lo = split(vt[pair, pl.ds(64 * i, 64)] * de[head, :])
            state = dot(
                jnp.concatenate([value_hi, value_lo], axis=0), kb[:, head_cols(pair, i)], NN
            )
            place(pair, 0, i, state[0:64] + state[64:128])
            row = small[head, :]

            @pl.when(pair == y)
            def _():
                yr[y, 0, 128 + i : 129 + i] = row

            @pl.when(pair != y)
            def _():
                ys[pair, 0, 128 + i : 129 + i] = row

        hand_over(pair, 0)

    def state_back(pair):
        gt[pair] = jnp.transpose(gb[:, pair_cols(pair)].astype(F32))
        for i in range(2):
            head = pl.ds(pair * 2 + i, 1)
            hi, lo = split(gt[pair, pl.ds(64 * i, 64)] * (fs[head, :] * wts[5, head, :]))
            back = dot(jnp.concatenate([hi, lo], axis=0), qb[:, head_cols(pair, i)], NN)
            place(pair, 1, i, back[0:64] + back[64:128])
        hand_over(pair, 1)

    def state_near(pair):
        for i in range(2):
            head = pl.ds(pair * 2 + i, 1)
            grad = gt[pair, pl.ds(64 * i, 64)]
            parts = [split(grad * (fs[head, :] * wts[level, head, :])) for level in (3, 4)]
            back = dot(
                jnp.concatenate([p[0] for p in parts] + [p[1] for p in parts], axis=0),
                qb[:, head_cols(pair, i)], NN,
            )
            for n in range(2):
                place(
                    pair, 2 + n, i, back[64 * n : 64 * n + 64] + back[128 + 64 * n : 192 + 64 * n]
                )
        hand_over(pair, 2)
        hand_over(pair, 3)

    def intra(pair):
        for i in range(2):
            number = pair * 2 + i
            head = pl.ds(number, 1)
            rows = pl.ds(64 * i, 64)
            query = qb[:, head_cols(pair, i)]
            key = kb[:, head_cols(pair, i)]
            grad = gb[:, pair_cols(pair)]
            value = vb[:, pair_cols(pair)]
            mine = lax.broadcasted_iota(jnp.int32, (64, 128), 1) // 64 == i
            weight = [wts[level, head, :] for level in range(3)]
            span = lax.broadcasted_iota(jnp.int32, (1, 256), 1) // 64
            cum_row = cum[head, :]
            level_rows = [jnp.zeros((1, 256), F32) for level in range(3)]
            drift_row = jnp.zeros((1, 256), F32)
            for b in range(4):
                low = 0 if b < 2 else 128
                blk = slice(64 * b, 64 * b + 64)
                score = dot(key[blk], query[low:256], NT)
                pair_dot = dot(
                    jnp.where(mine, value[blk], jnp.zeros((64, 128), BF16)), grad[low:256], NT
                )
                col = cm[number, blk, :]
                if low == 0:
                    col = jnp.concatenate([col, col], axis=1)
                decayed = jnp.exp((cum_row[:, low:256] - col) + bias[blk, low:256])
                at = span[:, low:256]
                near = (at == b).astype(jnp.int32), ((at ^ 1) == b).astype(jnp.int32)
                mix = jnp.where(
                    near[0] == 1, weight[0][:, low:256],
                    jnp.where(near[1] == 1, weight[1][:, low:256], weight[2][:, low:256]),
                )
                scored = decayed * score
                joint = jnp.sum(scored * pair_dot, axis=0, keepdims=True)
                prob = (scored * mix).astype(BF16)
                pt[blk, low:256] = prob
                rt[blk, low:256] = (decayed * mix * pair_dot).astype(BF16)
                drifted = jnp.sum(prob.astype(F32) * pair_dot, axis=0, keepdims=True)
                if low:
                    pad = jnp.zeros((1, 128), F32)
                    joint = jnp.concatenate([pad, joint], axis=1)
                    drifted = jnp.concatenate([pad, drifted], axis=1)
                drift_row = drift_row + drifted
                level_rows[0] = level_rows[0] + jnp.where(span == b, joint, 0.0)
                level_rows[1] = level_rows[1] + jnp.where((span ^ 1) == b, joint, 0.0)
                level_rows[2] = level_rows[2] + jnp.where(
                    (span != b) & ((span ^ 1) != b), joint, 0.0
                )
            for level in range(3):
                glw[level, head, :] = level_rows[level]
            drift[head, :] = drift_row
            gvt[pair, rows] = dot(gt[pair, rows].astype(BF16), pt[...], NT)
            gk[:, head_cols(pair, i)] = dot(rt[...], query, NN)
            gq[:, head_cols(pair, i)] = dot(rt[...], key, TN)

    def y2_copy(to_y, kind, src):
        return remote(
            src, zr.at[y, kind], y2_send.at[kind], y2_recv.at[y, kind // 3], seq_1=to_y
        )

    def y2_source(to_y, kind):
        if kind == 0:
            return yr.at[to_y - 1, 0, pl.ds(0, 128)]
        return zs.at[to_y, kind]

    def hand_back(to_y, kind):
        def go():
            @pl.when(to_y != y)
            def _():
                y2_copy(to_y, kind, y2_source(to_y, kind)).start()

            @pl.when(to_y == y)
            def _():
                zr[y, kind] = y2_source(to_y, kind)[...]

        if kind == 2:
            pl.when(x > 0)(go)
        else:
            go()

    def several(buf, count, kind, send, recv):
        rows = pl.ds(0, 136 if kind == 0 and buf is ys else 128)
        return remote(
            buf.at[pl.ds(0, count), kind, rows], buf.at[pl.ds(0, count), kind, rows],
            send, recv, seq_2=other,
        )

    def in_turn(kind, here, act):
        pl.when(here)(lambda: act(1))
        pl.when(jnp.logical_not(here))(lambda: act(2))

    def y1_wait(kind):
        def act(count):
            several(ys, count, kind, y1_send.at[kind], y1_recv.at[kind]).wait_recv()

        if kind == 0:
            act(3)
        elif kind == 1:
            pl.when(x > 0)(lambda: act(3))
        else:
            in_turn(kind, y % 2 == 1 if kind == 2 else y >= 2, act)

    def x_copy(to_x, kind):
        return remote(xs.at[kind], xr.at[x], x_send.at[to_x], x_recv.at[x], seq_0=to_x)

    def decays(i):
        return [yr[n, 0, 128 + i : 129 + i] for n in range(4)]

    def combine_fwd():
        y1_wait(0)
        for i in range(2):
            rows = slice(64 * i, 64 * i + 64)
            dec = decays(i)
            both = dec[1] * yr[0, 0, rows] + yr[1, 0, rows]
            zs[2, 1, rows] = both
            after = dec[2] * both
            zs[3, 1, rows] = after
            xs[0, rows] = dec[3] * (after + yr[2, 0, rows]) + yr[3, 0, rows]
            all_decay = dec[0] * dec[1] * (dec[2] * dec[3])
            xs[0, 128 + i : 129 + i] = all_decay
            xs[1, 128 + i : 129 + i] = all_decay
        for to_x in range(4):

            @pl.when(to_x > x)
            def _():
                x_copy(to_x, 0).start()

        hand_back(1, 0)
        hand_back(3, 0)
        hand_back(2, 1)
        hand_back(3, 1)

    def combine_back():
        y1_wait(1)

        @pl.when(x > 0)
        def _():
            for i in range(2):
                rows = slice(64 * i, 64 * i + 64)
                dec = decays(i)
                back = yr[2, 1, rows] + dec[2] * yr[3, 1, rows]
                back = yr[1, 1, rows] + dec[1] * back
                xs[1, rows] = yr[0, 1, rows] + dec[0] * back

        for to_x in range(4):

            @pl.when(to_x < x)
            def _():
                x_copy(to_x, 1).start()


    def take(acc, at_x):
        remote(
            xs.at[0], xr.at[at_x], x_send.at[at_x], x_recv.at[at_x], seq_0=at_x
        ).wait_recv()
        for i in range(2):
            rows = slice(64 * i, 64 * i + 64)
            acc[rows] = xr[at_x, 128 + i : 129 + i] * acc[rows] + xr[at_x, rows]

    def enter_far():
        for at_x in range(4):
            pl.when(at_x < x)(functools.partial(take, ein, at_x))
        for i in range(2):
            rows = slice(64 * i, 64 * i + 64)
            dec = decays(i)
            into = ein[rows]
            for at_y in range(4):
                zs[at_y, 2, rows] = into
                into = dec[at_y] * into
        for step in (2, 1, 3, 0):
            hand_back((y + step) % 4, 2)

    def leave_far():
        y1_wait(2)
        y1_wait(3)
        for at_x in range(3, -1, -1):
            pl.when(at_x > x)(functools.partial(take, xin, at_x))
        for i in range(2):
            rows = slice(64 * i, 64 * i + 64)
            dec = decays(i)
            late = xin[rows]
            zs[3, 3, rows] = late
            late = dec[3] * late
            zs[2, 3, rows] = late + yr[3, 2, rows]
            late = dec[2] * late + (yr[2, 3, rows] + dec[2] * yr[3, 3, rows])
            zs[1, 3, rows] = late
            zs[0, 3, rows] = dec[1] * late + yr[1, 2, rows]
        for step in (2, 1, 3, 0):
            hand_back((y + step) % 4, 3)

    def back_copy(pair, kind):
        if kind == 2:
            cols, src, dst = pair_cols(pair), gv, bv
        else:
            cols = pl.ds(pl.multiple_of(pair * 256, 256), 256)
            src, dst = ((gq, bq), (gk, bk))[kind]
        return remote(
            src.at[other_rows, cols], dst.at[:, cols],
            out_send.at[kind], out_recv.at[kind], seq_2=other,
        )

    def y2_wait(pair, first, count):
        remote(
            zr.at[pair, pl.ds(0, count)], zr.at[pair, pl.ds(0, count)], y2_send.at[0],
            y2_recv.at[pair, first // 3], seq_1=pair,
        ).wait_recv()

    def cross_in(pair):
        levels_in = y % 2 + y // 2 + (x > 0).astype(jnp.int32)
        for count in range(1, 4):
            pl.when((pair != y) & (levels_in == count))(
                functools.partial(y2_wait, pair, 0, count)
            )
        for i in range(2):
            head = pl.ds(pair * 2 + i, 1)
            rows = pl.ds(64 * i, 64)
            grad = gt[pair, rows]
            enter_hi, enter_lo = split(
                jnp.concatenate([zr[pair, n, rows] for n in range(3)], axis=0)
            )
            mixed = dot(
                jnp.concatenate([enter_hi, enter_lo], axis=0), qb[:, head_cols(pair, i)], NT
            )
            drift_row = drift[head, :]
            for n in range(3):
                state_row = mixed[64 * n : 64 * n + 64] + mixed[192 + 64 * n : 256 + 64 * n]
                level_row = fs[head, :] * jnp.sum(state_row * grad, axis=0, keepdims=True)
                glw[3 + n, head, :] = level_row
                drift_row = drift_row + wts[3 + n, head, :] * level_row
            drift[head, :] = drift_row

    def cross_out(pair):
        pl.when(pair != y)(functools.partial(y2_wait, pair, 3, 1))
        for i in range(2):
            head = pl.ds(pair * 2 + i, 1)
            rows = pl.ds(64 * i, 64)
            leave_hi, leave_lo = split(zr[pair, 3, rows])
            left = dot(
                jnp.concatenate([leave_hi, leave_lo], axis=0), kb[:, head_cols(pair, i)], NT
            )
            value_grad = gvt[pair, rows] + de[head, :] * (left[0:64] + left[64:128])
            gvt[pair, rows] = value_grad
            drift[head, :] = drift[head, :] - jnp.sum(
                vt[pair, rows] * value_grad, axis=0, keepdims=True
            )

    def cross_query(pair):
        for i in range(2):
            head = pl.ds(pair * 2 + i, 1)
            rows = pl.ds(64 * i, 64)
            enter_hi, enter_lo = split(
                jnp.concatenate([zr[pair, n, rows] for n in range(3)], axis=0)
            )
            weighted_hi, weighted_lo = split(
                jnp.concatenate(
                    [gt[pair, rows] * (fs[head, :] * wts[3 + n, head, :]) for n in range(3)], axis=0
                )
            )
            gq[:, head_cols(pair, i)] = gq[:, head_cols(pair, i)] + dot(
                jnp.concatenate([weighted_hi, weighted_lo, weighted_hi], axis=0),
                jnp.concatenate([enter_hi, enter_hi, enter_lo], axis=0), TN,
            )
        back_copy(pair, 0).start()
        wide = pl.ds(pl.multiple_of(pair * 256, 256), 256)
        out_wide = pl.ds(pl.multiple_of(c * 1024 + pair * 256, 256), 256)
        gq_out[:, out_wide] = gq[own_rows, wide].astype(BF16)

    def cross_grad(pair):
        for i in range(2):
            head = pl.ds(pair * 2 + i, 1)
            rows = pl.ds(64 * i, 64)
            leave_hi, leave_lo = split(zr[pair, 3, rows])
            ended_hi, ended_lo = split(vt[pair, rows] * de[head, :])
            gk[:, head_cols(pair, i)] = gk[:, head_cols(pair, i)] + dot(
                jnp.concatenate([ended_hi, ended_lo, ended_hi], axis=0),
                jnp.concatenate([leave_hi, leave_hi, leave_lo], axis=0), TN,
            )
        gv[:, pair_cols(pair)] = jnp.transpose(gvt[pair])
        back_copy(pair, 1).start()
        back_copy(pair, 2).start()
        wide = pl.ds(pl.multiple_of(pair * 256, 256), 256)
        out_wide = pl.ds(pl.multiple_of(c * 1024 + pair * 256, 256), 256)
        out_narrow = pl.ds(pl.multiple_of(c * 512 + pair * 128, 128), 128)
        gk_out[:, out_wide] = gk[own_rows, wide].astype(BF16)
        gv_out[:, out_narrow] = gv[own_rows, pair_cols(pair)].astype(BF16)

    def loop(low, high, body):
        def step(n, carry):
            body(n)
            return carry

        lax.fori_loop(low, high, step, 0)

    loop(0, 4, lambda n: state_fwd(toward(n)))
    swaps[1].wait_recv()
    gb[other_rows, :] = rg[...].astype(BF16)
    swaps[2].wait_recv()
    qb[other_rows, :] = rq[...].astype(BF16)
    loop(0, 4, lambda n: state_back(toward(n)))
    loop(0, 4, lambda n: state_near(toward(n)))
    combine_fwd()
    masks()
    loop(0, 1, intra)
    combine_back()
    loop(1, 2, intra)
    enter_far()
    loop(2, 4, intra)
    leave_far()
    loop(0, 4, lambda n: cross_in(nearby(n)))
    loop(0, 4, lambda n: cross_out(nearby(n)))
    lane = lax.broadcasted_iota(jnp.int32, (8, 256), 1)
    tail = suffix(drift[...], lane)
    drift[...] = tail
    bs_out = remote(small.at[:, :], bs.at[pl.ds(48, 8), :], last_send.at[1], last_recv.at[1], seq_2=other)
    tile = lax.broadcasted_iota(jnp.int32, (8, 128), 1)
    mine = lax.broadcasted_iota(jnp.int32, (8, 128), 0)
    head_total = tail[:, 0:1]
    head_square = jnp.sum(tail * tail, axis=1, keepdims=True)
    head_sum = jnp.sum(tail, axis=1, keepdims=True)
    slots = [
        jnp.where(tile == mine + 8 * n, jnp.broadcast_to(part, (8, 128)), 0.0)
        for n, part in enumerate((head_total, head_square, head_sum))
    ]
    place_here = chip * 8 + group
    a_buf[place_here] = jnp.sum(slots[0] + slots[1] + slots[2], axis=0, keepdims=True)

    def a_copy(dx, dy, dz, dc):
        return remote(
            a_buf.at[place_here], a_buf.at[place_here], a_send.at[0], a_recv.at[0],
            seq_0=(x + dx) % 4, seq_1=(y + dy) % 4, seq_2=(c + dc) % 2, head=(z + dz) % 4,
        )

    def hops(move):
        return -(sum(min(d, 4 - d) for d in move[:3]) + 0.5 * move[3])

    moves = [(dx, dy, dz, dc) for dx in range(4) for dy in range(4) for dz in range(4) for dc in (0, 1)]
    for move in sorted(moves, key=hops):
        if any(move):
            a_copy(*move).start()
    small[...] = drift[:, other_rows]
    for level in range(6):
        ss_rows = slice(8 * level, 8 * level + 8)
        ys[y, 1, ss_rows] = glw[level, :, other_rows]
    glw_copy = remote(
        ys.at[y, 1, pl.ds(0, 48)], bs.at[pl.ds(0, 48), :], last_send.at[0], last_recv.at[0],
        seq_2=other,
    )
    glw_copy.start()
    bs_out.start()
    for level in range(6):
        glw_out[level, own_heads, :] = glw[level, :, own_rows]

    loop(0, 4, cross_query)
    loop(0, 4, cross_grad)
    def back_whole(kind):
        src, dst = ((gq, bq), (gk, bk), (gv, bv))[kind]
        return remote(
            src.at[other_rows, :], dst, out_send.at[kind], out_recv.at[kind], seq_2=other
        )

    for kind in range(3):
        back_whole(kind).wait_recv()
    other_q = pl.ds(pl.multiple_of(other * 1024, 1024), 1024)
    other_v = pl.ds(pl.multiple_of(other * 512, 512), 512)
    gq_out[:, other_q] = bq[...].astype(BF16)
    gk_out[:, other_q] = bk[...].astype(BF16)
    gv_out[:, other_v] = bv[...].astype(BF16)
    glw_copy.wait_recv()
    for level in range(6):
        glw_out[level, other_heads, :] = bs[8 * level : 8 * level + 8, :]

    a_whole = remote(
        a_buf.at[pl.ds(0, 127)], a_buf.at[pl.ds(0, 127)], a_send.at[0], a_recv.at[0], seq_2=other
    )
    a_whole.wait_recv()
    run = jnp.zeros((8, 128), F32)
    later = jnp.zeros((8, 128), F32)
    squares = jnp.zeros((8, 128), F32)
    for at in range(15, -1, -1):
        now = a_buf[8 * at : 8 * at + 8, 0, :]
        later = later + run * (chip == at).astype(F32)
        square = pltpu.roll(now, 120, 1)
        total_of = pltpu.roll(now, 112, 1)
        squares = squares + square + run * (2.0 * total_of + 256.0 * run)
        run = run + now
    squares = jnp.where(tile < 8, squares, 0.0)
    total_square = jnp.sum(jnp.sum(squares, axis=1, keepdims=True), axis=0, keepdims=True)
    factor = jnp.minimum(1.0, lax.rsqrt(total_square / (64 * 4096) + 1e-06))

    def later_of(at_group):
        row = jnp.sum(jnp.where(mine == at_group, later, 0.0), axis=0, keepdims=True)
        return jnp.sum(
            jnp.where(tile == mine, jnp.broadcast_to(row, (8, 128)), 0.0), axis=1, keepdims=True
        )

    glg_out[own_heads, :] = (drift[:, own_rows] + later_of(group)) * factor
    bs_out.wait_recv()
    glg_out[other_heads, :] = (bs[48:56, :] + later_of(z * 2 + other)) * factor

    for swap in swaps:
        swap.wait_send()
    remote(sk, rk, kv_send.at[0], kv_recv.at[0, 0], seq_2=other).wait_send()
    remote(sv, rv, kv_send.at[1], kv_recv.at[1, 0], seq_2=other).wait_send()
    for kind in range(4):

        @pl.when(sent(kind, y))
        def _():
            several(ys, 3, kind, y1_send.at[kind], y1_recv.at[kind]).wait_send()

        def act(count):
            several(zs, count, kind, y2_send.at[kind], y2_recv.at[0, 0]).wait_send()

        if kind < 2:
            in_turn(kind, y % 2 == 1 if kind == 0 else y >= 2, act)
        else:
            pl.when(x > 0 if kind == 2 else y >= 0)(lambda: act(3))

    for pair in range(4):
        @pl.when(pair != x)
        def _():
            x_copy(pair, 0).wait_send()

    for kind in range(3):
        back_whole(kind).wait_send()
    glw_copy.wait_send()
    bs_out.wait_send()
    a_whole.wait_send()


def settle(*refs):
    source, target, sem = refs[:5], refs[5:10], refs[10]
    stores = []
    for n in range(5):
        cuts = 4 if n < 2 else 2 if n == 2 else 1
        rows = source[n].shape[0] // cuts
        for m in range(cuts):
            at = pl.ds(rows * m, rows)
            stores.append(
                pltpu.make_async_copy(source[n].at[at], target[n].at[at], sem.at[len(stores)])
            )
    for store in stores:
        store.start()
    for store in stores:
        store.wait()


def shards(queries, keys, values, out_grad, log_gate, level_weight, doc_start):
    args = (queries, keys, values, out_grad, log_gate, level_weight, doc_start.reshape(1, -1))
    anywhere = pl.BlockSpec(memory_space=pl.ANY)
    results = tuple(
        jax.ShapeDtypeStruct(a.shape, a.dtype)
        for a in (queries, keys, values, level_weight, log_gate)
    )
    held = tuple(pltpu.VMEM(r.shape, r.dtype) for r in results)
    scratch = [pltpu.VMEM(a.shape, a.dtype) for a in args] + [pltpu.SemaphoreType.DMA((7,))]
    swap = [(128, 1024), (128, 1024), (128, 512), (128, 512), (64, 128)]
    scratch += [pltpu.VMEM(s, F32) for s in swap * 2]
    scratch += [pltpu.VMEM(s, BF16) for s in ((256, 1024), (256, 1024), (256, 512), (256, 512))]
    scratch += [pltpu.VMEM((4, 128, 256), F32)] * 2
    scratch += [pltpu.VMEM((8, 256), F32)] * 6
    scratch += [pltpu.VMEM((6, 8, 256), F32), pltpu.VMEM((8, 256, 128), F32)]
    scratch += [pltpu.VMEM((256, 256), F32), pltpu.VMEM((256, 256), BF16), pltpu.VMEM((256, 256), BF16)]
    scratch += [pltpu.VMEM((256, 1024), F32), pltpu.VMEM((256, 1024), F32), pltpu.VMEM((256, 512), F32)]
    scratch += [pltpu.VMEM((4, 128, 256), F32), pltpu.VMEM((6, 8, 256), F32)]
    scratch += [pltpu.VMEM((8, 256), F32), pltpu.VMEM((8, 128), F32)]
    scratch += [pltpu.VMEM((4, 4, 136, 128), F32)] * 2 + [pltpu.VMEM((4, 4, 128, 128), F32)] * 2
    scratch += [pltpu.VMEM((2, 136, 128), F32), pltpu.VMEM((4, 136, 128), F32)]
    scratch += [pltpu.VMEM((128, 128), F32)] * 2
    scratch += [pltpu.VMEM((128, 1024), F32), pltpu.VMEM((128, 1024), F32), pltpu.VMEM((128, 512), F32)]
    scratch += [pltpu.VMEM((56, 128), F32)]
    scratch += [pltpu.VMEM((128, 1, 128), F32)]
    sems = [(3,), (3,), (2,), (2, 4), (4,), (4,), (4,), (4, 2), (4,), (4,), (3,), (3,), (2,), (2,)]
    sems += [(1,)] * 2
    scratch += [pltpu.SemaphoreType.DMA(s) for s in sems]
    outs = pl.pallas_call(
        kernel,
        out_shape=held,
        in_specs=[anywhere] * 7,
        out_specs=[pl.BlockSpec(memory_space=pltpu.VMEM)] * 5,
        scratch_shapes=scratch,
        compiler_params=pltpu.CompilerParams(
            collective_id=0, has_side_effects=True, vmem_limit_bytes=60 * 2**20
        ),
    )(*args)
    return pl.pallas_call(
        settle,
        out_shape=results,
        in_specs=[anywhere] * 5,
        out_specs=[anywhere] * 5,
        scratch_shapes=[pltpu.SemaphoreType.DMA((12,))],
        compiler_params=pltpu.CompilerParams(vmem_limit_bytes=48 * 2**20),
    )(*outs)


def solution(mesh):
    finer = Mesh(
        mesh.devices.reshape(4, 4, 2, mesh.shape["head"]), ("seq_0", "seq_1", "seq_2", "head")
    )
    wide = P(SEQ, "head")
    return jax.shard_map(
        shards,
        mesh=finer,
        in_specs=(wide, wide, wide, wide, P("head", SEQ), P(None, "head", SEQ), P(SEQ)),
        out_specs=(wide, wide, wide, P(None, "head", SEQ), P("head", SEQ)),
        check_vma=False,
    )
```

```python
import functools

import jax
import jax.numpy as jnp
from jax import lax
from jax.experimental import pallas as pl
from jax.experimental.pallas import tpu as pltpu
from jax.sharding import Mesh
from jax.sharding import PartitionSpec as P

SEQ = ("seq_0", "seq_1", "seq_2")
MESH = pl.DeviceIdType.MESH
F32 = jnp.float32
BF16 = jnp.bfloat16
NEG = -1e30

NN = (((1,), (0,)), ((), ()))
NT = (((1,), (1,)), ((), ()))
TN = (((0,), (0,)), ((), ()))


def dot(a, b, dims):
    return lax.dot_general(a, b, dims, preferred_element_type=F32)


def split(a):
    hi = a.astype(BF16)
    return hi, (a - hi.astype(F32)).astype(BF16)


def prefix(a, lane):
    shift = 1
    while shift < a.shape[1]:
        a = a + jnp.where(lane >= shift, pltpu.roll(a, shift, 1), 0.0)
        shift *= 2
    return a


def suffix(a, lane):
    size = a.shape[1]
    shift = 1
    while shift < size:
        a = a + jnp.where(lane < size - shift, pltpu.roll(a, size - shift, 1), 0.0)
        shift *= 2
    return a


def kernel(
    q_hbm, k_hbm, v_hbm, g_hbm, lg_hbm, lw_hbm, ds_hbm,
    gq_out, gk_out, gv_out, glw_out, glg_out,
    q_in, k_in, v_in, g_in, lg_in, lw_in, ds_in, load_sem,
    sq, sk, sv, sg, ss, rq, rk, rv, rg, rs,
    qb, kb, vb, gb, vt, gt,
    gates, doc, cum, resets, fs, de, wts, cm, bias, pt, rt,
    gq, gk, gv, gvt, glw, drift, small,
    ys, yr, zs, zr, xs, xr, ein, xin,
    bq, bk, bv, bs,
    a_buf,
    in_send, in_recv, kv_send, kv_recv, y1_send, y1_recv, y2_send, y2_recv, x_send, x_recv,
    out_send, out_recv, last_send, last_recv, a_send, a_recv,
):
    x, y, c, z = (lax.axis_index(n) for n in ("seq_0", "seq_1", "seq_2", "head"))
    other = 1 - c
    chip = x * 4 + y
    group = z * 2 + c

    def remote(src, dst, send, recv, **to):
        return pltpu.make_async_remote_copy(
            src_ref=src, dst_ref=dst, send_sem=send, recv_sem=recv,
            device_id=to, device_id_type=MESH,
        )

    loads = [
        pltpu.make_async_copy(src, dst, load_sem.at[n])
        for n, (src, dst) in enumerate((
            (ds_hbm, ds_in), (lg_hbm, lg_in), (lw_hbm, lw_in), (k_hbm, k_in),
            (v_hbm, v_in), (g_hbm, g_in), (q_hbm, q_in),
        ))
    ]
    for load in loads:
        load.start()

    barrier = pltpu.get_barrier_semaphore()
    for step in range(1, 4):
        for axis, place in (("seq_1", y), ("seq_0", x)):
            pl.semaphore_signal(
                barrier, inc=1, device_id={axis: (place + step) % 4}, device_id_type=MESH
            )
        pl.semaphore_signal(
            barrier, inc=1, device_id={"head": (z + step) % 4}, device_id_type=MESH
        )
    pl.semaphore_signal(barrier, inc=1, device_id={"seq_2": other}, device_id_type=MESH)

    q_cols = pl.ds(pl.multiple_of(other * 1024, 1024), 1024)
    v_cols = pl.ds(pl.multiple_of(other * 512, 512), 512)
    own_q = pl.ds(pl.multiple_of(c * 1024, 1024), 1024)
    own_v = pl.ds(pl.multiple_of(c * 512, 512), 512)
    own_rows = pl.ds(pl.multiple_of(c * 128, 128), 128)
    other_rows = pl.ds(pl.multiple_of(other * 128, 128), 128)
    own_heads = pl.ds(pl.multiple_of(c * 8, 8), 8)
    other_heads = pl.ds(pl.multiple_of(other * 8, 8), 8)
    swaps = [
        remote(src, dst, in_send.at[n], in_recv.at[n], seq_2=other)
        for n, (src, dst) in enumerate(((ss, rs), (sg, rg), (sq, rq)))
    ]

    def toward(n):
        return (y + jnp.where(n == 2, 3, jnp.where(n == 3, 0, 2 - n))) % 4

    def nearby(n):
        return (y + jnp.where(n == 2, 3, jnp.where(n == 3, 2, n))) % 4

    def key_copy(pair):
        cols = pl.ds(pl.multiple_of(pair * 256, 256), 256)
        return remote(
            sk.at[:, cols], rk.at[:, cols], kv_send.at[0], kv_recv.at[0, pair], seq_2=other
        )

    def value_copy(pair):
        cols = pl.ds(pl.multiple_of(pair * 128, 128), 128)
        return remote(
            sv.at[:, cols], rv.at[:, cols], kv_send.at[1], kv_recv.at[1, pair], seq_2=other
        )

    for load in loads[:3]:
        load.wait()
    ds_row = jnp.broadcast_to(ds_in[...].astype(F32), (8, 128))
    ss[0:8, :] = lg_in[other_heads, :]
    for level in range(6):
        ss[8 + 8 * level : 16 + 8 * level, :] = lw_in[level, other_heads, :]
    ss[56:64, :] = ds_row
    loads[3].wait()
    sk[...] = k_in[:, q_cols].astype(F32)
    loads[4].wait()
    sv[...] = v_in[:, v_cols].astype(F32)
    pl.semaphore_wait(barrier, 10)
    swaps[0].start()
    for n in (2, 1, 3, 0):
        key_copy((y + n) % 4).start()
        value_copy((y + n) % 4).start()
    loads[5].wait()
    sg[...] = g_in[:, v_cols].astype(F32)
    loads[6].wait()
    sq[...] = q_in[:, q_cols].astype(F32)
    for swap in swaps[1:]:
        swap.start()
    kb[own_rows, :] = k_in[:, own_q]
    vb[own_rows, :] = v_in[:, own_v]
    gb[own_rows, :] = g_in[:, own_v]
    qb[own_rows, :] = q_in[:, own_q]
    gates[:, own_rows] = lg_in[own_heads, :]
    for level in range(6):
        wts[level, :, own_rows] = lw_in[level, own_heads, :]
    doc[:, own_rows] = ds_row
    ein[...] = jnp.zeros_like(ein)
    xin[...] = jnp.zeros_like(xin)
    pt[128:256, 0:128] = jnp.zeros((128, 128), BF16)
    rt[128:256, 0:128] = jnp.zeros((128, 128), BF16)

    zero_slab = jnp.zeros((128, 128), F32)
    for level, absent in ((0, y % 2 == 0), (1, y < 2), (2, x == 0)):

        @pl.when(absent)
        def _():
            for pair in range(4):
                zr[pair, level] = zero_slab

    swaps[0].wait_recv()
    gates[:, other_rows] = rs[0:8, :]
    for level in range(6):
        wts[level, :, other_rows] = rs[8 + 8 * level : 16 + 8 * level, :]
    doc[:, other_rows] = rs[56:64, :]
    lane = lax.broadcasted_iota(jnp.int32, (8, 256), 1)
    cum_now = prefix(gates[...], lane)
    reset = prefix(doc[...], lane)
    total = cum_now[:, 255:256]
    reset_total = reset[:, 255:256]
    cum[...] = cum_now
    resets[...] = reset
    fs[...] = jnp.where(reset == 0.0, jnp.exp(cum_now), 0.0)
    de[...] = jnp.where(reset == reset_total, jnp.exp(total - cum_now), 0.0)
    decay = jnp.broadcast_to(jnp.where(reset_total == 0.0, jnp.exp(total), 0.0), (8, 128))
    small[...] = decay
    def masks():
        columns = jnp.transpose(
            jnp.concatenate([cum[...], resets[...], jnp.zeros((112, 256), F32)], axis=0)
        )
        for head in range(8):
            cm[head] = jnp.broadcast_to(columns[:, head : head + 1], (256, 128))
        reset_col = jnp.broadcast_to(columns[:, 8:9], (256, 128))
        for half in range(2):
            reset_row = jnp.broadcast_to(resets[0:1, 128 * half : 128 * half + 128], (256, 128))
            s_pos = lax.broadcasted_iota(jnp.int32, (256, 128), 0)
            t_pos = lax.broadcasted_iota(jnp.int32, (256, 128), 1) + 128 * half
            bias[:, 128 * half : 128 * half + 128] = jnp.where(
                (t_pos >= s_pos) & (reset_col == reset_row), 0.0, NEG
            )

    def head_cols(pair, i):
        return pl.ds(pl.multiple_of(pair * 256 + i * 128, 128), 128)

    def pair_cols(pair):
        return pl.ds(pl.multiple_of(pair * 128, 128), 128)

    def sent(kind, at_y):
        return (True, x > 0, at_y % 2 == 1, at_y >= 2)[kind]

    def y1_copy(pair, kind, at_y):
        rows = 136 if kind == 0 else 128
        return remote(
            ys.at[pair, kind, pl.ds(0, rows)], yr.at[at_y, kind, pl.ds(0, rows)],
            y1_send.at[kind], y1_recv.at[kind], seq_1=pair,
        )

    def place(pair, kind, i, slab):
        rows = pl.ds(64 * i, 64)

        @pl.when(pair == y)
        def _():
            yr[y, kind, rows] = slab

        @pl.when(pair != y)
        def _():
            ys[pair, kind, rows] = slab

    def hand_over(pair, kind):
        @pl.when((pair != y) & sent(kind, y))
        def _():
            y1_copy(pair, kind, y).start()

    def state_fwd(pair):
        wide = pl.ds(pl.multiple_of(pair * 256, 256), 256)
        key_copy(pair).wait_recv()
        kb[other_rows, wide] = rk[:, wide].astype(BF16)
        value_copy(pair).wait_recv()
        vb[other_rows, pair_cols(pair)] = rv[:, pair_cols(pair)].astype(BF16)
        vt[pair] = jnp.transpose(vb[:, pair_cols(pair)].astype(F32))
        for i in range(2):
            head = pl.ds(pair * 2 + i, 1)
            value_hi, value_lo = split(vt[pair, pl.ds(64 * i, 64)] * de[head, :])
            state = dot(
                jnp.concatenate([value_hi, value_lo], axis=0), kb[:, head_cols(pair, i)], NN
            )
            place(pair, 0, i, state[0:64] + state[64:128])
            row = small[head, :]

            @pl.when(pair == y)
            def _():
                yr[y, 0, 128 + i : 129 + i] = row

            @pl.when(pair != y)
            def _():
                ys[pair, 0, 128 + i : 129 + i] = row

        hand_over(pair, 0)

    def state_back(pair):
        gt[pair] = jnp.transpose(gb[:, pair_cols(pair)].astype(F32))
        for i in range(2):
            head = pl.ds(pair * 2 + i, 1)
            hi, lo = split(gt[pair, pl.ds(64 * i, 64)] * (fs[head, :] * wts[5, head, :]))
            back = dot(jnp.concatenate([hi, lo], axis=0), qb[:, head_cols(pair, i)], NN)
            place(pair, 1, i, back[0:64] + back[64:128])
        hand_over(pair, 1)

    def state_near(pair):
        for i in range(2):
            head = pl.ds(pair * 2 + i, 1)
            grad = gt[pair, pl.ds(64 * i, 64)]
            parts = [split(grad * (fs[head, :] * wts[level, head, :])) for level in (3, 4)]
            back = dot(
                jnp.concatenate([p[0] for p in parts] + [p[1] for p in parts], axis=0),
                qb[:, head_cols(pair, i)], NN,
            )
            for n in range(2):
                place(
                    pair, 2 + n, i, back[64 * n : 64 * n + 64] + back[128 + 64 * n : 192 + 64 * n]
                )
        hand_over(pair, 2)
        hand_over(pair, 3)

    def intra(pair):
        for i in range(2):
            number = pair * 2 + i
            head = pl.ds(number, 1)
            rows = pl.ds(64 * i, 64)
            query = qb[:, head_cols(pair, i)]
            key = kb[:, head_cols(pair, i)]
            grad = gb[:, pair_cols(pair)]
            value = vb[:, pair_cols(pair)]
            mine = lax.broadcasted_iota(jnp.int32, (64, 128), 1) // 64 == i
            weight = [wts[level, head, :] for level in range(3)]
            span = lax.broadcasted_iota(jnp.int32, (1, 256), 1) // 64
            cum_row = cum[head, :]
            level_rows = [jnp.zeros((1, 256), F32) for level in range(3)]
            drift_row = jnp.zeros((1, 256), F32)
            for b in range(4):
                low = 0 if b < 2 else 128
                blk = slice(64 * b, 64 * b + 64)
                score = dot(key[blk], query[low:256], NT)
                pair_dot = dot(
                    jnp.where(mine, value[blk], jnp.zeros((64, 128), BF16)), grad[low:256], NT
                )
                col = cm[number, blk, :]
                if low == 0:
                    col = jnp.concatenate([col, col], axis=1)
                decayed = jnp.exp((cum_row[:, low:256] - col) + bias[blk, low:256])
                at = span[:, low:256]
                near = (at == b).astype(jnp.int32), ((at ^ 1) == b).astype(jnp.int32)
                mix = jnp.where(
                    near[0] == 1, weight[0][:, low:256],
                    jnp.where(near[1] == 1, weight[1][:, low:256], weight[2][:, low:256]),
                )
                scored = decayed * score
                joint = jnp.sum(scored * pair_dot, axis=0, keepdims=True)
                prob = (scored * mix).astype(BF16)
                pt[blk, low:256] = prob
                rt[blk, low:256] = (decayed * mix * pair_dot).astype(BF16)
                drifted = jnp.sum(prob.astype(F32) * pair_dot, axis=0, keepdims=True)
                if low:
                    pad = jnp.zeros((1, 128), F32)
                    joint = jnp.concatenate([pad, joint], axis=1)
                    drifted = jnp.concatenate([pad, drifted], axis=1)
                drift_row = drift_row + drifted
                level_rows[0] = level_rows[0] + jnp.where(span == b, joint, 0.0)
                level_rows[1] = level_rows[1] + jnp.where((span ^ 1) == b, joint, 0.0)
                level_rows[2] = level_rows[2] + jnp.where(
                    (span != b) & ((span ^ 1) != b), joint, 0.0
                )
            for level in range(3):
                glw[level, head, :] = level_rows[level]
            drift[head, :] = drift_row
            gvt[pair, rows] = dot(gt[pair, rows].astype(BF16), pt[...], NT)
            gk[:, head_cols(pair, i)] = dot(rt[...], query, NN)
            gq[:, head_cols(pair, i)] = dot(rt[...], key, TN)

    def y2_copy(to_y, kind, src):
        return remote(
            src, zr.at[y, kind], y2_send.at[kind], y2_recv.at[y, kind // 3], seq_1=to_y
        )

    def y2_source(to_y, kind):
        if kind == 0:
            return yr.at[to_y - 1, 0, pl.ds(0, 128)]
        return zs.at[to_y, kind]

    def hand_back(to_y, kind):
        def go():
            @pl.when(to_y != y)
            def _():
                y2_copy(to_y, kind, y2_source(to_y, kind)).start()

            @pl.when(to_y == y)
            def _():
                zr[y, kind] = y2_source(to_y, kind)[...]

        if kind == 2:
            pl.when(x > 0)(go)
        else:
            go()

    def several(buf, count, kind, send, recv):
        rows = pl.ds(0, 136 if kind == 0 and buf is ys else 128)
        return remote(
            buf.at[pl.ds(0, count), kind, rows], buf.at[pl.ds(0, count), kind, rows],
            send, recv, seq_2=other,
        )

    def in_turn(kind, here, act):
        pl.when(here)(lambda: act(1))
        pl.when(jnp.logical_not(here))(lambda: act(2))

    def y1_wait(kind):
        def act(count):
            several(ys, count, kind, y1_send.at[kind], y1_recv.at[kind]).wait_recv()

        if kind == 0:
            act(3)
        elif kind == 1:
            pl.when(x > 0)(lambda: act(3))
        else:
            in_turn(kind, y % 2 == 1 if kind == 2 else y >= 2, act)

    def x_copy(to_x, kind):
        return remote(xs.at[kind], xr.at[x], x_send.at[to_x], x_recv.at[x], seq_0=to_x)

    def decays(i):
        return [yr[n, 0, 128 + i : 129 + i] for n in range(4)]

    def combine_fwd():
        y1_wait(0)
        for i in range(2):
            rows = slice(64 * i, 64 * i + 64)
            dec = decays(i)
            both = dec[1] * yr[0, 0, rows] + yr[1, 0, rows]
            zs[2, 1, rows] = both
            after = dec[2] * both
            zs[3, 1, rows] = after
            xs[0, rows] = dec[3] * (after + yr[2, 0, rows]) + yr[3, 0, rows]
            all_decay = dec[0] * dec[1] * (dec[2] * dec[3])
            xs[0, 128 + i : 129 + i] = all_decay
            xs[1, 128 + i : 129 + i] = all_decay
        for to_x in range(4):

            @pl.when(to_x > x)
            def _():
                x_copy(to_x, 0).start()

        @pl.when(y % 2 == 1)
        def _():
            zr[y, 0] = yr[(y + 3) % 4, 0, 0:128]

        hand_back(2, 1)
        hand_back(3, 1)

    def combine_back():
        y1_wait(1)

        @pl.when(x > 0)
        def _():
            for i in range(2):
                rows = slice(64 * i, 64 * i + 64)
                dec = decays(i)
                back = yr[2, 1, rows] + dec[2] * yr[3, 1, rows]
                back = yr[1, 1, rows] + dec[1] * back
                xs[1, rows] = yr[0, 1, rows] + dec[0] * back

        for to_x in range(4):

            @pl.when(to_x < x)
            def _():
                x_copy(to_x, 1).start()


    def next_copy(pair, src):
        return remote(
            src, zr.at[pair, 0], y2_send.at[0], y2_recv.at[pair, 0], seq_1=(y + 1) % 4
        )

    def hand_next(pair):
        @pl.when((y % 2 == 0) & (pair == y))
        def _():
            next_copy(pair, yr.at[y, 0, pl.ds(0, 128)]).start()

        @pl.when((y % 2 == 0) & (pair != y) & (pair != y + 1))
        def _():
            next_copy(pair, ys.at[pair, 0, pl.ds(0, 128)]).start()

    def take(acc, at_x):
        remote(
            xs.at[0], xr.at[at_x], x_send.at[at_x], x_recv.at[at_x], seq_0=at_x
        ).wait_recv()
        for i in range(2):
            rows = slice(64 * i, 64 * i + 64)
            acc[rows] = xr[at_x, 128 + i : 129 + i] * acc[rows] + xr[at_x, rows]

    def enter_far():
        for at_x in range(4):
            pl.when(at_x < x)(functools.partial(take, ein, at_x))
        for i in range(2):
            rows = slice(64 * i, 64 * i + 64)
            dec = decays(i)
            into = ein[rows]
            for at_y in range(4):
                zs[at_y, 2, rows] = into
                into = dec[at_y] * into
        for step in (2, 1, 3, 0):
            hand_back((y + step) % 4, 2)

    def leave_far():
        y1_wait(2)
        y1_wait(3)
        for at_x in range(3, -1, -1):
            pl.when(at_x > x)(functools.partial(take, xin, at_x))
        for i in range(2):
            rows = slice(64 * i, 64 * i + 64)
            dec = decays(i)
            late = xin[rows]
            zs[3, 3, rows] = late
            late = dec[3] * late
            zs[2, 3, rows] = late + yr[3, 2, rows]
            late = dec[2] * late + (yr[2, 3, rows] + dec[2] * yr[3, 3, rows])
            zs[1, 3, rows] = late
            zs[0, 3, rows] = dec[1] * late + yr[1, 2, rows]
        for step in (2, 1, 3, 0):
            hand_back((y + step) % 4, 3)

    def back_copy(pair, kind):
        if kind == 2:
            cols, src, dst = pair_cols(pair), gv, bv
        else:
            cols = pl.ds(pl.multiple_of(pair * 256, 256), 256)
            src, dst = ((gq, bq), (gk, bk))[kind]
        return remote(
            src.at[other_rows, cols], dst.at[:, cols],
            out_send.at[kind], out_recv.at[kind], seq_2=other,
        )

    def y2_wait(pair, first, count):
        remote(
            zr.at[pair, pl.ds(0, count)], zr.at[pair, pl.ds(0, count)], y2_send.at[0],
            y2_recv.at[pair, first // 3], seq_1=pair,
        ).wait_recv()

    def cross_in(pair):
        levels_in = y % 2 + y // 2 + (x > 0).astype(jnp.int32)
        for count in range(1, 4):
            pl.when((pair != y) & (levels_in == count))(
                functools.partial(y2_wait, pair, 0, count)
            )
        for i in range(2):
            head = pl.ds(pair * 2 + i, 1)
            rows = pl.ds(64 * i, 64)
            grad = gt[pair, rows]
            enter_hi, enter_lo = split(
                jnp.concatenate([zr[pair, n, rows] for n in range(3)], axis=0)
            )
            mixed = dot(
                jnp.concatenate([enter_hi, enter_lo], axis=0), qb[:, head_cols(pair, i)], NT
            )
            drift_row = drift[head, :]
            for n in range(3):
                state_row = mixed[64 * n : 64 * n + 64] + mixed[192 + 64 * n : 256 + 64 * n]
                level_row = fs[head, :] * jnp.sum(state_row * grad, axis=0, keepdims=True)
                glw[3 + n, head, :] = level_row
                drift_row = drift_row + wts[3 + n, head, :] * level_row
            drift[head, :] = drift_row

    def cross_out(pair):
        pl.when(pair != y)(functools.partial(y2_wait, pair, 3, 1))
        for i in range(2):
            head = pl.ds(pair * 2 + i, 1)
            rows = pl.ds(64 * i, 64)
            leave_hi, leave_lo = split(zr[pair, 3, rows])
            left = dot(
                jnp.concatenate([leave_hi, leave_lo], axis=0), kb[:, head_cols(pair, i)], NT
            )
            value_grad = gvt[pair, rows] + de[head, :] * (left[0:64] + left[64:128])
            gvt[pair, rows] = value_grad
            drift[head, :] = drift[head, :] - jnp.sum(
                vt[pair, rows] * value_grad, axis=0, keepdims=True
            )

    def cross_query(pair):
        for i in range(2):
            head = pl.ds(pair * 2 + i, 1)
            rows = pl.ds(64 * i, 64)
            enter_hi, enter_lo = split(
                jnp.concatenate([zr[pair, n, rows] for n in range(3)], axis=0)
            )
            weighted_hi, weighted_lo = split(
                jnp.concatenate(
                    [gt[pair, rows] * (fs[head, :] * wts[3 + n, head, :]) for n in range(3)], axis=0
                )
            )
            gq[:, head_cols(pair, i)] = gq[:, head_cols(pair, i)] + dot(
                jnp.concatenate([weighted_hi, weighted_lo, weighted_hi], axis=0),
                jnp.concatenate([enter_hi, enter_hi, enter_lo], axis=0), TN,
            )
        back_copy(pair, 0).start()
        wide = pl.ds(pl.multiple_of(pair * 256, 256), 256)
        out_wide = pl.ds(pl.multiple_of(c * 1024 + pair * 256, 256), 256)
        gq_out[:, out_wide] = gq[own_rows, wide].astype(BF16)

    def cross_grad(pair):
        for i in range(2):
            head = pl.ds(pair * 2 + i, 1)
            rows = pl.ds(64 * i, 64)
            leave_hi, leave_lo = split(zr[pair, 3, rows])
            ended_hi, ended_lo = split(vt[pair, rows] * de[head, :])
            gk[:, head_cols(pair, i)] = gk[:, head_cols(pair, i)] + dot(
                jnp.concatenate([ended_hi, ended_lo, ended_hi], axis=0),
                jnp.concatenate([leave_hi, leave_hi, leave_lo], axis=0), TN,
            )
        gv[:, pair_cols(pair)] = jnp.transpose(gvt[pair])
        back_copy(pair, 1).start()
        back_copy(pair, 2).start()
        wide = pl.ds(pl.multiple_of(pair * 256, 256), 256)
        out_wide = pl.ds(pl.multiple_of(c * 1024 + pair * 256, 256), 256)
        out_narrow = pl.ds(pl.multiple_of(c * 512 + pair * 128, 128), 128)
        gk_out[:, out_wide] = gk[own_rows, wide].astype(BF16)
        gv_out[:, out_narrow] = gv[own_rows, pair_cols(pair)].astype(BF16)

    def loop(low, high, body):
        def step(n, carry):
            body(n)
            return carry

        lax.fori_loop(low, high, step, 0)

    loop(0, 4, lambda n: state_fwd(toward(n)))
    swaps[1].wait_recv()
    gb[other_rows, :] = rg[...].astype(BF16)
    swaps[2].wait_recv()
    qb[other_rows, :] = rq[...].astype(BF16)
    loop(0, 4, lambda n: state_back(toward(n)))
    loop(0, 4, lambda n: state_near(toward(n)))
    loop(0, 4, hand_next)
    combine_fwd()
    masks()
    loop(0, 1, intra)
    combine_back()
    loop(1, 2, intra)
    enter_far()
    loop(2, 4, intra)
    leave_far()
    loop(0, 4, lambda n: cross_in(nearby(n)))
    loop(0, 4, lambda n: cross_out(nearby(n)))
    lane = lax.broadcasted_iota(jnp.int32, (8, 256), 1)
    tail = suffix(drift[...], lane)
    drift[...] = tail
    bs_out = remote(small.at[:, :], bs.at[pl.ds(48, 8), :], last_send.at[1], last_recv.at[1], seq_2=other)
    tile = lax.broadcasted_iota(jnp.int32, (8, 128), 1)
    mine = lax.broadcasted_iota(jnp.int32, (8, 128), 0)
    head_total = tail[:, 0:1]
    head_square = jnp.sum(tail * tail, axis=1, keepdims=True)
    head_sum = jnp.sum(tail, axis=1, keepdims=True)
    slots = [
        jnp.where(tile == mine + 8 * n, jnp.broadcast_to(part, (8, 128)), 0.0)
        for n, part in enumerate((head_total, head_square, head_sum))
    ]
    place_here = chip * 8 + group
    a_buf[place_here] = jnp.sum(slots[0] + slots[1] + slots[2], axis=0, keepdims=True)

    def a_copy(dx, dy, dz, dc):
        return remote(
            a_buf.at[place_here], a_buf.at[place_here], a_send.at[0], a_recv.at[0],
            seq_0=(x + dx) % 4, seq_1=(y + dy) % 4, seq_2=(c + dc) % 2, head=(z + dz) % 4,
        )

    def hops(move):
        return -(sum(min(d, 4 - d) for d in move[:3]) + 0.5 * move[3])

    moves = [(dx, dy, dz, dc) for dx in range(4) for dy in range(4) for dz in range(4) for dc in (0, 1)]
    for move in sorted(moves, key=hops):
        if any(move):
            a_copy(*move).start()
    small[...] = drift[:, other_rows]
    for level in range(6):
        ss_rows = slice(8 * level, 8 * level + 8)
        ys[y, 1, ss_rows] = glw[level, :, other_rows]
    glw_copy = remote(
        ys.at[y, 1, pl.ds(0, 48)], bs.at[pl.ds(0, 48), :], last_send.at[0], last_recv.at[0],
        seq_2=other,
    )
    glw_copy.start()
    bs_out.start()
    for level in range(6):
        glw_out[level, own_heads, :] = glw[level, :, own_rows]

    loop(0, 4, cross_query)
    loop(0, 4, cross_grad)
    def back_whole(kind):
        src, dst = ((gq, bq), (gk, bk), (gv, bv))[kind]
        return remote(
            src.at[other_rows, :], dst, out_send.at[kind], out_recv.at[kind], seq_2=other
        )

    for kind in range(3):
        back_whole(kind).wait_recv()
    other_q = pl.ds(pl.multiple_of(other * 1024, 1024), 1024)
    other_v = pl.ds(pl.multiple_of(other * 512, 512), 512)
    gq_out[:, other_q] = bq[...].astype(BF16)
    gk_out[:, other_q] = bk[...].astype(BF16)
    gv_out[:, other_v] = bv[...].astype(BF16)
    glw_copy.wait_recv()
    for level in range(6):
        glw_out[level, other_heads, :] = bs[8 * level : 8 * level + 8, :]

    a_whole = remote(
        a_buf.at[pl.ds(0, 127)], a_buf.at[pl.ds(0, 127)], a_send.at[0], a_recv.at[0], seq_2=other
    )
    a_whole.wait_recv()
    run = jnp.zeros((8, 128), F32)
    later = jnp.zeros((8, 128), F32)
    squares = jnp.zeros((8, 128), F32)
    for at in range(15, -1, -1):
        now = a_buf[8 * at : 8 * at + 8, 0, :]
        later = later + run * (chip == at).astype(F32)
        square = pltpu.roll(now, 120, 1)
        total_of = pltpu.roll(now, 112, 1)
        squares = squares + square + run * (2.0 * total_of + 256.0 * run)
        run = run + now
    squares = jnp.where(tile < 8, squares, 0.0)
    total_square = jnp.sum(jnp.sum(squares, axis=1, keepdims=True), axis=0, keepdims=True)
    factor = jnp.minimum(1.0, lax.rsqrt(total_square / (64 * 4096) + 1e-06))

    def later_of(at_group):
        row = jnp.sum(jnp.where(mine == at_group, later, 0.0), axis=0, keepdims=True)
        return jnp.sum(
            jnp.where(tile == mine, jnp.broadcast_to(row, (8, 128)), 0.0), axis=1, keepdims=True
        )

    glg_out[own_heads, :] = (drift[:, own_rows] + later_of(group)) * factor
    bs_out.wait_recv()
    glg_out[other_heads, :] = (bs[48:56, :] + later_of(z * 2 + other)) * factor

    for swap in swaps:
        swap.wait_send()
    remote(sk, rk, kv_send.at[0], kv_recv.at[0, 0], seq_2=other).wait_send()
    remote(sv, rv, kv_send.at[1], kv_recv.at[1, 0], seq_2=other).wait_send()
    for kind in range(4):

        @pl.when(sent(kind, y))
        def _():
            several(ys, 3, kind, y1_send.at[kind], y1_recv.at[kind]).wait_send()

        def act(count):
            several(zs, count, kind, y2_send.at[kind], y2_recv.at[0, 0]).wait_send()

        if kind == 0:
            pl.when(y % 2 == 0)(lambda: act(3))
        elif kind == 1:
            in_turn(kind, y >= 2, act)
        else:
            pl.when(x > 0 if kind == 2 else y >= 0)(lambda: act(3))

    for pair in range(4):
        @pl.when(pair != x)
        def _():
            x_copy(pair, 0).wait_send()

    for kind in range(3):
        back_whole(kind).wait_send()
    glw_copy.wait_send()
    bs_out.wait_send()
    a_whole.wait_send()


def settle(*refs):
    source, target, sem = refs[:5], refs[5:10], refs[10]
    stores = []
    for n in range(5):
        cuts = 4 if n < 2 else 2 if n == 2 else 1
        rows = source[n].shape[0] // cuts
        for m in range(cuts):
            at = pl.ds(rows * m, rows)
            stores.append(
                pltpu.make_async_copy(source[n].at[at], target[n].at[at], sem.at[len(stores)])
            )
    for store in stores:
        store.start()
    for store in stores:
        store.wait()


def shards(queries, keys, values, out_grad, log_gate, level_weight, doc_start):
    args = (queries, keys, values, out_grad, log_gate, level_weight, doc_start.reshape(1, -1))
    anywhere = pl.BlockSpec(memory_space=pl.ANY)
    results = tuple(
        jax.ShapeDtypeStruct(a.shape, a.dtype)
        for a in (queries, keys, values, level_weight, log_gate)
    )
    held = tuple(pltpu.VMEM(r.shape, r.dtype) for r in results)
    scratch = [pltpu.VMEM(a.shape, a.dtype) for a in args] + [pltpu.SemaphoreType.DMA((7,))]
    swap = [(128, 1024), (128, 1024), (128, 512), (128, 512), (64, 128)]
    scratch += [pltpu.VMEM(s, F32) for s in swap * 2]
    scratch += [pltpu.VMEM(s, BF16) for s in ((256, 1024), (256, 1024), (256, 512), (256, 512))]
    scratch += [pltpu.VMEM((4, 128, 256), F32)] * 2
    scratch += [pltpu.VMEM((8, 256), F32)] * 6
    scratch += [pltpu.VMEM((6, 8, 256), F32), pltpu.VMEM((8, 256, 128), F32)]
    scratch += [pltpu.VMEM((256, 256), F32), pltpu.VMEM((256, 256), BF16), pltpu.VMEM((256, 256), BF16)]
    scratch += [pltpu.VMEM((256, 1024), F32), pltpu.VMEM((256, 1024), F32), pltpu.VMEM((256, 512), F32)]
    scratch += [pltpu.VMEM((4, 128, 256), F32), pltpu.VMEM((6, 8, 256), F32)]
    scratch += [pltpu.VMEM((8, 256), F32), pltpu.VMEM((8, 128), F32)]
    scratch += [pltpu.VMEM((4, 4, 136, 128), F32)] * 2 + [pltpu.VMEM((4, 4, 128, 128), F32)] * 2
    scratch += [pltpu.VMEM((2, 136, 128), F32), pltpu.VMEM((4, 136, 128), F32)]
    scratch += [pltpu.VMEM((128, 128), F32)] * 2
    scratch += [pltpu.VMEM((128, 1024), F32), pltpu.VMEM((128, 1024), F32), pltpu.VMEM((128, 512), F32)]
    scratch += [pltpu.VMEM((56, 128), F32)]
    scratch += [pltpu.VMEM((128, 1, 128), F32)]
    sems = [(3,), (3,), (2,), (2, 4), (4,), (4,), (4,), (4, 2), (4,), (4,), (3,), (3,), (2,), (2,)]
    sems += [(1,)] * 2
    scratch += [pltpu.SemaphoreType.DMA(s) for s in sems]
    outs = pl.pallas_call(
        kernel,
        out_shape=held,
        in_specs=[anywhere] * 7,
        out_specs=[pl.BlockSpec(memory_space=pltpu.VMEM)] * 5,
        scratch_shapes=scratch,
        compiler_params=pltpu.CompilerParams(
            collective_id=0, has_side_effects=True, vmem_limit_bytes=60 * 2**20
        ),
    )(*args)
    return pl.pallas_call(
        settle,
        out_shape=results,
        in_specs=[anywhere] * 5,
        out_specs=[anywhere] * 5,
        scratch_shapes=[pltpu.SemaphoreType.DMA((12,))],
        compiler_params=pltpu.CompilerParams(vmem_limit_bytes=48 * 2**20),
    )(*outs)


def solution(mesh):
    finer = Mesh(
        mesh.devices.reshape(4, 4, 2, mesh.shape["head"]), ("seq_0", "seq_1", "seq_2", "head")
    )
    wide = P(SEQ, "head")
    return jax.shard_map(
        shards,
        mesh=finer,
        in_specs=(wide, wide, wide, wide, P("head", SEQ), P(None, "head", SEQ), P(SEQ)),
        out_specs=(wide, wide, wide, P(None, "head", SEQ), P("head", SEQ)),
        check_vma=False,
    )
```

```python
import functools

import jax
import jax.numpy as jnp
from jax import lax
from jax.experimental import pallas as pl
from jax.experimental.pallas import tpu as pltpu
from jax.sharding import Mesh
from jax.sharding import PartitionSpec as P

SEQ = ("seq_0", "seq_1", "seq_2")
MESH = pl.DeviceIdType.MESH
F32 = jnp.float32
BF16 = jnp.bfloat16
NEG = -1e30

NN = (((1,), (0,)), ((), ()))
NT = (((1,), (1,)), ((), ()))
TN = (((0,), (0,)), ((), ()))


def dot(a, b, dims):
    return lax.dot_general(a, b, dims, preferred_element_type=F32)


def split(a):
    hi = a.astype(BF16)
    return hi, (a - hi.astype(F32)).astype(BF16)


def prefix(a, lane):
    shift = 1
    while shift < a.shape[1]:
        a = a + jnp.where(lane >= shift, pltpu.roll(a, shift, 1), 0.0)
        shift *= 2
    return a


def suffix(a, lane):
    size = a.shape[1]
    shift = 1
    while shift < size:
        a = a + jnp.where(lane < size - shift, pltpu.roll(a, size - shift, 1), 0.0)
        shift *= 2
    return a


def kernel(
    q_hbm, k_hbm, v_hbm, g_hbm, lg_hbm, lw_hbm, ds_hbm,
    gq_out, gk_out, gv_out, glw_out, glg_out,
    q_in, k_in, v_in, g_in, lg_in, lw_in, ds_in, load_sem,
    sq, sk, sv, sg, ss, rq, rk, rv, rg, rs,
    qb, kb, vb, gb, vt, gt,
    gates, doc, cum, resets, fs, de, wts, cm, bias, pt, rt,
    gq, gk, gv, gvt, glw, drift, small,
    ys, yr, zs, zr, xs, xr, ein, xin,
    bq, bk, bv, bs,
    a_buf,
    in_send, in_recv, kv_send, kv_recv, y1_send, y1_recv, y2_send, y2_recv, x_send, x_recv,
    out_send, out_recv, last_send, last_recv, a_send, a_recv,
):
    x, y, c, z = (lax.axis_index(n) for n in ("seq_0", "seq_1", "seq_2", "head"))
    other = 1 - c
    chip = x * 4 + y
    group = z * 2 + c

    def remote(src, dst, send, recv, **to):
        return pltpu.make_async_remote_copy(
            src_ref=src, dst_ref=dst, send_sem=send, recv_sem=recv,
            device_id=to, device_id_type=MESH,
        )

    loads = [
        pltpu.make_async_copy(src, dst, load_sem.at[n])
        for n, (src, dst) in enumerate((
            (ds_hbm, ds_in), (lg_hbm, lg_in), (lw_hbm, lw_in), (k_hbm, k_in),
            (v_hbm, v_in), (g_hbm, g_in), (q_hbm, q_in),
        ))
    ]
    for load in loads:
        load.start()

    barrier = pltpu.get_barrier_semaphore()
    for step in range(1, 4):
        for axis, place in (("seq_1", y), ("seq_0", x)):
            pl.semaphore_signal(
                barrier, inc=1, device_id={axis: (place + step) % 4}, device_id_type=MESH
            )
        pl.semaphore_signal(
            barrier, inc=1, device_id={"head": (z + step) % 4}, device_id_type=MESH
        )
    pl.semaphore_signal(barrier, inc=1, device_id={"seq_2": other}, device_id_type=MESH)

    q_cols = pl.ds(pl.multiple_of(other * 1024, 1024), 1024)
    v_cols = pl.ds(pl.multiple_of(other * 512, 512), 512)
    own_q = pl.ds(pl.multiple_of(c * 1024, 1024), 1024)
    own_v = pl.ds(pl.multiple_of(c * 512, 512), 512)
    own_rows = pl.ds(pl.multiple_of(c * 128, 128), 128)
    other_rows = pl.ds(pl.multiple_of(other * 128, 128), 128)
    own_heads = pl.ds(pl.multiple_of(c * 8, 8), 8)
    other_heads = pl.ds(pl.multiple_of(other * 8, 8), 8)
    swaps = [
        remote(src, dst, in_send.at[n], in_recv.at[n], seq_2=other)
        for n, (src, dst) in enumerate(((ss, rs), (sg, rg), (sq, rq)))
    ]

    def toward(n):
        return (y + jnp.where(n == 2, 3, jnp.where(n == 3, 0, 2 - n))) % 4

    def nearby(n):
        return (y + jnp.where(n == 2, 3, jnp.where(n == 3, 2, n))) % 4

    def key_copy(pair):
        cols = pl.ds(pl.multiple_of(pair * 256, 256), 256)
        return remote(
            sk.at[:, cols], rk.at[:, cols], kv_send.at[0], kv_recv.at[0, pair], seq_2=other
        )

    def value_copy(pair):
        cols = pl.ds(pl.multiple_of(pair * 128, 128), 128)
        return remote(
            sv.at[:, cols], rv.at[:, cols], kv_send.at[1], kv_recv.at[1, pair], seq_2=other
        )

    for load in loads[:3]:
        load.wait()
    ds_row = jnp.broadcast_to(ds_in[...].astype(F32), (8, 128))
    ss[0:8, :] = lg_in[other_heads, :]
    for level in range(6):
        ss[8 + 8 * level : 16 + 8 * level, :] = lw_in[level, other_heads, :]
    ss[56:64, :] = ds_row
    loads[3].wait()
    sk[...] = k_in[:, q_cols].astype(F32)
    loads[4].wait()
    sv[...] = v_in[:, v_cols].astype(F32)
    pl.semaphore_wait(barrier, 10)
    swaps[0].start()
    for n in (2, 1, 3, 0):
        key_copy((y + n) % 4).start()
        value_copy((y + n) % 4).start()
    loads[5].wait()
    sg[...] = g_in[:, v_cols].astype(F32)
    loads[6].wait()
    sq[...] = q_in[:, q_cols].astype(F32)
    for swap in swaps[1:]:
        swap.start()
    kb[own_rows, :] = k_in[:, own_q]
    vb[own_rows, :] = v_in[:, own_v]
    gb[own_rows, :] = g_in[:, own_v]
    qb[own_rows, :] = q_in[:, own_q]
    gates[:, own_rows] = lg_in[own_heads, :]
    for level in range(6):
        wts[level, :, own_rows] = lw_in[level, own_heads, :]
    doc[:, own_rows] = ds_row
    ein[...] = jnp.zeros_like(ein)
    xin[...] = jnp.zeros_like(xin)
    pt[128:256, 0:128] = jnp.zeros((128, 128), BF16)
    rt[128:256, 0:128] = jnp.zeros((128, 128), BF16)

    zero_slab = jnp.zeros((128, 128), F32)
    for level, absent in ((0, y % 2 == 0), (1, y < 2), (2, x == 0)):

        @pl.when(absent)
        def _():
            for pair in range(4):
                zr[pair, level] = zero_slab

    swaps[0].wait_recv()
    gates[:, other_rows] = rs[0:8, :]
    for level in range(6):
        wts[level, :, other_rows] = rs[8 + 8 * level : 16 + 8 * level, :]
    doc[:, other_rows] = rs[56:64, :]
    lane = lax.broadcasted_iota(jnp.int32, (8, 256), 1)
    cum_now = prefix(gates[...], lane)
    reset = prefix(doc[...], lane)
    total = cum_now[:, 255:256]
    reset_total = reset[:, 255:256]
    cum[...] = cum_now
    resets[...] = reset
    fs[...] = jnp.where(reset == 0.0, jnp.exp(cum_now), 0.0)
    de[...] = jnp.where(reset == reset_total, jnp.exp(total - cum_now), 0.0)
    decay = jnp.broadcast_to(jnp.where(reset_total == 0.0, jnp.exp(total), 0.0), (8, 128))
    small[...] = decay
    def masks():
        columns = jnp.transpose(
            jnp.concatenate([cum[...], resets[...], jnp.zeros((112, 256), F32)], axis=0)
        )
        for head in range(8):
            cm[head] = jnp.broadcast_to(columns[:, head : head + 1], (256, 128))
        reset_col = jnp.broadcast_to(columns[:, 8:9], (256, 128))
        for half in range(2):
            reset_row = jnp.broadcast_to(resets[0:1, 128 * half : 128 * half + 128], (256, 128))
            s_pos = lax.broadcasted_iota(jnp.int32, (256, 128), 0)
            t_pos = lax.broadcasted_iota(jnp.int32, (256, 128), 1) + 128 * half
            bias[:, 128 * half : 128 * half + 128] = jnp.where(
                (t_pos >= s_pos) & (reset_col == reset_row), 0.0, NEG
            )

    def head_cols(pair, i):
        return pl.ds(pl.multiple_of(pair * 256 + i * 128, 128), 128)

    def pair_cols(pair):
        return pl.ds(pl.multiple_of(pair * 128, 128), 128)

    def sent(kind, at_y):
        return (True, x > 0, at_y % 2 == 1, at_y >= 2)[kind]

    def y1_copy(pair, kind, at_y):
        rows = 136 if kind == 0 else 128
        return remote(
            ys.at[pair, kind, pl.ds(0, rows)], yr.at[at_y, kind, pl.ds(0, rows)],
            y1_send.at[kind], y1_recv.at[kind], seq_1=pair,
        )

    def place(pair, kind, i, slab):
        rows = pl.ds(64 * i, 64)

        @pl.when(pair == y)
        def _():
            yr[y, kind, rows] = slab

        @pl.when(pair != y)
        def _():
            ys[pair, kind, rows] = slab

    def hand_over(pair, kind):
        @pl.when((pair != y) & sent(kind, y))
        def _():
            y1_copy(pair, kind, y).start()

    def state_fwd(pair):
        wide = pl.ds(pl.multiple_of(pair * 256, 256), 256)
        key_copy(pair).wait_recv()
        kb[other_rows, wide] = rk[:, wide].astype(BF16)
        value_copy(pair).wait_recv()
        vb[other_rows, pair_cols(pair)] = rv[:, pair_cols(pair)].astype(BF16)
        vt[pair] = jnp.transpose(vb[:, pair_cols(pair)].astype(F32))
        for i in range(2):
            head = pl.ds(pair * 2 + i, 1)
            value_hi, value_lo = split(vt[pair, pl.ds(64 * i, 64)] * de[head, :])
            state = dot(
                jnp.concatenate([value_hi, value_lo], axis=0), kb[:, head_cols(pair, i)], NN
            )
            place(pair, 0, i, state[0:64] + state[64:128])
            row = small[head, :]

            @pl.when(pair == y)
            def _():
                yr[y, 0, 128 + i : 129 + i] = row

            @pl.when(pair != y)
            def _():
                ys[pair, 0, 128 + i : 129 + i] = row

        hand_over(pair, 0)

    def state_back(pair):
        gt[pair] = jnp.transpose(gb[:, pair_cols(pair)].astype(F32))
        for i in range(2):
            head = pl.ds(pair * 2 + i, 1)
            hi, lo = split(gt[pair, pl.ds(64 * i, 64)] * (fs[head, :] * wts[5, head, :]))
            back = dot(jnp.concatenate([hi, lo], axis=0), qb[:, head_cols(pair, i)], NN)
            place(pair, 1, i, back[0:64] + back[64:128])
        hand_over(pair, 1)

    def state_near(pair):
        for i in range(2):
            head = pl.ds(pair * 2 + i, 1)
            grad = gt[pair, pl.ds(64 * i, 64)]
            parts = [split(grad * (fs[head, :] * wts[level, head, :])) for level in (3, 4)]
            back = dot(
                jnp.concatenate([p[0] for p in parts] + [p[1] for p in parts], axis=0),
                qb[:, head_cols(pair, i)], NN,
            )
            for n in range(2):
                place(
                    pair, 2 + n, i, back[64 * n : 64 * n + 64] + back[128 + 64 * n : 192 + 64 * n]
                )
        hand_over(pair, 2)
        hand_over(pair, 3)

    def intra(pair):
        for i in range(2):
            number = pair * 2 + i
            head = pl.ds(number, 1)
            rows = pl.ds(64 * i, 64)
            query = qb[:, head_cols(pair, i)]
            key = kb[:, head_cols(pair, i)]
            grad = gb[:, pair_cols(pair)]
            value = vb[:, pair_cols(pair)]
            mine = lax.broadcasted_iota(jnp.int32, (64, 128), 1) // 64 == i
            weight = [wts[level, head, :] for level in range(3)]
            span = lax.broadcasted_iota(jnp.int32, (1, 256), 1) // 64
            cum_row = cum[head, :]
            level_rows = [jnp.zeros((1, 256), F32) for level in range(3)]
            drift_row = jnp.zeros((1, 256), F32)
            for b in range(4):
                low = 0 if b < 2 else 128
                blk = slice(64 * b, 64 * b + 64)
                score = dot(key[blk], query[low:256], NT)
                pair_dot = dot(
                    jnp.where(mine, value[blk], jnp.zeros((64, 128), BF16)), grad[low:256], NT
                )
                col = cm[number, blk, :]
                if low == 0:
                    col = jnp.concatenate([col, col], axis=1)
                decayed = jnp.exp((cum_row[:, low:256] - col) + bias[blk, low:256])
                at = span[:, low:256]
                near = (at == b).astype(jnp.int32), ((at ^ 1) == b).astype(jnp.int32)
                mix = jnp.where(
                    near[0] == 1, weight[0][:, low:256],
                    jnp.where(near[1] == 1, weight[1][:, low:256], weight[2][:, low:256]),
                )
                scored = decayed * score
                joint = jnp.sum(scored * pair_dot, axis=0, keepdims=True)
                prob = (scored * mix).astype(BF16)
                pt[blk, low:256] = prob
                rt[blk, low:256] = (decayed * mix * pair_dot).astype(BF16)
                drifted = jnp.sum(prob.astype(F32) * pair_dot, axis=0, keepdims=True)
                if low:
                    pad = jnp.zeros((1, 128), F32)
                    joint = jnp.concatenate([pad, joint], axis=1)
                    drifted = jnp.concatenate([pad, drifted], axis=1)
                drift_row = drift_row + drifted
                level_rows[0] = level_rows[0] + jnp.where(span == b, joint, 0.0)
                level_rows[1] = level_rows[1] + jnp.where((span ^ 1) == b, joint, 0.0)
                level_rows[2] = level_rows[2] + jnp.where(
                    (span != b) & ((span ^ 1) != b), joint, 0.0
                )
            for level in range(3):
                glw[level, head, :] = level_rows[level]
            drift[head, :] = drift_row
            gvt[pair, rows] = dot(gt[pair, rows].astype(BF16), pt[...], NT)
            gk[:, head_cols(pair, i)] = dot(rt[...], query, NN)
            gq[:, head_cols(pair, i)] = dot(rt[...], key, TN)

    def y2_copy(to_y, kind, src):
        return remote(
            src, zr.at[y, kind], y2_send.at[kind], y2_recv.at[y, kind // 3], seq_1=to_y
        )

    def y2_source(to_y, kind):
        if kind == 0:
            return yr.at[to_y - 1, 0, pl.ds(0, 128)]
        return zs.at[to_y, kind]

    def hand_back(to_y, kind):
        def go():
            @pl.when(to_y != y)
            def _():
                y2_copy(to_y, kind, y2_source(to_y, kind)).start()

            @pl.when(to_y == y)
            def _():
                zr[y, kind] = y2_source(to_y, kind)[...]

        if kind == 2:
            pl.when(x > 0)(go)
        else:
            go()

    def several(buf, count, kind, send, recv):
        rows = pl.ds(0, 136 if kind == 0 and buf is ys else 128)
        return remote(
            buf.at[pl.ds(0, count), kind, rows], buf.at[pl.ds(0, count), kind, rows],
            send, recv, seq_2=other,
        )

    def in_turn(kind, here, act):
        pl.when(here)(lambda: act(1))
        pl.when(jnp.logical_not(here))(lambda: act(2))

    def y1_wait(kind):
        def act(count):
            several(ys, count, kind, y1_send.at[kind], y1_recv.at[kind]).wait_recv()

        if kind == 0:
            act(3)
        elif kind == 1:
            pl.when(x > 0)(lambda: act(3))
        else:
            in_turn(kind, y % 2 == 1 if kind == 2 else y >= 2, act)

    def x_copy(to_x, kind):
        return remote(xs.at[kind], xr.at[x], x_send.at[to_x], x_recv.at[x], seq_0=to_x)

    def decays(i):
        return [yr[n, 0, 128 + i : 129 + i] for n in range(4)]

    def combine_fwd():
        y1_wait(0)
        for i in range(2):
            rows = slice(64 * i, 64 * i + 64)
            dec = decays(i)
            both = dec[1] * yr[0, 0, rows] + yr[1, 0, rows]
            zs[2, 1, rows] = both
            after = dec[2] * both
            zs[3, 1, rows] = after
            xs[0, rows] = dec[3] * (after + yr[2, 0, rows]) + yr[3, 0, rows]
            all_decay = dec[0] * dec[1] * (dec[2] * dec[3])
            xs[0, 128 + i : 129 + i] = all_decay
            xs[1, 128 + i : 129 + i] = all_decay
        for to_x in range(4):

            @pl.when(to_x > x)
            def _():
                x_copy(to_x, 0).start()

        @pl.when(y % 2 == 1)
        def _():
            zr[y, 0] = yr[(y + 3) % 4, 0, 0:128]

        hand_back(2, 1)
        hand_back(3, 1)

    def combine_back():
        y1_wait(1)

        @pl.when(x > 0)
        def _():
            for i in range(2):
                rows = slice(64 * i, 64 * i + 64)
                dec = decays(i)
                back = yr[2, 1, rows] + dec[2] * yr[3, 1, rows]
                back = yr[1, 1, rows] + dec[1] * back
                xs[1, rows] = yr[0, 1, rows] + dec[0] * back

        for to_x in range(4):

            @pl.when(to_x < x)
            def _():
                x_copy(to_x, 1).start()


    def next_copy(pair, src):
        return remote(
            src, zr.at[pair, 0], y2_send.at[0], y2_recv.at[pair, 0], seq_1=(y + 1) % 4
        )

    def hand_next(pair):
        @pl.when((y % 2 == 0) & (pair == y))
        def _():
            next_copy(pair, yr.at[y, 0, pl.ds(0, 128)]).start()

        @pl.when((y % 2 == 0) & (pair != y) & (pair != y + 1))
        def _():
            next_copy(pair, ys.at[pair, 0, pl.ds(0, 128)]).start()

    def take(acc, at_x):
        remote(
            xs.at[0], xr.at[at_x], x_send.at[at_x], x_recv.at[at_x], seq_0=at_x
        ).wait_recv()
        for i in range(2):
            rows = slice(64 * i, 64 * i + 64)
            acc[rows] = xr[at_x, 128 + i : 129 + i] * acc[rows] + xr[at_x, rows]

    def enter_far():
        for at_x in range(4):
            pl.when(at_x < x)(functools.partial(take, ein, at_x))
        for i in range(2):
            rows = slice(64 * i, 64 * i + 64)
            dec = decays(i)
            into = ein[rows]
            for at_y in range(4):
                zs[at_y, 2, rows] = into
                into = dec[at_y] * into
        for step in (2, 1, 3, 0):
            hand_back((y + step) % 4, 2)

    def leave_far():
        y1_wait(2)
        y1_wait(3)
        for at_x in range(3, -1, -1):
            pl.when(at_x > x)(functools.partial(take, xin, at_x))
        for i in range(2):
            rows = slice(64 * i, 64 * i + 64)
            dec = decays(i)
            late = xin[rows]
            zs[3, 3, rows] = late
            late = dec[3] * late
            zs[2, 3, rows] = late + yr[3, 2, rows]
            late = dec[2] * late + (yr[2, 3, rows] + dec[2] * yr[3, 3, rows])
            zs[1, 3, rows] = late
            zs[0, 3, rows] = dec[1] * late + yr[1, 2, rows]
        for step in (2, 1, 3, 0):
            hand_back((y + step) % 4, 3)

    def back_copy(pair, kind):
        if kind == 2:
            cols, src, dst = pair_cols(pair), gv, bv
        else:
            cols = pl.ds(pl.multiple_of(pair * 256, 256), 256)
            src, dst = ((gq, bq), (gk, bk))[kind]
        return remote(
            src.at[other_rows, cols], dst.at[:, cols],
            out_send.at[kind], out_recv.at[kind], seq_2=other,
        )

    def y2_wait(pair, first, count):
        remote(
            zr.at[pair, pl.ds(0, count)], zr.at[pair, pl.ds(0, count)], y2_send.at[0],
            y2_recv.at[pair, first // 3], seq_1=pair,
        ).wait_recv()

    def cross_in(pair):
        levels_in = y % 2 + y // 2 + (x > 0).astype(jnp.int32)
        for count in range(1, 4):
            pl.when((pair != y) & (levels_in == count))(
                functools.partial(y2_wait, pair, 0, count)
            )
        for i in range(2):
            head = pl.ds(pair * 2 + i, 1)
            rows = pl.ds(64 * i, 64)
            grad = gt[pair, rows]
            enter_hi, enter_lo = split(
                jnp.concatenate([zr[pair, n, rows] for n in range(3)], axis=0)
            )
            mixed = dot(
                jnp.concatenate([enter_hi, enter_lo], axis=0), qb[:, head_cols(pair, i)], NT
            )
            drift_row = drift[head, :]
            for n in range(3):
                state_row = mixed[64 * n : 64 * n + 64] + mixed[192 + 64 * n : 256 + 64 * n]
                level_row = fs[head, :] * jnp.sum(state_row * grad, axis=0, keepdims=True)
                glw[3 + n, head, :] = level_row
                drift_row = drift_row + wts[3 + n, head, :] * level_row
            drift[head, :] = drift_row

    def cross_out(pair):
        pl.when(pair != y)(functools.partial(y2_wait, pair, 3, 1))
        for i in range(2):
            head = pl.ds(pair * 2 + i, 1)
            rows = pl.ds(64 * i, 64)
            leave_hi, leave_lo = split(zr[pair, 3, rows])
            left = dot(
                jnp.concatenate([leave_hi, leave_lo], axis=0), kb[:, head_cols(pair, i)], NT
            )
            value_grad = gvt[pair, rows] + de[head, :] * (left[0:64] + left[64:128])
            gvt[pair, rows] = value_grad
            drift[head, :] = drift[head, :] - jnp.sum(
                vt[pair, rows] * value_grad, axis=0, keepdims=True
            )

    def cross_query(pair):
        for i in range(2):
            head = pl.ds(pair * 2 + i, 1)
            rows = pl.ds(64 * i, 64)
            enter_hi, enter_lo = split(
                jnp.concatenate([zr[pair, n, rows] for n in range(3)], axis=0)
            )
            weighted_hi, weighted_lo = split(
                jnp.concatenate(
                    [gt[pair, rows] * (fs[head, :] * wts[3 + n, head, :]) for n in range(3)], axis=0
                )
            )
            gq[:, head_cols(pair, i)] = gq[:, head_cols(pair, i)] + dot(
                jnp.concatenate([weighted_hi, weighted_lo, weighted_hi], axis=0),
                jnp.concatenate([enter_hi, enter_hi, enter_lo], axis=0), TN,
            )
        back_copy(pair, 0).start()
        wide = pl.ds(pl.multiple_of(pair * 256, 256), 256)
        out_wide = pl.ds(pl.multiple_of(c * 1024 + pair * 256, 256), 256)
        gq_out[:, out_wide] = gq[own_rows, wide].astype(BF16)

    def cross_grad(pair):
        for i in range(2):
            head = pl.ds(pair * 2 + i, 1)
            rows = pl.ds(64 * i, 64)
            leave_hi, leave_lo = split(zr[pair, 3, rows])
            ended_hi, ended_lo = split(vt[pair, rows] * de[head, :])
            gk[:, head_cols(pair, i)] = gk[:, head_cols(pair, i)] + dot(
                jnp.concatenate([ended_hi, ended_lo, ended_hi], axis=0),
                jnp.concatenate([leave_hi, leave_hi, leave_lo], axis=0), TN,
            )
        gv[:, pair_cols(pair)] = jnp.transpose(gvt[pair])
        back_copy(pair, 1).start()
        back_copy(pair, 2).start()
        wide = pl.ds(pl.multiple_of(pair * 256, 256), 256)
        out_wide = pl.ds(pl.multiple_of(c * 1024 + pair * 256, 256), 256)
        out_narrow = pl.ds(pl.multiple_of(c * 512 + pair * 128, 128), 128)
        gk_out[:, out_wide] = gk[own_rows, wide].astype(BF16)
        gv_out[:, out_narrow] = gv[own_rows, pair_cols(pair)].astype(BF16)

    def loop(low, high, body):
        def step(n, carry):
            body(n)
            return carry

        lax.fori_loop(low, high, step, 0)

    loop(0, 4, lambda n: state_fwd(toward(n)))
    swaps[1].wait_recv()
    gb[other_rows, :] = rg[...].astype(BF16)
    swaps[2].wait_recv()
    qb[other_rows, :] = rq[...].astype(BF16)
    loop(0, 4, lambda n: state_back(toward(n)))
    loop(0, 4, lambda n: state_near(toward(n)))
    loop(0, 4, hand_next)
    combine_fwd()
    masks()
    loop(0, 1, intra)
    combine_back()
    loop(1, 2, intra)
    enter_far()
    loop(2, 4, intra)
    leave_far()
    loop(0, 4, lambda n: cross_in(nearby(n)))
    loop(0, 4, lambda n: cross_out(nearby(n)))
    lane = lax.broadcasted_iota(jnp.int32, (8, 256), 1)
    tail = suffix(drift[...], lane)
    drift[...] = tail
    bs_out = remote(small.at[:, :], bs.at[pl.ds(48, 8), :], last_send.at[1], last_recv.at[1], seq_2=other)
    tile = lax.broadcasted_iota(jnp.int32, (8, 128), 1)
    mine = lax.broadcasted_iota(jnp.int32, (8, 128), 0)
    head_total = tail[:, 0:1]
    head_square = jnp.sum(tail * tail, axis=1, keepdims=True)
    head_sum = jnp.sum(tail, axis=1, keepdims=True)
    slots = [
        jnp.where(tile == mine + 8 * n, jnp.broadcast_to(part, (8, 128)), 0.0)
        for n, part in enumerate((head_total, head_square, head_sum))
    ]
    place_here = chip * 8 + group
    a_buf[place_here] = jnp.sum(slots[0] + slots[1] + slots[2], axis=0, keepdims=True)

    def a_copy(dx, dy, dz, dc):
        return remote(
            a_buf.at[place_here], a_buf.at[place_here], a_send.at[0], a_recv.at[0],
            seq_0=(x + dx) % 4, seq_1=(y + dy) % 4, seq_2=(c + dc) % 2, head=(z + dz) % 4,
        )

    def hops(move):
        return -(sum(min(d, 4 - d) for d in move[:3]) + 0.5 * move[3])

    moves = [(dx, dy, dz, dc) for dx in range(4) for dy in range(4) for dz in range(4) for dc in (0, 1)]
    for move in sorted(moves, key=hops):
        if any(move):
            a_copy(*move).start()
    small[...] = drift[:, other_rows]
    for level in range(6):
        ss_rows = slice(8 * level, 8 * level + 8)
        ys[y, 1, ss_rows] = glw[level, :, other_rows]
    glw_copy = remote(
        ys.at[y, 1, pl.ds(0, 48)], bs.at[pl.ds(0, 48), :], last_send.at[0], last_recv.at[0],
        seq_2=other,
    )
    glw_copy.start()
    bs_out.start()
    for level in range(6):
        glw_out[level, own_heads, :] = glw[level, :, own_rows]

    loop(0, 4, cross_query)
    loop(0, 4, cross_grad)
    def back_whole(kind):
        src, dst = ((gq, bq), (gk, bk), (gv, bv))[kind]
        return remote(
            src.at[other_rows, :], dst, out_send.at[kind], out_recv.at[kind], seq_2=other
        )

    for kind in range(3):
        back_whole(kind).wait_recv()
    other_q = pl.ds(pl.multiple_of(other * 1024, 1024), 1024)
    other_v = pl.ds(pl.multiple_of(other * 512, 512), 512)
    gq_out[:, other_q] = bq[...].astype(BF16)
    gk_out[:, other_q] = bk[...].astype(BF16)
    gv_out[:, other_v] = bv[...].astype(BF16)
    glw_copy.wait_recv()
    for level in range(6):
        glw_out[level, other_heads, :] = bs[8 * level : 8 * level + 8, :]

    a_whole = remote(
        a_buf.at[pl.ds(0, 127)], a_buf.at[pl.ds(0, 127)], a_send.at[0], a_recv.at[0], seq_2=other
    )
    a_whole.wait_recv()
    run = jnp.zeros((8, 128), F32)
    later = jnp.zeros((8, 128), F32)
    squares = jnp.zeros((8, 128), F32)
    for at in range(15, -1, -1):
        now = a_buf[8 * at : 8 * at + 8, 0, :]
        later = later + run * (chip == at).astype(F32)
        square = pltpu.roll(now, 120, 1)
        total_of = pltpu.roll(now, 112, 1)
        squares = squares + square + run * (2.0 * total_of + 256.0 * run)
        run = run + now
    squares = jnp.where(tile < 8, squares, 0.0)
    total_square = jnp.sum(jnp.sum(squares, axis=1, keepdims=True), axis=0, keepdims=True)
    factor = jnp.minimum(1.0, lax.rsqrt(total_square / (64 * 4096) + 1e-06))

    def later_of(at_group):
        row = jnp.sum(jnp.where(mine == at_group, later, 0.0), axis=0, keepdims=True)
        return jnp.sum(
            jnp.where(tile == mine, jnp.broadcast_to(row, (8, 128)), 0.0), axis=1, keepdims=True
        )

    glg_out[own_heads, :] = (drift[:, own_rows] + later_of(group)) * factor
    bs_out.wait_recv()
    glg_out[other_heads, :] = (bs[48:56, :] + later_of(z * 2 + other)) * factor

    for swap in swaps:
        swap.wait_send()
    remote(sk, rk, kv_send.at[0], kv_recv.at[0, 0], seq_2=other).wait_send()
    remote(sv, rv, kv_send.at[1], kv_recv.at[1, 0], seq_2=other).wait_send()
    for kind in range(4):

        @pl.when(sent(kind, y))
        def _():
            several(ys, 3, kind, y1_send.at[kind], y1_recv.at[kind]).wait_send()

        def act(count):
            several(zs, count, kind, y2_send.at[kind], y2_recv.at[0, 0]).wait_send()

        if kind == 0:
            pl.when(y % 2 == 0)(lambda: act(3))
        elif kind == 1:
            in_turn(kind, y >= 2, act)
        else:
            pl.when(x > 0 if kind == 2 else y >= 0)(lambda: act(3))

    for pair in range(4):
        @pl.when(pair != x)
        def _():
            x_copy(pair, 0).wait_send()

    for kind in range(3):
        back_whole(kind).wait_send()
    glw_copy.wait_send()
    bs_out.wait_send()
    a_whole.wait_send()


def settle(*refs):
    source, target, sem = refs[:5], refs[5:10], refs[10]
    stores = []
    for n in range(5):
        cuts = 1
        rows = source[n].shape[0] // cuts
        for m in range(cuts):
            at = pl.ds(rows * m, rows)
            stores.append(
                pltpu.make_async_copy(source[n].at[at], target[n].at[at], sem.at[len(stores)])
            )
    for store in stores:
        store.start()
    for store in stores:
        store.wait()


def shards(queries, keys, values, out_grad, log_gate, level_weight, doc_start):
    args = (queries, keys, values, out_grad, log_gate, level_weight, doc_start.reshape(1, -1))
    anywhere = pl.BlockSpec(memory_space=pl.ANY)
    results = tuple(
        jax.ShapeDtypeStruct(a.shape, a.dtype)
        for a in (queries, keys, values, level_weight, log_gate)
    )
    held = tuple(pltpu.VMEM(r.shape, r.dtype) for r in results)
    scratch = [pltpu.VMEM(a.shape, a.dtype) for a in args] + [pltpu.SemaphoreType.DMA((7,))]
    swap = [(128, 1024), (128, 1024), (128, 512), (128, 512), (64, 128)]
    scratch += [pltpu.VMEM(s, F32) for s in swap * 2]
    scratch += [pltpu.VMEM(s, BF16) for s in ((256, 1024), (256, 1024), (256, 512), (256, 512))]
    scratch += [pltpu.VMEM((4, 128, 256), F32)] * 2
    scratch += [pltpu.VMEM((8, 256), F32)] * 6
    scratch += [pltpu.VMEM((6, 8, 256), F32), pltpu.VMEM((8, 256, 128), F32)]
    scratch += [pltpu.VMEM((256, 256), F32), pltpu.VMEM((256, 256), BF16), pltpu.VMEM((256, 256), BF16)]
    scratch += [pltpu.VMEM((256, 1024), F32), pltpu.VMEM((256, 1024), F32), pltpu.VMEM((256, 512), F32)]
    scratch += [pltpu.VMEM((4, 128, 256), F32), pltpu.VMEM((6, 8, 256), F32)]
    scratch += [pltpu.VMEM((8, 256), F32), pltpu.VMEM((8, 128), F32)]
    scratch += [pltpu.VMEM((4, 4, 136, 128), F32)] * 2 + [pltpu.VMEM((4, 4, 128, 128), F32)] * 2
    scratch += [pltpu.VMEM((2, 136, 128), F32), pltpu.VMEM((4, 136, 128), F32)]
    scratch += [pltpu.VMEM((128, 128), F32)] * 2
    scratch += [pltpu.VMEM((128, 1024), F32), pltpu.VMEM((128, 1024), F32), pltpu.VMEM((128, 512), F32)]
    scratch += [pltpu.VMEM((56, 128), F32)]
    scratch += [pltpu.VMEM((128, 1, 128), F32)]
    sems = [(3,), (3,), (2,), (2, 4), (4,), (4,), (4,), (4, 2), (4,), (4,), (3,), (3,), (2,), (2,)]
    sems += [(1,)] * 2
    scratch += [pltpu.SemaphoreType.DMA(s) for s in sems]
    outs = pl.pallas_call(
        kernel,
        out_shape=held,
        in_specs=[anywhere] * 7,
        out_specs=[pl.BlockSpec(memory_space=pltpu.VMEM)] * 5,
        scratch_shapes=scratch,
        compiler_params=pltpu.CompilerParams(
            collective_id=0, has_side_effects=True, vmem_limit_bytes=60 * 2**20
        ),
    )(*args)
    return pl.pallas_call(
        settle,
        out_shape=results,
        in_specs=[anywhere] * 5,
        out_specs=[anywhere] * 5,
        scratch_shapes=[pltpu.SemaphoreType.DMA((12,))],
        compiler_params=pltpu.CompilerParams(vmem_limit_bytes=48 * 2**20),
    )(*outs)


def solution(mesh):
    finer = Mesh(
        mesh.devices.reshape(4, 4, 2, mesh.shape["head"]), ("seq_0", "seq_1", "seq_2", "head")
    )
    wide = P(SEQ, "head")
    return jax.shard_map(
        shards,
        mesh=finer,
        in_specs=(wide, wide, wide, wide, P("head", SEQ), P(None, "head", SEQ), P(SEQ)),
        out_specs=(wide, wide, wide, P(None, "head", SEQ), P("head", SEQ)),
        check_vma=False,
    )
```
